32 devices in a mesh: dp: 4 (over y, x), seq: 8 (over z, core).
Axes of the slice: x: 2, y: 2, z: 4, core: 2. Of those that a mesh axis runs over, the one named last changes fastest.
Arguments:
- inputs: bfloat16 [2, 4, 1024, 768], P(None, 'dp', 'seq'), may hold values from -6 to 6
- row_segment: int32 [2, 4, 1024], P(None, 'dp', 'seq'), may hold values from 0 to 7, as said below
- row_flag: int32 [2, 4, 1024], P(None, 'dp', 'seq'), may hold values from 0 to 1, as said below
- row_block: int32 [2, 4, 1024], P(None, 'dp', 'seq'), may hold values from 0 to 31, as said below
- norm1_scale: float32 [768], P('seq'), may hold values from 0.5 to 1.5
- w_qkv: float32 [768, 2304], P('dp', 'seq'), may hold values from -0.21875 to 0.21875
- w_out: float32 [768, 768], P('dp', 'seq'), may hold values from -1.75 to 1.75
- norm2_scale: float32 [768], P('seq'), may hold values from 0.5 to 1.5
- w_fc1: float32 [768, 3072], P('dp', 'seq'), may hold values from -0.21875 to 0.21875
- b_fc1: float32 [3072], P('seq'), may hold values from -3 to 3
- w_fc2: float32 [3072, 768], P('dp', 'seq'), may hold values from -0.109375 to 0.109375
- b_fc2: float32 [768], P('seq'), may hold values from -3 to 3
- cotangent: bfloat16 [2, 4, 1024, 768], P(None, 'dp', 'seq'), may hold values from -6 to 6
Outputs:
- outputs: bfloat16 [2, 4, 1024, 768], P(None, 'dp', 'seq')
- input_grad: bfloat16 [2, 4, 1024, 768], P(None, 'dp', 'seq')
- norm1_scale_grad: float32 [768], P('seq')
- w_qkv_grad: float32 [768, 2304], P('dp', 'seq')
- w_out_grad: float32 [768, 768], P('dp', 'seq')
- norm2_scale_grad: float32 [768], P('seq')
- w_fc1_grad: float32 [768, 3072], P('dp', 'seq')
- b_fc1_grad: float32 [3072], P('seq')
- w_fc2_grad: float32 [3072, 768], P('dp', 'seq')
- b_fc2_grad: float32 [768], P('seq')
The draws below stay inside these ranges and needn't reach their ends.
Inputs may be any that keep to these rules, and one draw needn't show every extreme that they name: `row_flag`: in every sequence each aligned group of 16 rows carries one flag and one block number, and each pair of a flag and a block 0 to 31 is carried by exactly one group. `row_block`: constant on each aligned group of 16 rows; see row_flag. `row_segment`: A function of the position 16 * row_block + (row mod 16) alone, the same for the noisy and the clean row of a position, never falling as the position grows; every sequence holds exactly 8 documents, numbered from 0.
All inputs are finite; a program needn't handle non-finite values.
Results may differ from the reference program's by a relative error of at most 0.02.
Values may be sent and summed in bfloat16 or wider, within the bound.
No kernel may reach another device: no remote copies, remote signals or barrier semaphores. Data moves between devices by JAX's collectives and lax.ppermute only.
A program may use at most 192 MiB of HBM per device.

```python
import jax
import jax.numpy as jnp
from jax import lax

D = 768
H = 12
HD = 64
FF = 3072
BLK = 16
MB = 2
SEQS = 4
R = 1024
L = 512
NB = 32
DOCS = 8


def layout(key):
    base = jax.random.fold_in(key, 11)
    seq_keys = jax.random.split(base, MB * SEQS)

    def one_sequence(seq_key):
        order_key, cut_key = jax.random.split(seq_key, 2)
        order = jax.random.permutation(order_key, 2 * NB).astype(jnp.int32)
        flags = jnp.repeat(order // NB, BLK)
        blocks = jnp.repeat(order % NB, BLK)
        shuffled = jax.random.permutation(cut_key, L - 1).astype(jnp.int32) + 1
        starts = shuffled[:DOCS - 1]
        positions = blocks * BLK + jnp.arange(R, dtype=jnp.int32) % BLK
        segments = jnp.sum((starts[None, :] <= positions[:, None]).astype(jnp.int32), axis=1)
        return (segments.astype(jnp.int32), flags.astype(jnp.int32), blocks.astype(jnp.int32))
    segments, flags, blocks = jax.vmap(one_sequence)(seq_keys)
    return (segments.reshape(MB, SEQS, R), flags.reshape(MB, SEQS, R), blocks.reshape(MB, SEQS, R))


def draw_row_segment(key, part):
    return layout(key)[0]


def draw_row_flag(key, part):
    return layout(key)[1]


def draw_row_block(key, part):
    return layout(key)[2]


def block_levels(stream_key, extent, shards, least, high):
    gain, own = 1.0, jax.random.fold_in(stream_key, 6)
    for dim, shards_of in shards:
        steps = jnp.exp(jax.random.uniform(jax.random.fold_in(own, dim), (shards_of,), jnp.float32, least / len(shards), high / len(shards)))
        gain = gain * jnp.repeat(steps, extent[dim] // shards_of).reshape([-1 if axis == dim else 1 for axis in range(len(extent))])
    return gain


def noise(key, shape, spread, most, shards=(), held_as=jnp.bfloat16):
    array = spread * jax.random.normal(key, shape, jnp.float32)
    if shards:
        array = array * block_levels(key, shape, shards, -0.22, 0.18)
    return jnp.clip(array, -most, most).astype(held_as)


def setup_inputs(seed: int = 0) -> dict:
    arg_keys = jax.random.split(jax.random.key(seed), 14)
    inputs = noise(arg_keys[0], (MB, SEQS, R, D), 1.0, 6.0, ((1, 4), (2, 8)))
    row_segment = draw_row_segment(jax.random.fold_in(arg_keys[13], 71), 0)
    row_flag = draw_row_flag(jax.random.fold_in(arg_keys[13], 71), 0)
    row_block = draw_row_block(jax.random.fold_in(arg_keys[13], 71), 0)
    norm1_scale = jnp.clip(1.0 + 0.1 * jax.random.normal(arg_keys[4], (D,), jnp.float32), 0.5, 1.5)
    w_qkv = noise(arg_keys[5], (D, 3 * D), D ** -0.5, 0.21875, ((0, 4), (1, 8)), jnp.float32)
    w_out = noise(arg_keys[6], (D, D), (max(D // 64, 1)) ** -0.5, 1.75, ((0, 4), (1, 8)), jnp.float32)
    norm2_scale = jnp.clip(1.0 + 0.1 * jax.random.normal(arg_keys[7], (D,), jnp.float32), 0.5, 1.5)
    w_fc1 = noise(arg_keys[8], (D, FF), D ** -0.5, 0.21875, ((0, 4), (1, 8)), jnp.float32)
    b_fc1 = noise(arg_keys[9], (FF,), 0.5, 3.0, ((0, 8),), jnp.float32)
    w_fc2 = noise(arg_keys[10], (FF, D), FF ** -0.5, 0.109375, ((0, 4), (1, 8)), jnp.float32)
    b_fc2 = noise(arg_keys[11], (D,), 0.5, 3.0, ((0, 8),), jnp.float32)
    cotangent = noise(arg_keys[12], (MB, SEQS, R, D), 1.0, 6.0, ((1, 4), (2, 8)))
    return dict(inputs=inputs, row_segment=row_segment, row_flag=row_flag, row_block=row_block, norm1_scale=norm1_scale, w_qkv=w_qkv, w_out=w_out, norm2_scale=norm2_scale, w_fc1=w_fc1, b_fc1=b_fc1, w_fc2=w_fc2, b_fc2=b_fc2, cotangent=cotangent)


highest = lax.Precision.HIGHEST

@jax.custom_vjp
def low(v):
    return lax.optimization_barrier(v.astype(jnp.bfloat16)).astype(jnp.float32)

@jax.custom_vjp
def low_back(v):
    return v

def low_keep(v):
    return (low(v), None)

def low_pass(kept, grad):
    return (grad,)

def back_keep(v):
    return (v, None)

def back_low(kept, grad):
    return (low(grad),)
low.defvjp(low_keep, low_pass)
low_back.defvjp(back_keep, back_low)

def layer_norm(v):
    row_mean = lax.optimization_barrier(jnp.mean(v, axis=-1, keepdims=True))
    centered = v - row_mean
    row_var = lax.optimization_barrier(jnp.mean(centered * centered, axis=-1, keepdims=True))
    return centered * lax.rsqrt(row_var + 1e-05)

def rotate(t, cosine, sine_table):
    half_width = t.shape[-1] // 2
    leading = t[..., :half_width]
    trailing = t[..., half_width:]
    return jnp.concatenate([leading * cosine - trailing * sine_table, trailing * cosine + leading * sine_table], axis=-1)

def angles(block_ids):
    count_rows = block_ids.shape[0]
    positions = (block_ids * BLK + jnp.arange(count_rows, dtype=jnp.int32) % BLK).astype(jnp.float32)
    frequency = 10000.0 ** (-2.0 * jnp.arange(HD // 2, dtype=jnp.float32) / HD)
    phase_angle = positions[:, None] * frequency[None, :]
    return (jnp.cos(phase_angle)[:, None, :], jnp.sin(phase_angle)[:, None, :])

def allowed(own_labels, key_labels):
    same_doc = own_labels[0][:, None] == key_labels[0][None, :]
    query_flag = own_labels[1][:, None]
    key_flag = key_labels[1][None, :]
    query_block = own_labels[2][:, None]
    key_block = key_labels[2][None, :]
    noisy_pair = (query_flag == 0) & (key_flag == 0) & (query_block == key_block)
    cross_pair = (query_flag == 0) & (key_flag == 1) & (key_block < query_block)
    clean_pair = (query_flag == 1) & (key_flag == 1) & (key_block <= query_block)
    return same_doc & (noisy_pair | cross_pair | clean_pair)

def attention(queries, keys, values, labels):
    total_rows = queries.shape[0]
    block_rows = min(512, total_rows)
    count = total_rows // block_rows

    def one_block(position):
        offset = (position * block_rows).astype(jnp.int32)
        query_block = lax.dynamic_slice_in_dim(queries, offset, block_rows, 0)
        own_labels = lax.dynamic_slice_in_dim(labels, offset, block_rows, 1)
        scores = jnp.einsum('qhd,khd->hqk', query_block, keys, precision=highest) * HD ** (-0.5)
        scores = low_back(scores)
        pairs = allowed(own_labels, labels)
        scores = jnp.where(pairs[None], scores, -1e+30)
        probs = jax.nn.softmax(scores, axis=-1)
        return jnp.einsum('hqk,khd->qhd', low(probs), values, precision=highest)
    blocks = lax.map(jax.checkpoint(one_block), jnp.arange(count, dtype=jnp.int32))
    return blocks.reshape(total_rows, H, HD)

def forward(hidden_in, gain_one, w_qkv, w_out, gain_two, w_fc1, b_fc1, w_fc2, b_fc2, labels):
    total_rows = hidden_in.shape[0]
    first_in = low(layer_norm(hidden_in) * low(gain_one))
    projected = low_back(jnp.dot(first_in, low(w_qkv), precision=highest))
    cosine, sine_table = angles(labels[2])
    queries = low(rotate(projected[:, :D].reshape(total_rows, H, HD), cosine, sine_table))
    keys = low(rotate(projected[:, D:2 * D].reshape(total_rows, H, HD), cosine, sine_table))
    values = low(projected[:, 2 * D:].reshape(total_rows, H, HD))
    attended = attention(queries, keys, values, labels).reshape(total_rows, D)
    mixed = low(low_back(attended))
    residual = hidden_in + low_back(jnp.dot(mixed, low(w_out), precision=highest))
    second_in = low(layer_norm(residual) * low(gain_two))
    pre_act = low_back(jnp.dot(second_in, low(w_fc1), precision=highest) + low(b_fc1))
    activated = low(jax.nn.gelu(pre_act, approximate=True))
    branch = low_back(jnp.dot(activated, low(w_fc2), precision=highest) + low(b_fc2))
    return residual + branch

def reference(inputs, row_segment, row_flag, row_block, norm1_scale, w_qkv, w_out, norm2_scale, w_fc1, b_fc1, w_fc2, b_fc2, cotangent):
    params = (norm1_scale, w_qkv, w_out, norm2_scale, w_fc1, b_fc1, w_fc2, b_fc2)
    count = inputs.shape[0] * inputs.shape[1]
    total_rows = inputs.shape[2]
    flat_in = inputs.reshape(count, total_rows, D)
    flat_cot = cotangent.reshape(count, total_rows, D)
    flat_labels = jnp.stack([row_segment.reshape(count, total_rows), row_flag.reshape(count, total_rows), row_block.reshape(count, total_rows)], axis=1)

    def add_sequence(totals, sequence_data):
        hidden_in, cot_rows, labels = sequence_data

        def run_layer(x_rows, *weights):
            return forward(x_rows, *weights, labels)
        result_rows, pull_back = jax.vjp(run_layer, hidden_in.astype(jnp.float32), *params)
        grads = pull_back(cot_rows.astype(jnp.float32))
        totals = tuple((a + b for a, b in zip(totals, grads[1:])))
        return (totals, (result_rows.astype(jnp.bfloat16), grads[0].astype(jnp.bfloat16)))
    zeros = tuple((jnp.zeros_like(p) for p in params))
    totals, (result_all, grad_all) = lax.scan(add_sequence, zeros, (flat_in, flat_cot, flat_labels))
    return (result_all.reshape(inputs.shape), grad_all.reshape(inputs.shape), totals[0], totals[1], totals[2], totals[3], totals[4], totals[5], totals[6], totals[7])
```

```python
import functools

import jax
import jax.numpy as jnp
import numpy as np
from jax import lax
from jax.experimental import pallas as pl
from jax.experimental.pallas import tpu as pltpu
from jax.sharding import PartitionSpec as P

D = 768
H = 12
HD = 64
FF = 3072
BLK = 16
F32 = jnp.float32
BF = jnp.bfloat16
NEG = -1e30
VMEM_LIMIT = 56 * 1024 * 1024


def cost(flops, nbytes):
    return pl.CostEstimate(flops=int(flops), bytes_accessed=int(nbytes), transcendentals=0)


def params(*semantics):
    return pltpu.CompilerParams(
        dimension_semantics=semantics or None, vmem_limit_bytes=VMEM_LIMIT
    )


def dot(a, b):
    return lax.dot_general(a, b, (((1,), (0,)), ((), ())), preferred_element_type=F32)


def dot_t(a, b):
    return lax.dot_general(a, b, (((1,), (1,)), ((), ())), preferred_element_type=F32)


def whole(shape):
    return pl.BlockSpec(shape, lambda *_: (0,) * len(shape))


def cuts(count, step):
    return [(at, min(step, count - at)) for at in range(0, count, step)]


def lane_mask(width, head):
    lanes = lax.broadcasted_iota(jnp.int32, (1, width), 1)
    return jnp.where(lanes // HD == head, 1.0, 0.0).astype(BF)


def per_head(block, heads):
    return jnp.concatenate([block * lane_mask(block.shape[1], h) for h in range(heads)], axis=0)


def swap_halves(v):
    out = []
    for at in range(0, v.shape[1], 128):
        part = v[:, at : at + 128]
        lanes = lax.broadcasted_iota(jnp.int32, part.shape, 1)
        out.append(
            jnp.where(
                lanes % HD < HD // 2,
                pltpu.roll(part, 128 - HD // 2, 1),
                pltpu.roll(part, HD // 2, 1),
            )
        )
    return jnp.concatenate(out, axis=1)


def widen(table, width):
    return jnp.concatenate([table] * (width // 128), axis=1)


def cos_sin(angle):
    turns = jnp.round(angle * np.float32(2.0 / np.pi))
    left = angle - turns * np.float32(1.5703125)
    left = left - turns * np.float32(4.837512969970703125e-4)
    left = left - turns * np.float32(7.54978995489188e-8)
    sq = left * left
    sine = left + left * sq * (
        np.float32(-1.6666654611e-1)
        + sq * (np.float32(8.3321608736e-3) + sq * np.float32(-1.9515295891e-4))
    )
    cosine = (
        1.0
        - 0.5 * sq
        + sq
        * sq
        * (
            np.float32(4.166664568298827e-2)
            + sq * (np.float32(-1.388731625493765e-3) + sq * np.float32(2.443315711809948e-5))
        )
    )
    quarter = jnp.bitwise_and(turns.astype(jnp.int32), 3)
    odd = jnp.bitwise_and(quarter, 1) == 1
    sin_out = jnp.where(odd, cosine, sine)
    cos_out = jnp.where(odd, sine, cosine)
    sin_out = jnp.where(quarter >= 2, -sin_out, sin_out)
    cos_out = jnp.where((quarter == 1) | (quarter == 2), -cos_out, cos_out)
    return cos_out, sin_out


def normed(v):
    centered = v - jnp.mean(v, axis=1, keepdims=True)
    var = jnp.mean(centered * centered, axis=1, keepdims=True)
    rstd = lax.rsqrt(var + 1e-05)
    return centered * rstd, rstd


def fold8(v, op):
    return op(v.reshape(v.shape[0] // 8, 8, v.shape[1]), axis=0)


def pair_mask(kcol_ref, rows, codes):
    key = kcol_ref[rows, 0:1]
    low, high, same = codes
    return ((key >= low) & (key < high)) | (key == same)


def query_codes(qrow_ref, at, count):
    cols = pl.ds(at, count)
    return qrow_ref[0:1, cols], qrow_ref[1:2, cols], qrow_ref[2:3, cols]


SUB = 64


def attention_forward(arrays, plan, kcol, qrow, freq, wq, gain, heads, chunk):
    total = kcol.shape[0]
    blocks = total // chunk
    lq = wq.shape[1] // 3
    hw = heads * HD
    count = len(arrays)

    def kernel(*refs):
        x_refs = refs[:count]
        kcol_ref, qrow_ref, freq_ref, wq_ref, gain_ref = refs[count : count + 5]
        outs = refs[count + 5 :]
        h1_ref, q_ref, k_ref, v_ref, cs_ref, sn_ref, att_t_ref, lse_ref = outs[:8]
        att_refs = outs[8 : 8 + blocks]
        vt_scr, s_scr, p_scr = outs[8 + blocks :]
        step = pl.program_id(0)

        @pl.when(step == 0)
        def _():
            gain_row = gain_ref[...]
            for which, src, dst, rows in plan:
                for at, size in cuts(rows, 64):
                    xhat, _ = normed(x_refs[which][src + at : src + at + size, :].astype(F32))
                    h1_ref[dst + at : dst + at + size, :] = (xhat * gain_row).astype(BF)
            lanes = lax.broadcasted_iota(jnp.int32, (1, 128), 1)
            sign = jnp.where(lanes % HD < HD // 2, -1.0, 1.0)

            def project(block, carry):
                rows = pl.ds(pl.multiple_of(block * chunk, chunk), chunk)
                cosine, sine = cos_sin(kcol_ref[rows, 1:2] * freq_ref[...])
                sine = sine * sign
                cs_ref[rows, :] = cosine
                sn_ref[rows, :] = sine
                cosine = widen(cosine, lq)
                sine = widen(sine, lq)
                made = dot(h1_ref[rows, :], wq_ref[...])
                q = made[:, :lq]
                q_ref[rows, :] = ((q * cosine + swap_halves(q) * sine).astype(BF) * 0.125).astype(
                    BF
                )
                k = made[:, lq : 2 * lq]
                k_ref[rows, :] = (k * cosine + swap_halves(k) * sine).astype(BF)
                v = made[:, 2 * lq :]
                v_ref[rows, :] = v.astype(BF)
                vt_scr[:, rows] = v.T.astype(BF)
                return carry

            lax.fori_loop(0, blocks, project, 0)

        at = pl.multiple_of(step * chunk, chunk)
        codes = query_codes(qrow_ref, at, chunk)
        query = per_head(q_ref[pl.ds(at, chunk), :], heads)

        def score(block, best):
            base = pl.multiple_of(block * chunk, chunk)
            s_scr[pl.ds(base, chunk), :] = dot_t(k_ref[pl.ds(base, chunk), :], query)
            best = list(best)
            for sub in range(0, chunk, SUB):
                rows = pl.ds(base + sub, SUB)
                mask = pair_mask(kcol_ref, rows, codes)
                for h in range(heads):
                    cols = slice(h * chunk, (h + 1) * chunk)
                    value = jnp.where(mask, s_scr[rows, cols], NEG)
                    s_scr[rows, cols] = value
                    best[h] = jnp.maximum(best[h], fold8(value, jnp.max))
            return tuple(best)

        best = lax.fori_loop(
            0, blocks, score, tuple(jnp.full((8, chunk), NEG, F32) for _ in range(heads))
        )
        best = [jnp.max(b, axis=0, keepdims=True) for b in best]

        def soften(block, sums):
            base = pl.multiple_of(block * chunk, chunk)
            sums = list(sums)
            for sub in range(0, chunk, SUB):
                rows = pl.ds(base + sub, SUB)
                for h in range(heads):
                    cols = slice(h * chunk, (h + 1) * chunk)
                    value = jnp.exp(s_scr[rows, cols] - best[h])
                    sums[h] = sums[h] + fold8(value, jnp.sum)
                    p_scr[rows, cols] = value.astype(BF)
            return tuple(sums)

        sums = lax.fori_loop(
            0, blocks, soften, tuple(jnp.zeros((8, chunk), F32) for _ in range(heads))
        )
        sums = [jnp.sum(s, axis=0, keepdims=True) for s in sums]
        tops = []
        for h in range(heads):
            made = dot(vt_scr[...], p_scr[:, h * chunk : (h + 1) * chunk])
            tops.append(made[h * HD : (h + 1) * HD, :] * (1.0 / sums[h]))
        if hw < lq:
            tops.append(jnp.zeros((lq - hw, chunk), F32))
        joined = jnp.concatenate(tops, axis=0)
        att_t_ref[0] = joined
        lse_rows = [best[h] + jnp.log(sums[h]) for h in range(heads)]
        lse_rows.append(jnp.zeros((8 - heads, chunk), F32))
        lse_ref[0] = jnp.concatenate(lse_rows, axis=0)
        attended = joined.T[:, :hw].astype(BF)
        for b in range(blocks):

            @pl.when(step == b)
            def _(b=b):
                att_refs[b][...] = attended

    ins = list(arrays) + [kcol, qrow, freq, wq, gain]
    shapes = [
        ((total, D), BF),
        ((total, lq), BF),
        ((total, lq), BF),
        ((total, lq), BF),
        ((total, 128), F32),
        ((total, 128), F32),
    ]
    out_shape = [jax.ShapeDtypeStruct(*s) for s in shapes]
    out_specs = [whole(s[0]) for s in shapes]
    out_shape.append(jax.ShapeDtypeStruct((blocks, lq, chunk), F32))
    out_specs.append(pl.BlockSpec((1, lq, chunk), lambda i: (i, 0, 0)))
    out_shape.append(jax.ShapeDtypeStruct((blocks, 8, chunk), F32))
    out_specs.append(pl.BlockSpec((1, 8, chunk), lambda i: (i, 0, 0)))
    for _ in range(blocks):
        out_shape.append(jax.ShapeDtypeStruct((chunk, hw), BF))
        out_specs.append(whole((chunk, hw)))
    made = pl.pallas_call(
        kernel,
        name="attention_forward",
        grid=(blocks,),
        in_specs=[whole(v.shape) for v in ins],
        out_specs=out_specs,
        out_shape=out_shape,
        scratch_shapes=[
            pltpu.VMEM((lq, total), BF),
            pltpu.VMEM((total, heads * chunk), F32),
            pltpu.VMEM((total, heads * chunk), BF),
        ],
        compiler_params=params("arbitrary"),
        cost_estimate=cost(8e9, 8e6),
    )(*ins)
    return made[:8], made[8:]


def attention_backward(pulls, saved, kcol, qrow, wq, heads, chunk):
    _, q, k, v, cs, sn, att_t, lse = saved
    total = kcol.shape[0]
    blocks = total // chunk
    lq = wq.shape[1] // 3
    hw = heads * HD

    def kernel(*refs):
        g_refs = refs[:blocks]
        q_ref, k_ref, v_ref, cs_ref, sn_ref, att_t_ref, lse_ref, kcol_ref, qrow_ref, wq_ref = refs[
            blocks : blocks + 10
        ]
        outs = refs[blocks + 10 :]
        gqkv_ref = outs[0]
        gh_refs = outs[1 : 1 + blocks]
        g_scr, kt_scr, dk_scr, dv_scr, s_scr, dp_scr, pb_scr, ds_scr, dst_scr = outs[1 + blocks :]
        step = pl.program_id(0)

        @pl.when(step == 0)
        def _():
            for b in range(blocks):
                rows = slice(b * chunk, (b + 1) * chunk)
                g_scr[rows, :hw] = g_refs[b][...]
                if hw < lq:
                    g_scr[rows, hw:] = jnp.zeros((chunk, lq - hw), BF)
            dk_scr[...] = jnp.zeros_like(dk_scr)
            dv_scr[...] = jnp.zeros_like(dv_scr)

            def turn(block, carry):
                rows = pl.ds(pl.multiple_of(block * chunk, chunk), chunk)
                for h in range(heads):
                    part = k_ref[rows, :] * lane_mask(lq, h)
                    kt_scr[block, :, h * chunk : (h + 1) * chunk] = part.astype(F32).T.astype(BF)
                return carry

            lax.fori_loop(0, blocks, turn, 0)

        at = pl.multiple_of(step * chunk, chunk)
        own = pl.ds(at, chunk)
        codes = query_codes(qrow_ref, at, chunk)
        query = per_head(q_ref[own, :], heads)
        pull = g_scr[own, :]
        product = pull.astype(F32).T * att_t_ref[0]
        delta = [
            jnp.sum(product[h * HD : (h + 1) * HD, :], axis=0, keepdims=True) for h in range(heads)
        ]
        top = [lse_ref[0, h : h + 1, :] for h in range(heads)]
        pull = per_head(pull, heads)

        def keys(block, dq_t):
            base = pl.multiple_of(block * chunk, chunk)
            rows = pl.ds(base, chunk)
            s_scr[...] = dot_t(k_ref[rows, :], query)
            dp_scr[...] = dot_t(v_ref[rows, :], pull)
            for sub in range(0, chunk, SUB):
                part = slice(sub, sub + SUB)
                mask = pair_mask(kcol_ref, pl.ds(base + sub, SUB), codes)
                for h in range(heads):
                    cols = slice(h * chunk, (h + 1) * chunk)
                    prob = jnp.exp(jnp.where(mask, s_scr[part, cols] - top[h], NEG))
                    slope = (prob * (dp_scr[part, cols] - delta[h])).astype(BF)
                    pb_scr[part, cols] = prob.astype(BF)
                    ds_scr[part, cols] = slope
                    dst_scr[h * chunk + sub : h * chunk + sub + SUB, :] = slope
            dv_scr[rows, :] += dot(pb_scr[...], pull)
            dk_scr[rows, :] += dot(ds_scr[...], query)
            return dq_t + dot(kt_scr[block], dst_scr[...])

        dq_t = lax.fori_loop(0, blocks, keys, jnp.zeros((lq, chunk), F32))

        def unrotate(value, rows):
            return value * widen(cs_ref[rows, :], lq) - swap_halves(value) * widen(
                sn_ref[rows, :], lq
            )

        gqkv_ref[own, :lq] = unrotate(dq_t.T * 0.125, own).astype(BF)

        @pl.when(step == blocks - 1)
        def _():
            for b in range(blocks):
                rows = slice(b * chunk, (b + 1) * chunk)
                gqkv_ref[rows, lq : 2 * lq] = unrotate(dk_scr[rows, :], rows).astype(BF)
                gqkv_ref[rows, 2 * lq :] = dv_scr[rows, :].astype(BF)
                gh_refs[b][...] = dot_t(gqkv_ref[rows, :], wq_ref[...]).astype(gh_refs[b].dtype)

    ins = list(pulls) + [q, k, v, cs, sn, att_t, lse, kcol, qrow, wq]
    in_specs = [whole(a.shape) for a in ins]
    in_specs[blocks + 5] = pl.BlockSpec((1, lq, chunk), lambda i: (i, 0, 0))
    in_specs[blocks + 6] = pl.BlockSpec((1, 8, chunk), lambda i: (i, 0, 0))
    out_shape = [jax.ShapeDtypeStruct((total, 3 * lq), BF)]
    for b in range(blocks):
        out_shape.append(jax.ShapeDtypeStruct((chunk, D), F32 if b == 0 else BF))
    made = pl.pallas_call(
        kernel,
        name="attention_backward",
        grid=(blocks,),
        in_specs=in_specs,
        out_specs=[whole(o.shape) for o in out_shape],
        out_shape=out_shape,
        scratch_shapes=[
            pltpu.VMEM((total, lq), BF),
            pltpu.VMEM((blocks, lq, heads * chunk), BF),
            pltpu.VMEM((total, lq), F32),
            pltpu.VMEM((total, lq), F32),
            pltpu.VMEM((chunk, heads * chunk), F32),
            pltpu.VMEM((chunk, heads * chunk), F32),
            pltpu.VMEM((chunk, heads * chunk), BF),
            pltpu.VMEM((chunk, heads * chunk), BF),
            pltpu.VMEM((heads * chunk, chunk), BF),
        ],
        compiler_params=params("arbitrary"),
        cost_estimate=cost(1.2e10, 1e7),
    )(*ins)
    return made[0], made[1:]


def output_projection(place, mixed, wout, x, gain):
    groups = len(mixed)
    rows = x.shape[0]

    def kernel(place_ref, *refs):
        m_refs = refs[:groups]
        w_ref, x_ref, gain_ref, res_ref, h2_ref = refs[groups:]
        z = place_ref[1]
        total = x_ref[...].astype(F32)
        for k in range(groups):
            total = total + dot(m_refs[k][...], w_ref[lax.rem(z + (groups - k), groups)])
        res_ref[...] = total
        for at, size in cuts(rows, 64):
            xhat, _ = normed(res_ref[at : at + size, :])
            h2_ref[at : at + size, :] = (xhat * gain_ref[...]).astype(BF)

    ins = list(mixed) + [wout, x, gain]
    return pl.pallas_call(
        kernel,
        name="output_projection",
        grid_spec=pltpu.PrefetchScalarGridSpec(
            num_scalar_prefetch=1,
            grid=(1,),
            in_specs=[whole(a.shape) for a in ins],
            out_specs=[whole((rows, D)), whole((rows, D))],
        ),
        out_shape=[jax.ShapeDtypeStruct((rows, D), F32), jax.ShapeDtypeStruct((rows, D), BF)],
        compiler_params=params("arbitrary"),
        cost_estimate=cost(1e9, 3e6),
    )(place, *ins)


def feed_forward(place, h2_own, h2_other, dy_own, dy_other, w1, w2a, w2b, bias):
    rows = h2_own.shape[0]
    both = 2 * rows
    width = 384

    def kernel(
        place_ref, ho_ref, hp_ref, go_ref, gp_ref, w1_ref, w2a_ref, w2b_ref, b_ref,
        out_own, out_other, gh_own, gh_other, dw1_ref, dw2a_ref, dw2b_ref, db_ref,
        h_scr, g_scr, ht_scr, gt_scr, w1_scr, w2_scr, pre_scr, ga_scr, act_scr, slope_scr, out_scr,
        gh_scr,
    ):
        step = pl.program_id(0)
        d = place_ref[0]
        z = place_ref[1]

        @pl.when(step == 0)
        def _():
            h_scr[:rows, :] = ho_ref[...]
            h_scr[rows:, :] = hp_ref[...]
            g_scr[:rows, :] = go_ref[...]
            g_scr[rows:, :] = gp_ref[...]
            for at in range(0, both, 256):
                part = slice(at, at + 256)
                ht_scr[:, part] = h_scr[part, :].astype(F32).T.astype(BF)
                gt_scr[:, part] = g_scr[part, :].astype(F32).T.astype(BF)

        for j in range(4):
            m = d ^ j
            w1_scr[192 * j : 192 * j + 192, :] = w1_ref[0, m // 2, m % 2]
            k = lax.rem(j - z + 4, 4)
            w2_scr[192 * j : 192 * j + 96, :] = w2a_ref[0, 0, k]
            w2_scr[192 * j + 96 : 192 * j + 192, :] = w2b_ref[0, 0, k]
        pre_scr[...] = dot(h_scr[...], w1_scr[...])
        ga_scr[...] = dot(g_scr[...], w2_scr[...])
        bias_row = b_ref[0].astype(F32)
        total = jnp.zeros((8, width), F32)
        for at in range(0, both, 32):
            part = slice(at, at + 32)
            u = pre_scr[part, :] + bias_row
            usq = u * u
            c = np.float32(np.sqrt(2.0 / np.pi))
            t = jnp.tanh(c * (u + np.float32(0.044715) * (usq * u)))
            half = 0.5 * (1.0 + t)
            act_scr[part, :] = (u * half).astype(BF)
            rise = half + 0.5 * u * (1.0 - t * t) * (c * (1.0 + np.float32(0.134145) * usq))
            slope = (ga_scr[part, :] * rise).astype(BF)
            slope_scr[part, :] = slope
            total = total + fold8(slope.astype(F32), jnp.sum)
        db_ref[0] = total

        out_now = dot_t(act_scr[...], w2_scr[...])
        gh_now = dot_t(slope_scr[...], w1_scr[...])

        @pl.when(step == 0)
        def _():
            out_scr[...] = out_now
            gh_scr[...] = gh_now

        @pl.when(step > 0)
        def _():
            out_scr[...] += out_now
            gh_scr[...] += gh_now

        dw1 = dot(ht_scr[...], slope_scr[...]).astype(BF)
        dw2 = dot(gt_scr[...], act_scr[...]).astype(BF)
        for j in range(4):
            m = d ^ j
            dw1_ref[0, m // 2, m % 2] = dw1[192 * j : 192 * j + 192, :]
            k = lax.rem(j - z + 4, 4)
            dw2a_ref[0, 0, k] = dw2[192 * j : 192 * j + 96, :]
            dw2b_ref[0, 0, k] = dw2[192 * j + 96 : 192 * j + 192, :]

        @pl.when(step == 3)
        def _():
            out_own[...] = out_scr[:rows, :]
            out_other[...] = out_scr[rows:, :].astype(BF)
            gh_own[...] = gh_scr[:rows, :]
            gh_other[...] = gh_scr[rows:, :].astype(BF)

    def by_z(i, place_ref):
        return lax.rem(i - place_ref[1] + 4, 4)

    def one_spec(i, place_ref):
        return (by_z(i, place_ref), 0, 0, 0, 0)

    def a_spec(i, place_ref):
        m = i ^ place_ref[0]
        return (m % 2, m // 2, 0, 0, 0)

    def b_spec(i, place_ref):
        m = i ^ place_ref[0]
        return (m // 2, m % 2, 0, 0, 0)

    ins = [h2_own, h2_other, dy_own, dy_other]
    in_specs = [whole(a.shape) for a in ins] + [
        pl.BlockSpec((1, 2, 2, 192, width), one_spec),
        pl.BlockSpec((1, 1, 4, 96, width), a_spec),
        pl.BlockSpec((1, 1, 4, 96, width), b_spec),
        pl.BlockSpec((1, 1, width), lambda i, p: (by_z(i, p), 0, 0)),
    ]
    out_shape = [
        jax.ShapeDtypeStruct((rows, D), F32),
        jax.ShapeDtypeStruct((rows, D), BF),
        jax.ShapeDtypeStruct((rows, D), F32),
        jax.ShapeDtypeStruct((rows, D), BF),
        jax.ShapeDtypeStruct((4, 2, 2, 192, width), BF),
        jax.ShapeDtypeStruct((2, 2, 4, 96, width), BF),
        jax.ShapeDtypeStruct((2, 2, 4, 96, width), BF),
        jax.ShapeDtypeStruct((4, 8, width), F32),
    ]
    out_specs = [whole((rows, D))] * 4 + [
        pl.BlockSpec((1, 2, 2, 192, width), one_spec),
        pl.BlockSpec((1, 1, 4, 96, width), a_spec),
        pl.BlockSpec((1, 1, 4, 96, width), b_spec),
        pl.BlockSpec((1, 8, width), lambda i, p: (by_z(i, p), 0, 0)),
    ]
    return pl.pallas_call(
        kernel,
        name="feed_forward",
        grid_spec=pltpu.PrefetchScalarGridSpec(
            num_scalar_prefetch=1,
            grid=(4,),
            in_specs=in_specs,
            out_specs=out_specs,
            scratch_shapes=[
                pltpu.VMEM((both, D), BF),
                pltpu.VMEM((both, D), BF),
                pltpu.VMEM((D, both), BF),
                pltpu.VMEM((D, both), BF),
                pltpu.VMEM((D, width), BF),
                pltpu.VMEM((D, width), BF),
                pltpu.VMEM((both, width), F32),
                pltpu.VMEM((both, width), F32),
                pltpu.VMEM((both, width), BF),
                pltpu.VMEM((both, width), BF),
                pltpu.VMEM((both, D), F32),
                pltpu.VMEM((both, D), F32),
            ],
        ),
        out_shape=out_shape,
        compiler_params=params("arbitrary"),
        cost_estimate=cost(7.2e9, 1.5e7),
    )(place, *ins, w1, w2a, w2b, bias)


def residual_backward(place, gh_own, gh_in, residual, dy, gain, wout):
    rows = dy.shape[0]
    groups, hw = wout.shape[0], wout.shape[1]

    def kernel(place_ref, gh_ref, gi_ref, res_ref, dy_ref, gain_ref, w_ref, *outs):
        gres_ref, gproj_ref, vec_ref = outs[:3]
        gm_refs = outs[3:]
        z = place_ref[1]
        gain_row = gain_ref[...]
        gsum = jnp.zeros((8, D), F32)
        bsum = jnp.zeros((8, D), F32)
        for at, size in cuts(rows, 32):
            part = slice(at, at + size)
            xhat, rstd = normed(res_ref[part, :])
            dy_now = dy_ref[part, :].astype(F32)
            grad = gh_ref[part, :] + gi_ref[part, :].astype(F32)
            along = grad * xhat
            gsum = gsum + fold8(along, jnp.sum)
            bsum = bsum + fold8(dy_now, jnp.sum)
            u = grad * gain_row
            back = (
                u
                - jnp.mean(u, axis=1, keepdims=True)
                - xhat * jnp.mean(along * gain_row, axis=1, keepdims=True)
            )
            value = dy_now + back * rstd
            gres_ref[part, :] = value
            gproj_ref[part, :] = value.astype(BF)
        vec_ref[0:8, :] = gsum
        vec_ref[8:16, :] = bsum
        for k in range(groups):
            gm_refs[k][...] = dot_t(gproj_ref[...], w_ref[lax.rem(z + k, groups)]).astype(BF)

    ins = [gh_own, gh_in, residual, dy, gain, wout]
    out_shape = [
        jax.ShapeDtypeStruct((rows, D), F32),
        jax.ShapeDtypeStruct((rows, D), BF),
        jax.ShapeDtypeStruct((16, D), F32),
    ] + [jax.ShapeDtypeStruct((rows, hw), BF) for _ in range(groups)]
    made = pl.pallas_call(
        kernel,
        name="residual_backward",
        grid_spec=pltpu.PrefetchScalarGridSpec(
            num_scalar_prefetch=1,
            grid=(1,),
            in_specs=[whole(a.shape) for a in ins],
            out_specs=[whole(o.shape) for o in out_shape],
        ),
        out_shape=out_shape,
        compiler_params=params("arbitrary"),
        cost_estimate=cost(1e9, 4e6),
    )(place, *ins)
    return made[0], made[1], made[2], made[3:]


def input_backward(terms, x, gain, gres):
    rows = x.shape[0]
    count = len(terms)

    def kernel(*refs):
        x_ref, gain_ref, gres_ref, out_ref = refs[count:]
        for at, size in cuts(rows, 32):
            part = slice(at, at + size)
            grad = refs[0][part, :].astype(F32)
            for t in range(1, count):
                grad = grad + refs[t][part, :].astype(F32)
            xhat, rstd = normed(x_ref[part, :].astype(F32))
            u = grad * gain_ref[...]
            back = (
                u
                - jnp.mean(u, axis=1, keepdims=True)
                - xhat * jnp.mean(u * xhat, axis=1, keepdims=True)
            )
            out_ref[part, :] = (gres_ref[part, :] + back * rstd).astype(BF)

    ins = list(terms) + [x, gain, gres]
    return pl.pallas_call(
        kernel,
        name="input_backward",
        grid=(1,),
        in_specs=[whole(a.shape) for a in ins],
        out_specs=whole((rows, D)),
        out_shape=jax.ShapeDtypeStruct((rows, D), BF),
        compiler_params=params("arbitrary"),
        cost_estimate=cost(1e8, 3e6),
    )(*ins)


def add_low(a, b):
    return (a.astype(F32) + b.astype(F32)).astype(BF)


def pick(v, index):
    return lax.dynamic_index_in_dim(v, index, 0, keepdims=False)


class Links:
    def __init__(self, n_dp, n_seq):
        self.n_dp, self.n_seq, self.nz = n_dp, n_seq, n_seq // 2

    def core(self, v):
        return lax.ppermute(v, "seq", [(s, s ^ 1) for s in range(self.n_seq)])

    def flip(self, v, bit):
        return lax.ppermute(v, "dp", [(i, i ^ bit) for i in range(self.n_dp)])

    def shift(self, v, k):
        n = self.nz
        return lax.ppermute(
            v, "seq", [(s, 2 * ((s // 2 + k) % n) + s % 2) for s in range(self.n_seq)]
        )

    def gather_z(self, v, split):
        rows = v.shape[0]
        if self.nz != 4:
            return [[v]] + [[self.shift(v, -k)] for k in range(1, self.nz)]
        before = self.shift(v, 1)
        after = self.shift(v, -1)
        low = self.shift(before[:split], 1)
        high = self.shift(after[split:rows], -1)
        return [[v], [after], [low, high], [before]]

    def scatter_z(self, blocks, split):
        if self.nz != 4:
            return [blocks[0]] + [self.shift(blocks[k], k) for k in range(1, self.nz)]
        low = self.shift(blocks[2][:split], 1)
        high = self.shift(blocks[2][split:], -1)
        up = jnp.concatenate([add_low(blocks[1][:split], low), blocks[1][split:]], axis=0)
        down = jnp.concatenate([blocks[3][:split], add_low(blocks[3][split:], high)], axis=0)
        return [blocks[0], self.shift(up, 1), self.shift(down, -1)]

    def swap_z(self, blocks):
        return [blocks[0]] + [self.shift(blocks[k], k) for k in range(1, self.nz)]


def xor_order(v, index):
    return jnp.stack([pick(v, index ^ j) for j in range(v.shape[0])])


def per_device(
    n_dp,
    n_seq,
    inputs,
    row_segment,
    row_flag,
    row_block,
    norm1_scale,
    w_qkv,
    w_out,
    norm2_scale,
    w_fc1,
    b_fc1,
    w_fc2,
    b_fc2,
    cotangent,
):
    links = Links(n_dp, n_seq)
    nz = links.nz
    local = inputs.shape[2]
    chunk = 2 * local
    heads = -(-H // nz)
    hw = heads * HD
    lq = -(-hw // 128) * 128
    fast = n_dp == 4 and nz == 4 and H % nz == 0
    d = lax.axis_index("dp")
    s = lax.axis_index("seq")
    z = s // 2
    c = s % 2
    zero = jnp.zeros((), jnp.int32)
    place = jnp.stack([d, z]).astype(jnp.int32)
    own_c = n1_w = D // n_seq
    b1_w = FF // n_seq

    x_loc = inputs[:, 0]
    x_keep = pick(x_loc, c)
    labels = jnp.stack([row_segment[:, 0], row_flag[:, 0], row_block[:, 0]], axis=1)
    labels = labels.astype(BF).reshape(2, 3 * local)
    vector = jnp.concatenate([norm1_scale, norm2_scale, b_fc2, b_fc1]).astype(BF)
    vector = jnp.pad(vector, (0, D - vector.shape[0]))
    lab_keep, lab_send = pick(labels, c), pick(labels, 1 - c)
    extra = jnp.stack([jnp.pad(lab_send, (0, D - 3 * local)), vector])
    message = jnp.concatenate([pick(x_loc, 1 - c), jnp.pad(extra, ((0, 14), (0, 0)))], axis=0)
    swapped = links.core(message)
    extra = jnp.stack(
        [
            jnp.concatenate([lab_keep, swapped[local, : 3 * local]]),
            vector,
            swapped[local + 1],
        ]
    )
    x_own = jnp.concatenate([x_keep, swapped[:local]], axis=0)
    x_ext = jnp.concatenate([x_own, jnp.pad(extra, ((0, 13), (0, 0)))], axis=0)
    gathered = links.gather_z(x_ext, 144)

    cot = cotangent[:, 0]
    cot_in = links.core(cot)
    dy_own = jnp.concatenate([pick(cot, c), pick(cot_in, c)], axis=0)
    dy_other = jnp.concatenate([pick(cot_in, 1 - c), pick(cot, 1 - c)], axis=0)

    arrays, plan, extras = [], [], []
    for k, pieces in enumerate(gathered):
        at = 0
        for piece in pieces:
            rows = min(piece.shape[0], chunk - at)
            plan.append((len(arrays), 0, k * chunk + at, rows))
            at += rows
            arrays.append(piece)
        extras.append(pieces[-1][-16:])
    extras = jnp.stack(extras)
    labels_all = extras[:, 0].astype(F32).reshape(nz, 2, 3, local)
    segment = labels_all[:, :, 0].reshape(-1)
    flag = labels_all[:, :, 1].reshape(-1)
    block = labels_all[:, :, 2].reshape(-1)
    total = segment.shape[0]
    start = segment * 4096.0
    key_code = start + jnp.where(flag > 0.5, block, block + 2048.0)
    low = start
    high = start + block + flag
    same = jnp.where(flag > 0.5, -1.0, key_code)
    position = block * BLK + (jnp.arange(total, dtype=jnp.int32) % BLK).astype(F32)
    qrow = jnp.pad(jnp.stack([low, high, same]), ((0, 5), (0, 0)))
    kcol = jnp.pad(jnp.stack([key_code, position], axis=1), ((0, 0), (0, 6)))
    freq = np.tile(
        np.float32(10000.0) ** (np.float32(-2.0) * np.arange(32, dtype=np.float32) / HD), 4
    )
    freq = jnp.asarray(freq.astype(np.float32)[None, :])
    vectors = extras[:, 1:3]
    bias_rel = vectors[:, 0, 3 * n1_w : 3 * n1_w + b1_w]
    vectors = jnp.roll(jnp.where(c == 0, vectors, vectors[:, ::-1]), z, axis=0)
    gain_one = vectors[:, :, :n1_w].reshape(1, D).astype(F32)
    gain_two = vectors[:, :, n1_w : 2 * n1_w].reshape(1, D).astype(F32)
    bias_two = vectors[:, :, 2 * n1_w : 3 * n1_w].reshape(1, D).astype(F32)

    if fast:
        wq_parts = w_qkv.astype(BF)
        parts = []
        for i in range(3):
            parts.append(
                lax.ppermute(
                    wq_parts[:, 96 * i : 96 * i + 96],
                    "seq",
                    [(q, (3 * q + i) % 8) for q in range(8)],
                )
            )
        parts = jnp.stack(parts)
        wq_own = jnp.concatenate([pick(parts, (2 * t + s) % 3) for t in range(3)], axis=1)
        for bit in (2, 1):
            wq_own = jnp.stack([wq_own, links.flip(wq_own, bit)])
        wq_own = wq_own.swapaxes(0, 1)
        wq_in = links.core(wq_own)

        def both_parities(own, other):
            return jnp.where(
                c == 0, jnp.stack([own, other], axis=-2), jnp.stack([other, own], axis=-2)
            )

        wq = both_parities(
            wq_own.reshape(4, 192, 3, 96), wq_in.reshape(4, 192, 3, 96)
        ).reshape(4, 192, 3, hw)
        wq = xor_order(jnp.pad(wq, ((0, 0), (0, 0), (0, 0), (0, lq - hw))), d).reshape(D, 3 * lq)

        one = jnp.concatenate([w_fc1.astype(BF), w_out.astype(BF)], axis=1)
        for bit in (1, 2):
            one = jnp.stack([one, links.flip(one, bit)])
        one = [jnp.concatenate(p, axis=0) for p in links.gather_z(one, 1)]
        w1 = jnp.stack(one)
        wo_own = w1[..., 384:].reshape(4, 4, 192, 96)
        wo_in = links.core(wo_own)
        wout = both_parities(wo_own, wo_in)
        wout = jnp.roll(wout, z, axis=0).transpose(1, 2, 0, 3, 4).reshape(4, 192, D)
        wout = xor_order(wout, d)

        two = w_fc2.astype(BF).T.reshape(96, 2, 384)
        two_keep = jnp.where(c == 0, two[:, 0], two[:, 1])
        two_in = links.core(jnp.where(c == 0, two[:, 1], two[:, 0]))
        two = jnp.where(c == 0, jnp.stack([two_keep, two_in]), jnp.stack([two_in, two_keep]))
        two = jnp.stack([jnp.concatenate(p, axis=0) for p in links.gather_z(two, 1)])
        w2a, w2b = two[:, 0], two[:, 1]
        for bit in (2, 1):
            w2a = jnp.stack([w2a, links.flip(w2a, bit)])
        for bit in (1, 2):
            w2b = jnp.stack([w2b, links.flip(w2b, bit)])
        bias_one = bias_rel.reshape(4, 1, 384)
        ff_place = place
    else:

        def everywhere(w):
            w = lax.all_gather(w.astype(BF), "seq", axis=1, tiled=True)
            return lax.all_gather(w, "dp", axis=0, tiled=True)

        wq = everywhere(w_qkv).reshape(D, 3, D)
        wq = jnp.pad(wq, ((0, 0), (0, 0), (0, nz * hw - D)))
        wq = lax.dynamic_slice_in_dim(wq, z * hw, hw, 2)
        wq = jnp.pad(wq, ((0, 0), (0, 0), (0, lq - hw))).reshape(D, 3 * lq)
        wout = jnp.pad(everywhere(w_out), ((0, nz * hw - D), (0, 0))).reshape(nz, hw, D)
        w1 = lax.dynamic_slice_in_dim(everywhere(w_fc1), c * (FF // 2), FF // 2, 1)
        w1 = w1.reshape(2, 2, 192, 4, 384).transpose(3, 0, 1, 2, 4)
        w2 = lax.dynamic_slice_in_dim(everywhere(w_fc2), c * (FF // 2), FF // 2, 0)
        w2 = w2.reshape(2, 2, 384, 4, 2, 96).transpose(4, 0, 1, 3, 5, 2)
        w2a, w2b = w2[0].swapaxes(0, 1), w2[1]
        bias_all = vectors[:, :, 3 * n1_w : 3 * n1_w + b1_w].reshape(FF)
        bias_one = lax.dynamic_slice_in_dim(bias_all, c * (FF // 2), FF // 2, 0).reshape(4, 1, 384)
        ff_place = jnp.zeros((2,), jnp.int32)

    saved, attended = attention_forward(
        arrays, plan, kcol, qrow, freq, wq, gain_one, heads, chunk
    )
    mixed = links.swap_z(attended)
    residual, h2 = output_projection(place, mixed, wout, x_own, gain_two)
    h2_in = links.core(h2)
    (out_own, out_other, gh_own, gh_other, dw1, dw2a, dw2b, db1) = feed_forward(
        ff_place, h2, h2_in, dy_own, dy_other, w1, w2a, w2b, bias_one
    )
    gh_in = links.core(gh_other)
    gres, gproj, sums, gmixed = residual_backward(
        place, gh_own, gh_in, residual, dy_own, gain_two, wout
    )
    pulled = links.swap_z(gmixed)
    pulled = [pulled[(nz - k) % nz] for k in range(nz)]
    gqkv, gh1 = attention_backward(pulled, saved, kcol, qrow, wq, heads, chunk)
    terms = links.scatter_z(list(gh1), local)
    grad_rows = input_backward(terms, x_own, gain_one, gres)
    grad_in = links.core(grad_rows[local:])
    out_in = links.core(out_other)
    out_rows = (residual + out_own + out_in.astype(F32) + bias_two).astype(BF)
    rows_in = links.core(out_rows[local:])

    def by_micro(own, other):
        return jnp.where(c == 0, jnp.stack([own, other]), jnp.stack([other, own]))[:, None]

    outputs = by_micro(out_rows[:local], rows_in)
    input_grad = by_micro(grad_rows[:local], grad_in)

    dwq = jnp.einsum("rd,rj->dj", saved[0], gqkv, preferred_element_type=F32)
    grad_gain_one = jnp.sum(dwq * wq.astype(F32), axis=1) / gain_one[0]
    grad_gain_two = jnp.sum(sums[:8], axis=0)
    grad_bias_two = jnp.sum(sums[8:], axis=0)
    grad_bias_one = jnp.sum(db1, axis=1)
    mixed_all = jnp.concatenate(mixed, axis=1)
    dwo = jnp.einsum("ri,ro->io", mixed_all, gproj, preferred_element_type=F32)

    if fast:
        for bit in (1, 2):
            dw2a = add_low(dw2a[0], links.flip(dw2a[1], bit))
        for bit in (2, 1):
            dw2b = add_low(dw2b[0], links.flip(dw2b[1], bit))
        dw2 = jnp.stack([dw2a, dw2b], axis=1)
        dw2 = sum(t.astype(F32) for t in links.scatter_z([dw2[k] for k in range(4)], 1))
        keep = jnp.where(c == 0, dw2[0], dw2[1])
        came = links.core(jnp.where(c == 0, dw2[1], dw2[0]))
        g_fc2 = jnp.where(
            c == 0,
            jnp.concatenate([keep, came], axis=1),
            jnp.concatenate([came, keep], axis=1),
        ).T
        dw1 = links.scatter_z([dw1[k] for k in range(4)], 1)
        dw1 = sum(t.astype(F32) for t in dw1).astype(BF)
        dw1 = add_low(dw1[:, 0], links.flip(dw1[:, 1], 1))
        g_fc1 = dw1[0].astype(F32) + links.flip(dw1[1], 2).astype(F32)
        dwo = dwo.astype(BF).reshape(4, 192, 4, 2, 96)
        dwo = jnp.stack([pick(dwo, lax.rem(z - (d ^ j) + 4, 4)) for j in range(4)])
        dwo = jnp.roll(dwo, -z, axis=2)
        keep = jnp.where(c == 0, dwo[..., 0, :], dwo[..., 1, :])
        came = links.core(jnp.where(c == 0, dwo[..., 1, :], dwo[..., 0, :]))
        dwo = add_low(keep, came)
        dwo = sum(t.astype(F32) for t in links.swap_z([dwo[:, :, k] for k in range(4)]))
        dwq = xor_order(dwq.astype(BF).reshape(4, 192, 3, lq)[..., :hw], d)
        dwq = dwq.reshape(4, 192, 3, 2, 96)
        keep = jnp.where(c == 0, dwq[..., 0, :], dwq[..., 1, :])
        came = links.core(jnp.where(c == 0, dwq[..., 1, :], dwq[..., 0, :]))
        dwq = add_low(keep, came).reshape(4, 192, 288)
        joint = jnp.concatenate([dwq, dwo.astype(BF)], axis=2).reshape(2, 2, 192, 384)
        joint = add_low(joint[:, 0], links.flip(joint[:, 1], 1))
        joint = joint[0].astype(F32) + links.flip(joint[1], 2).astype(F32)
        g_out = joint[:, 288:]
        third = jnp.stack([joint[:, 96 * t : 96 * t + 96] for t in range(3)])
        g_qkv = jnp.concatenate(
            [
                lax.ppermute(
                    pick(third, lax.rem(2 * (i - s + 9), 3)),
                    "seq",
                    [((3 * q + i) % 8, q) for q in range(8)],
                )
                for i in range(3)
            ],
            axis=1,
        )
        three = jnp.stack([grad_gain_one, grad_gain_two, grad_bias_two]).reshape(3, 4, 2, 96)
        three = jnp.roll(three, -z, axis=1)
        keep = jnp.where(c == 0, three[:, :, 0], three[:, :, 1])
        came = links.core(jnp.where(c == 0, three[:, :, 1], three[:, :, 0]))
        three = (keep + came).transpose(1, 0, 2).reshape(4, 288)
        vec = jnp.concatenate([three, grad_bias_one, jnp.zeros((4, 352), F32)], axis=1)
        vec = vec.reshape(4, 8, 128)
        vec = sum(links.swap_z([vec[k] for k in range(4)]))
        for bit in (1, 2):
            vec = vec + links.flip(vec, bit)
        vec = vec.reshape(1024)
        vecs = (vec[:96], vec[96:192], vec[288:672], vec[192:288])
    else:

        def owned(w):
            w = lax.psum_scatter(w.astype(BF), "seq", scatter_dimension=1, tiled=True)
            return lax.psum_scatter(w, "dp", scatter_dimension=0, tiled=True).astype(F32)

        spread = jnp.zeros((D, 3, nz * hw), F32)
        spread = lax.dynamic_update_slice_in_dim(
            spread, dwq.reshape(D, 3, lq)[..., :hw], z * hw, 2
        )
        g_qkv = owned(spread[..., :D].reshape(D, 3 * D))
        dwo = dwo.reshape(nz, hw, D)
        dwo = jnp.roll(dwo[::-1], z + 1, axis=0).reshape(nz * hw, D)[:D]
        g_out = owned(dwo)
        half = dw1.transpose(1, 2, 3, 0, 4).reshape(D, FF // 2)
        full = lax.dynamic_update_slice_in_dim(
            jnp.zeros((D, FF), BF), half, c * (FF // 2), 1
        )
        g_fc1 = owned(full)
        half = jnp.stack([dw2a.swapaxes(0, 1), dw2b])
        half = half.transpose(1, 2, 5, 3, 0, 4).reshape(FF // 2, D)
        full = lax.dynamic_update_slice_in_dim(
            jnp.zeros((FF, D), BF), half, c * (FF // 2), 0
        )
        g_fc2 = owned(full)
        bias_full = lax.dynamic_update_slice_in_dim(
            jnp.zeros((FF,), F32), grad_bias_one.reshape(-1), c * (FF // 2), 0
        )
        vecs = tuple(
            lax.psum(lax.psum_scatter(v, "seq", scatter_dimension=0, tiled=True), "dp")
            for v in (grad_gain_one, grad_gain_two, bias_full, grad_bias_two)
        )

    return (
        outputs,
        input_grad,
        vecs[0],
        g_qkv,
        g_out,
        vecs[1],
        g_fc1,
        vecs[2],
        g_fc2,
        vecs[3],
    )


def solution(mesh):
    rows = P(None, "dp", "seq", None)
    labels = P(None, "dp", "seq")
    matrix = P("dp", "seq")
    vector = P("seq")
    return jax.shard_map(
        functools.partial(per_device, mesh.shape["dp"], mesh.shape["seq"]),
        mesh=mesh,
        in_specs=(
            rows, labels, labels, labels, vector, matrix, matrix, vector, matrix, vector, matrix,
            vector, rows,
        ),
        out_specs=(
            rows, rows, vector, matrix, matrix, vector, matrix, vector, matrix, vector,
        ),
        check_vma=False,
    )
```

```python
import functools

import jax
import jax.numpy as jnp
import numpy as np
from jax import lax
from jax.experimental import pallas as pl
from jax.experimental.pallas import tpu as pltpu
from jax.sharding import PartitionSpec as P

D = 768
H = 12
HD = 64
FF = 3072
BLK = 16
F32 = jnp.float32
BF = jnp.bfloat16
NEG = -1e30
VMEM_LIMIT = 56 * 1024 * 1024


def cost(flops, nbytes):
    return pl.CostEstimate(flops=int(flops), bytes_accessed=int(nbytes), transcendentals=0)


def params(*semantics):
    return pltpu.CompilerParams(
        dimension_semantics=semantics or None, vmem_limit_bytes=VMEM_LIMIT
    )


def dot(a, b):
    return lax.dot_general(a, b, (((1,), (0,)), ((), ())), preferred_element_type=F32)


def dot_t(a, b):
    return lax.dot_general(a, b, (((1,), (1,)), ((), ())), preferred_element_type=F32)


def whole(shape):
    return pl.BlockSpec(shape, lambda *_: (0,) * len(shape))


def cuts(count, step):
    return [(at, min(step, count - at)) for at in range(0, count, step)]


def lane_mask(width, head):
    lanes = lax.broadcasted_iota(jnp.int32, (1, width), 1)
    return jnp.where(lanes // HD == head, 1.0, 0.0).astype(BF)


def per_head(block, heads):
    return jnp.concatenate([block * lane_mask(block.shape[1], h) for h in range(heads)], axis=0)


def swap_halves(v):
    out = []
    for at in range(0, v.shape[1], 128):
        part = v[:, at : at + 128]
        lanes = lax.broadcasted_iota(jnp.int32, part.shape, 1)
        out.append(
            jnp.where(
                lanes % HD < HD // 2,
                pltpu.roll(part, 128 - HD // 2, 1),
                pltpu.roll(part, HD // 2, 1),
            )
        )
    return jnp.concatenate(out, axis=1)


def widen(table, width):
    return jnp.concatenate([table] * (width // 128), axis=1)


def cos_sin(angle):
    turns = jnp.round(angle * np.float32(2.0 / np.pi))
    left = angle - turns * np.float32(1.5703125)
    left = left - turns * np.float32(4.837512969970703125e-4)
    left = left - turns * np.float32(7.54978995489188e-8)
    sq = left * left
    sine = left + left * sq * (
        np.float32(-1.6666654611e-1)
        + sq * (np.float32(8.3321608736e-3) + sq * np.float32(-1.9515295891e-4))
    )
    cosine = (
        1.0
        - 0.5 * sq
        + sq
        * sq
        * (
            np.float32(4.166664568298827e-2)
            + sq * (np.float32(-1.388731625493765e-3) + sq * np.float32(2.443315711809948e-5))
        )
    )
    quarter = jnp.bitwise_and(turns.astype(jnp.int32), 3)
    odd = jnp.bitwise_and(quarter, 1) == 1
    sin_out = jnp.where(odd, cosine, sine)
    cos_out = jnp.where(odd, sine, cosine)
    sin_out = jnp.where(quarter >= 2, -sin_out, sin_out)
    cos_out = jnp.where((quarter == 1) | (quarter == 2), -cos_out, cos_out)
    return cos_out, sin_out


def normed(v):
    centered = v - jnp.mean(v, axis=1, keepdims=True)
    var = jnp.mean(centered * centered, axis=1, keepdims=True)
    rstd = lax.rsqrt(var + 1e-05)
    return centered * rstd, rstd


def fold8(v, op):
    return op(v.reshape(v.shape[0] // 8, 8, v.shape[1]), axis=0)


def pair_mask(kcol_ref, rows, codes):
    key = kcol_ref[rows, 0:1]
    low, high, same = codes
    return ((key >= low) & (key < high)) | (key == same)


def query_codes(qrow_ref, at, count):
    cols = pl.ds(at, count)
    return qrow_ref[0:1, cols], qrow_ref[1:2, cols], qrow_ref[2:3, cols]


SUB = 64


def chosen(step, entries):
    value = jnp.int32(entries[0])
    for i, e in enumerate(entries[1:], 1):
        value = jnp.where(step == i, jnp.int32(e), value)
    return value


def attend(step, entries, q_ref, k_ref, vt_ref, kcol_ref, qrow_ref, s_scr, p_scr, heads, chunk):
    blocks = k_ref.shape[0] // chunk
    lq = k_ref.shape[1]
    at = pl.multiple_of(chosen(step, entries) * chunk, chunk)
    codes = query_codes(qrow_ref, at, chunk)
    query = per_head(q_ref[pl.ds(at, chunk), :], heads)

    def score(block, best):
        base = pl.multiple_of(block * chunk, chunk)
        s_scr[pl.ds(base, chunk), :] = dot_t(k_ref[pl.ds(base, chunk), :], query)
        best = list(best)
        for sub in range(0, chunk, SUB):
            rows = pl.ds(base + sub, SUB)
            mask = pair_mask(kcol_ref, rows, codes)
            for h in range(heads):
                cols = slice(h * chunk, (h + 1) * chunk)
                value = jnp.where(mask, s_scr[rows, cols], NEG)
                s_scr[rows, cols] = value
                best[h] = jnp.maximum(best[h], fold8(value, jnp.max))
        return tuple(best)

    best = lax.fori_loop(
        0, blocks, score, tuple(jnp.full((8, chunk), NEG, F32) for _ in range(heads))
    )
    best = [jnp.max(b, axis=0, keepdims=True) for b in best]

    def soften(block, sums):
        base = pl.multiple_of(block * chunk, chunk)
        sums = list(sums)
        for sub in range(0, chunk, SUB):
            rows = pl.ds(base + sub, SUB)
            for h in range(heads):
                cols = slice(h * chunk, (h + 1) * chunk)
                value = jnp.exp(s_scr[rows, cols] - best[h])
                sums[h] = sums[h] + fold8(value, jnp.sum)
                p_scr[rows, cols] = value.astype(BF)
        return tuple(sums)

    sums = lax.fori_loop(
        0, blocks, soften, tuple(jnp.zeros((8, chunk), F32) for _ in range(heads))
    )
    sums = [jnp.sum(s, axis=0, keepdims=True) for s in sums]
    tops = []
    for h in range(heads):
        made = dot(vt_ref[...], p_scr[:, h * chunk : (h + 1) * chunk])
        tops.append(made[h * HD : (h + 1) * HD, :] * (1.0 / sums[h]))
    if heads * HD < lq:
        tops.append(jnp.zeros((lq - heads * HD, chunk), F32))
    logs = [best[h] + jnp.log(sums[h]) for h in range(heads)]
    logs.append(jnp.zeros((8 - heads, chunk), F32))
    return jnp.concatenate(tops, axis=0), jnp.concatenate(logs, axis=0)


def block_outputs(entries, lq, hw, chunk):
    shapes = []
    for _ in entries:
        shapes += [
            jax.ShapeDtypeStruct((chunk, hw), BF),
            jax.ShapeDtypeStruct((lq, chunk), F32),
            jax.ShapeDtypeStruct((8, chunk), F32),
        ]
    return shapes


def store_block(step, entries, refs, joined, logs, hw):
    attended = joined.T[:, :hw].astype(BF)
    for i in range(len(entries)):

        @pl.when(step == i)
        def _(i=i):
            refs[3 * i][...] = attended
            refs[3 * i + 1][...] = joined
            refs[3 * i + 2][...] = logs


def by_block(entries, made):
    return {e: tuple(made[3 * i : 3 * i + 3]) for i, e in enumerate(entries)}


def attention_first(arrays, plan, kcol, qrow, freq, wq, gain, heads, chunk, entries):
    total = kcol.shape[0]
    blocks = total // chunk
    lq = wq.shape[1] // 3
    hw = heads * HD
    count = len(arrays)

    def kernel(*refs):
        x_refs = refs[:count]
        kcol_ref, qrow_ref, freq_ref, wq_ref, gain_ref = refs[count : count + 5]
        h1_ref, q_ref, k_ref, v_ref, vt_ref, cs_ref, sn_ref = refs[count + 5 : count + 12]
        block_refs = refs[count + 12 : count + 12 + 3 * len(entries)]
        s_scr, p_scr = refs[count + 12 + 3 * len(entries) :]
        step = pl.program_id(0)

        @pl.when(step == 0)
        def _():
            gain_row = gain_ref[...]
            for which, src, dst, rows in plan:
                for at, size in cuts(rows, 64):
                    xhat, _ = normed(x_refs[which][src + at : src + at + size, :].astype(F32))
                    h1_ref[dst + at : dst + at + size, :] = (xhat * gain_row).astype(BF)
            lanes = lax.broadcasted_iota(jnp.int32, (1, 128), 1)
            sign = jnp.where(lanes % HD < HD // 2, -1.0, 1.0)

            def project(block, carry):
                rows = pl.ds(pl.multiple_of(block * chunk, chunk), chunk)
                cosine, sine = cos_sin(kcol_ref[rows, 1:2] * freq_ref[...])
                sine = sine * sign
                cs_ref[rows, :] = cosine
                sn_ref[rows, :] = sine
                cosine = widen(cosine, lq)
                sine = widen(sine, lq)
                made = dot(h1_ref[rows, :], wq_ref[...])
                q = made[:, :lq]
                q_ref[rows, :] = ((q * cosine + swap_halves(q) * sine).astype(BF) * 0.125).astype(
                    BF
                )
                k = made[:, lq : 2 * lq]
                k_ref[rows, :] = (k * cosine + swap_halves(k) * sine).astype(BF)
                v = made[:, 2 * lq :]
                v_ref[rows, :] = v.astype(BF)
                vt_ref[:, rows] = v.T.astype(BF)
                return carry

            lax.fori_loop(0, blocks, project, 0)

        joined, logs = attend(
            step, entries, q_ref, k_ref, vt_ref, kcol_ref, qrow_ref, s_scr, p_scr, heads, chunk
        )
        store_block(step, entries, block_refs, joined, logs, hw)

    ins = list(arrays) + [kcol, qrow, freq, wq, gain]
    out_shape = [
        jax.ShapeDtypeStruct((total, D), BF),
        jax.ShapeDtypeStruct((total, lq), BF),
        jax.ShapeDtypeStruct((total, lq), BF),
        jax.ShapeDtypeStruct((total, lq), BF),
        jax.ShapeDtypeStruct((lq, total), BF),
        jax.ShapeDtypeStruct((total, 128), F32),
        jax.ShapeDtypeStruct((total, 128), F32),
    ] + block_outputs(entries, lq, hw, chunk)
    made = pl.pallas_call(
        kernel,
        name="attention_first",
        grid=(len(entries),),
        in_specs=[whole(v.shape) for v in ins],
        out_specs=[whole(o.shape) for o in out_shape],
        out_shape=out_shape,
        scratch_shapes=[
            pltpu.VMEM((total, heads * chunk), F32),
            pltpu.VMEM((total, heads * chunk), BF),
        ],
        compiler_params=params("arbitrary"),
        cost_estimate=cost(8e9, 8e6),
    )(*ins)
    return made[:7], by_block(entries, made[7:])


def attention_rest(saved, kcol, qrow, heads, chunk, entries):
    _, q, k, _, vt, _, _ = saved
    total, lq = k.shape
    hw = heads * HD

    def kernel(q_ref, k_ref, vt_ref, kcol_ref, qrow_ref, *refs):
        step = pl.program_id(0)
        s_scr, p_scr = refs[3 * len(entries) :]
        joined, logs = attend(
            step, entries, q_ref, k_ref, vt_ref, kcol_ref, qrow_ref, s_scr, p_scr, heads, chunk
        )
        store_block(step, entries, refs, joined, logs, hw)

    ins = [q, k, vt, kcol, qrow]
    out_shape = block_outputs(entries, lq, hw, chunk)
    made = pl.pallas_call(
        kernel,
        name="attention_rest",
        grid=(len(entries),),
        in_specs=[whole(v.shape) for v in ins],
        out_specs=[whole(o.shape) for o in out_shape],
        out_shape=out_shape,
        scratch_shapes=[
            pltpu.VMEM((total, heads * chunk), F32),
            pltpu.VMEM((total, heads * chunk), BF),
        ],
        compiler_params=params("arbitrary"),
        cost_estimate=cost(5e9, 4e6),
    )(*ins)
    return by_block(entries, made)


def attention_backward(pulls, by, saved, kcol, qrow, wq, heads, chunk, entries, before, last):
    h1, q, k, v, _, cs, sn = saved
    total, lq = k.shape
    blocks = total // chunk
    hw = heads * HD
    n = len(entries)

    def kernel(*refs):
        g_refs, att_refs, lse_refs = refs[:n], refs[n : 2 * n], refs[2 * n : 3 * n]
        q_ref, k_ref, v_ref, cs_ref, sn_ref, kcol_ref, qrow_ref = refs[3 * n : 3 * n + 7]
        refs = refs[3 * n + 7 :]
        if last:
            dq_in, dk_in, dv_in, wq_ref, h1_ref = refs[:5]
            gqkv_ref, n1_ref = refs[5:7]
            gh_refs = refs[7 : 7 + blocks]
            scr = refs[7 + blocks :]
        else:
            dq_out, dk_out, dv_out = refs[:3]
            scr = refs[3:]
        g_scr, row_scr, kt_scr, dk_scr, dv_scr, s_scr, dp_scr, pb_scr, ds_scr, dst_scr = scr
        step = pl.program_id(0)

        @pl.when(step == 0)
        def _():
            for i in range(n):
                g_scr[i, :, :hw] = g_refs[i][...]
                if hw < lq:
                    g_scr[i, :, hw:] = jnp.zeros((chunk, lq - hw), BF)
                product = g_scr[i].astype(F32).T * att_refs[i][...]
                for h in range(heads):
                    row_scr[i, h : h + 1, :] = jnp.sum(
                        product[h * HD : (h + 1) * HD, :], axis=0, keepdims=True
                    )
                row_scr[i, 8:16, :] = lse_refs[i][...]
            if last:
                dk_scr[...] = dk_in[...]
                dv_scr[...] = dv_in[...]
            else:
                dk_scr[...] = jnp.zeros_like(dk_scr)
                dv_scr[...] = jnp.zeros_like(dv_scr)

            def turn(block, carry):
                rows = pl.ds(pl.multiple_of(block * chunk, chunk), chunk)
                flat = k_ref[rows, :].astype(F32).T
                line = lax.broadcasted_iota(jnp.int32, (lq, 1), 0) // HD
                for h in range(heads):
                    kt_scr[block, :, h * chunk : (h + 1) * chunk] = jnp.where(
                        line == h, flat, 0.0
                    ).astype(BF)
                return carry

            lax.fori_loop(0, blocks, turn, 0)

        at = pl.multiple_of(chosen(step, entries) * chunk, chunk)
        own = pl.ds(at, chunk)
        codes = query_codes(qrow_ref, at, chunk)
        query = per_head(q_ref[own, :], heads)
        pull = per_head(g_scr[step], heads)
        delta = [row_scr[step, h : h + 1, :] for h in range(heads)]
        top = [row_scr[step, 8 + h : 9 + h, :] for h in range(heads)]

        def keys(block, dq_t):
            base = pl.multiple_of(block * chunk, chunk)
            rows = pl.ds(base, chunk)
            s_scr[...] = dot_t(k_ref[rows, :], query)
            dp_scr[...] = dot_t(v_ref[rows, :], pull)
            for sub in range(0, chunk, SUB):
                part = slice(sub, sub + SUB)
                mask = pair_mask(kcol_ref, pl.ds(base + sub, SUB), codes)
                for h in range(heads):
                    cols = slice(h * chunk, (h + 1) * chunk)
                    prob = jnp.exp(jnp.where(mask, s_scr[part, cols] - top[h], NEG))
                    slope = (prob * (dp_scr[part, cols] - delta[h])).astype(BF)
                    pb_scr[part, cols] = prob.astype(BF)
                    ds_scr[part, cols] = slope
                    dst_scr[h * chunk + sub : h * chunk + sub + SUB, :] = slope
            dv_scr[rows, :] += dot(pb_scr[...], pull)
            dk_scr[rows, :] += dot(ds_scr[...], query)
            return dq_t + dot(kt_scr[block], dst_scr[...])

        dq_t = lax.fori_loop(0, blocks, keys, jnp.zeros((lq, chunk), F32))

        def unrotate(value, rows):
            return value * widen(cs_ref[rows, :], lq) - swap_halves(value) * widen(
                sn_ref[rows, :], lq
            )

        dq = unrotate(dq_t.T * 0.125, own).astype(BF)
        if not last:
            dq_out[...] = dq

            @pl.when(step == n - 1)
            def _():
                dk_out[...] = dk_scr[...]
                dv_out[...] = dv_scr[...]

        else:
            gqkv_ref[own, :lq] = dq

            @pl.when(step == n - 1)
            def _():
                gqkv_ref[0:chunk, :lq] = dq_in[...]
                n1 = jnp.zeros((8, D), F32)
                for b in range(blocks):
                    rows = slice(b * chunk, (b + 1) * chunk)
                    gqkv_ref[rows, lq : 2 * lq] = unrotate(dk_scr[rows, :], rows).astype(BF)
                    gqkv_ref[rows, 2 * lq :] = dv_scr[rows, :].astype(BF)
                    gh = dot_t(gqkv_ref[rows, :], wq_ref[...])
                    gh_refs[b][...] = gh.astype(gh_refs[b].dtype)
                    n1 = n1 + fold8(gh * h1_ref[rows, :].astype(F32), jnp.sum)
                n1_ref[...] = n1

    ins = [pulls[e] for e in entries] + [by[e][1] for e in entries] + [by[e][2] for e in entries]
    ins += [q, k, v, cs, sn, kcol, qrow]
    if last:
        ins += list(before) + [wq, h1]
        out_shape = [
            jax.ShapeDtypeStruct((total, 3 * lq), BF),
            jax.ShapeDtypeStruct((8, D), F32),
        ]
        for b in range(blocks):
            out_shape.append(jax.ShapeDtypeStruct((chunk, D), F32 if b == 0 else BF))
    else:
        out_shape = [
            jax.ShapeDtypeStruct((chunk, lq), BF),
            jax.ShapeDtypeStruct((total, lq), F32),
            jax.ShapeDtypeStruct((total, lq), F32),
        ]
    return pl.pallas_call(
        kernel,
        name="attention_backward_last" if last else "attention_backward_own",
        grid=(n,),
        in_specs=[whole(a.shape) for a in ins],
        out_specs=[whole(o.shape) for o in out_shape],
        out_shape=out_shape,
        scratch_shapes=[
            pltpu.VMEM((n, chunk, lq), BF),
            pltpu.VMEM((n, 16, chunk), F32),
            pltpu.VMEM((blocks, lq, heads * chunk), BF),
            pltpu.VMEM((total, lq), F32),
            pltpu.VMEM((total, lq), F32),
            pltpu.VMEM((chunk, heads * chunk), F32),
            pltpu.VMEM((chunk, heads * chunk), F32),
            pltpu.VMEM((chunk, heads * chunk), BF),
            pltpu.VMEM((chunk, heads * chunk), BF),
            pltpu.VMEM((heads * chunk, chunk), BF),
        ],
        compiler_params=params("arbitrary"),
        cost_estimate=cost(3e9 * n, 1e7),
    )(*ins)


def dot_first(a, b):
    return lax.dot_general(a, b, (((0,), (0,)), ((), ())), preferred_element_type=F32)


def reorder_columns(place, own, other, order):
    width = own.shape[2]
    out = order.shape[0]

    def kernel(place_ref, own_ref, other_ref, order_ref, out_ref, scr):
        d = place_ref[0]
        scr[...] = jnp.zeros_like(scr)
        for j in range(4):
            scr[192 * j : 192 * j + 192, :width] = own_ref[d ^ j]
            scr[192 * j : 192 * j + 192, 384 : 384 + width] = other_ref[d ^ j]
        out_ref[...] = dot_t(scr[...], order_ref[...]).astype(BF)

    return pl.pallas_call(
        kernel,
        name="reorder_columns",
        grid_spec=pltpu.PrefetchScalarGridSpec(
            num_scalar_prefetch=1,
            grid=(1,),
            in_specs=[whole(own.shape), whole(other.shape), whole(order.shape)],
            out_specs=whole((D, out)),
            scratch_shapes=[pltpu.VMEM((D, 768), BF)],
        ),
        out_shape=jax.ShapeDtypeStruct((D, out), BF),
        compiler_params=params("arbitrary"),
        cost_estimate=cost(1e9, 3e6),
    )(place, own, other, order)


def reorder_out(place, own, other, order):
    def kernel(place_ref, own_ref, other_ref, order_ref, out_ref, scr):
        d = place_ref[0]
        for j in range(4):
            for k in range(4):
                at = 96 * k
                part = slice(96 * j, 96 * j + 96)
                scr[j, :, at : at + 96] = own_ref[k, :, part]
                scr[j, :, 384 + at : 384 + at + 96] = other_ref[k, :, part]
        for j in range(4):
            out_ref[j] = dot_t(scr[d ^ j], order_ref[...]).astype(BF)

    return pl.pallas_call(
        kernel,
        name="reorder_out",
        grid_spec=pltpu.PrefetchScalarGridSpec(
            num_scalar_prefetch=1,
            grid=(1,),
            in_specs=[whole(own.shape), whole(other.shape), whole(order.shape)],
            out_specs=whole((4, 192, D)),
            scratch_shapes=[pltpu.VMEM((4, 192, 768), BF)],
        ),
        out_shape=jax.ShapeDtypeStruct((4, 192, D), BF),
        compiler_params=params("arbitrary"),
        cost_estimate=cost(1e9, 3e6),
    )(place, own, other, order)


def qkv_weight(place, h1, gqkv, order):
    def kernel(place_ref, h_ref, g_ref, order_ref, keep_ref, send_ref):
        d = place_ref[0]
        made = dot_first(h_ref[...], g_ref[...]).astype(BF)
        made = dot(made, order_ref[...]).astype(BF)
        for j in range(4):
            rows = slice(192 * j, 192 * j + 192)
            keep_ref[d ^ j] = made[rows, :288]
            send_ref[d ^ j] = made[rows, 384:672]

    shape = jax.ShapeDtypeStruct((4, 192, 288), BF)
    return pl.pallas_call(
        kernel,
        name="qkv_weight",
        grid_spec=pltpu.PrefetchScalarGridSpec(
            num_scalar_prefetch=1,
            grid=(1,),
            in_specs=[whole(h1.shape), whole(gqkv.shape), whole(order.shape)],
            out_specs=[whole(shape.shape)] * 2,
        ),
        out_shape=[shape, shape],
        compiler_params=params("arbitrary"),
        cost_estimate=cost(2e9, 5e6),
    )(place, h1, gqkv, order)


def out_weight(place, mixed, gproj, order):
    groups = len(mixed)

    def kernel(place_ref, *refs):
        m_refs = refs[:groups]
        g_ref, order_ref, keep_ref, send_ref = refs[groups:]
        d, z = place_ref[0], place_ref[1]
        for k in range(groups):
            made = dot_first(m_refs[k][...], g_ref[...]).astype(BF)
            made = dot(made, order_ref[...]).astype(BF)
            row = d ^ lax.rem(z + (groups - k), groups)
            keep_ref[row] = made[:, :384]
            send_ref[row] = made[:, 384:]

    ins = list(mixed) + [gproj, order]
    shape = jax.ShapeDtypeStruct((4, 192, 384), BF)
    return pl.pallas_call(
        kernel,
        name="out_weight",
        grid_spec=pltpu.PrefetchScalarGridSpec(
            num_scalar_prefetch=1,
            grid=(1,),
            in_specs=[whole(a.shape) for a in ins],
            out_specs=[whole(shape.shape)] * 2,
        ),
        out_shape=[shape, shape],
        compiler_params=params("arbitrary"),
        cost_estimate=cost(1e9, 4e6),
    )(place, *ins)


def output_projection(place, mixed, wout, x, gain):
    groups = len(mixed)
    rows = x.shape[0]

    def kernel(place_ref, *refs):
        m_refs = refs[:groups]
        w_ref, x_ref, gain_ref, res_ref, h2_ref = refs[groups:]
        z = place_ref[1]
        total = x_ref[...].astype(F32)
        for k in range(groups):
            total = total + dot(m_refs[k][...], w_ref[lax.rem(z + (groups - k), groups)])
        res_ref[...] = total
        for at, size in cuts(rows, 64):
            xhat, _ = normed(res_ref[at : at + size, :])
            h2_ref[at : at + size, :] = (xhat * gain_ref[...]).astype(BF)

    ins = list(mixed) + [wout, x, gain]
    return pl.pallas_call(
        kernel,
        name="output_projection",
        grid_spec=pltpu.PrefetchScalarGridSpec(
            num_scalar_prefetch=1,
            grid=(1,),
            in_specs=[whole(a.shape) for a in ins],
            out_specs=[whole((rows, D)), whole((rows, D))],
        ),
        out_shape=[jax.ShapeDtypeStruct((rows, D), F32), jax.ShapeDtypeStruct((rows, D), BF)],
        compiler_params=params("arbitrary"),
        cost_estimate=cost(1e9, 3e6),
    )(place, *ins)


def feed_forward(place, h2_own, h2_other, dy_own, dy_other, weights, bias):
    rows = h2_own.shape[0]
    both = 2 * rows
    width = 384

    def kernel(
        place_ref, ho_ref, hp_ref, go_ref, gp_ref, w1a_ref, w1b_ref, w2a_ref, w2b_ref, b_ref,
        out_own, out_other, gh_own, gh_other, d1a_ref, d1b_ref, d2a_ref, d2b_ref, db_ref,
        h_scr, g_scr, ht_scr, gt_scr, w1_scr, w2_scr, pre_scr, ga_scr, act_scr, slope_scr, out_scr,
        gh_scr, dw_scr,
    ):
        step = pl.program_id(0)
        d = place_ref[0]
        z = place_ref[1]

        @pl.when(step == 0)
        def _():
            h_scr[:rows, :] = ho_ref[...]
            h_scr[rows:, :] = hp_ref[...]
            g_scr[:rows, :] = go_ref[...]
            g_scr[rows:, :] = gp_ref[...]
            for at in range(0, both, 256):
                part = slice(at, at + 256)
                ht_scr[:, part] = h_scr[part, :].astype(F32).T.astype(BF)
                gt_scr[:, part] = g_scr[part, :].astype(F32).T.astype(BF)

        near = lax.rem(step - z + 4, 4)
        hidden = step ^ d
        for odd in range(2):

            @pl.when(d % 2 == odd)
            def _(odd=odd):
                for j in range(4):
                    src = (w1a_ref, w1b_ref)[odd ^ (j % 2)]
                    w1_scr[192 * j : 192 * j + 192, :] = src[(d ^ j) // 2, near]

            @pl.when(hidden // 2 == odd)
            def _(odd=odd):
                for j in range(4):
                    src = (w2a_ref, w2b_ref)[odd]
                    w2_scr[192 * j : 192 * j + 192, :] = src[hidden % 2, lax.rem(j - z + 4, 4)]

        pre_scr[...] = dot(h_scr[...], w1_scr[...])
        ga_scr[...] = dot(g_scr[...], w2_scr[...])
        bias_row = b_ref[0].astype(F32)
        total = jnp.zeros((8, width), F32)
        for at in range(0, both, 32):
            part = slice(at, at + 32)
            u = pre_scr[part, :] + bias_row
            usq = u * u
            c = np.float32(np.sqrt(2.0 / np.pi))
            t = jnp.tanh(c * (u + np.float32(0.044715) * (usq * u)))
            half = 0.5 * (1.0 + t)
            act_scr[part, :] = (u * half).astype(BF)
            rise = half + 0.5 * u * (1.0 - t * t) * (c * (1.0 + np.float32(0.134145) * usq))
            slope = (ga_scr[part, :] * rise).astype(BF)
            slope_scr[part, :] = slope
            total = total + fold8(slope.astype(F32), jnp.sum)
        db_ref[0] = total

        out_now = dot_t(act_scr[...], w2_scr[...])
        gh_now = dot_t(slope_scr[...], w1_scr[...])

        @pl.when(step == 0)
        def _():
            out_scr[...] = out_now
            gh_scr[...] = gh_now

        @pl.when(step > 0)
        def _():
            out_scr[...] += out_now
            gh_scr[...] += gh_now

        dw_scr[0] = dot(ht_scr[...], slope_scr[...]).astype(BF)
        dw_scr[1] = dot(gt_scr[...], act_scr[...]).astype(BF)
        for odd in range(2):

            @pl.when(d % 2 == odd)
            def _(odd=odd):
                for j in range(4):
                    dst = (d1a_ref, d1b_ref)[odd ^ (j % 2)]
                    dst[(d ^ j) // 2, near] = dw_scr[0, 192 * j : 192 * j + 192, :]

            @pl.when(hidden // 2 == odd)
            def _(odd=odd):
                for j in range(4):
                    dst = (d2a_ref, d2b_ref)[odd]
                    dst[hidden % 2, lax.rem(j - z + 4, 4)] = dw_scr[1, 192 * j : 192 * j + 192, :]

        @pl.when(step == 3)
        def _():
            out_own[...] = out_scr[:rows, :]
            out_other[...] = out_scr[rows:, :].astype(BF)
            gh_own[...] = gh_scr[:rows, :]
            gh_other[...] = gh_scr[rows:, :].astype(BF)

    def by_z(i, place_ref):
        return (lax.rem(i - place_ref[1] + 4, 4), 0, 0)

    ins = [h2_own, h2_other, dy_own, dy_other] + list(weights)
    full = jax.ShapeDtypeStruct((2, 4, 192, width), BF)
    out_shape = [
        jax.ShapeDtypeStruct((rows, D), F32),
        jax.ShapeDtypeStruct((rows, D), BF),
        jax.ShapeDtypeStruct((rows, D), F32),
        jax.ShapeDtypeStruct((rows, D), BF),
        full,
        full,
        full,
        full,
        jax.ShapeDtypeStruct((4, 8, width), F32),
    ]
    return pl.pallas_call(
        kernel,
        name="feed_forward",
        grid_spec=pltpu.PrefetchScalarGridSpec(
            num_scalar_prefetch=1,
            grid=(4,),
            in_specs=[whole(a.shape) for a in ins] + [pl.BlockSpec((1, 1, width), by_z)],
            out_specs=[whole(o.shape) for o in out_shape[:-1]]
            + [pl.BlockSpec((1, 8, width), by_z)],
            scratch_shapes=[
                pltpu.VMEM((both, D), BF),
                pltpu.VMEM((both, D), BF),
                pltpu.VMEM((D, both), BF),
                pltpu.VMEM((D, both), BF),
                pltpu.VMEM((D, width), BF),
                pltpu.VMEM((D, width), BF),
                pltpu.VMEM((both, width), F32),
                pltpu.VMEM((both, width), F32),
                pltpu.VMEM((both, width), BF),
                pltpu.VMEM((both, width), BF),
                pltpu.VMEM((both, D), F32),
                pltpu.VMEM((both, D), F32),
                pltpu.VMEM((2, D, width), BF),
            ],
        ),
        out_shape=out_shape,
        compiler_params=params("arbitrary"),
        cost_estimate=cost(7.2e9, 1.5e7),
    )(place, *ins, bias)


def residual_backward(place, gh_own, gh_in, residual, dy, gain, wout):
    rows = dy.shape[0]
    groups, hw = wout.shape[0], wout.shape[1]

    def kernel(place_ref, gh_ref, gi_ref, res_ref, dy_ref, gain_ref, w_ref, *outs):
        gres_ref, gproj_ref, vec_ref = outs[:3]
        gm_refs = outs[3:]
        z = place_ref[1]
        gain_row = gain_ref[...]
        gsum = jnp.zeros((8, D), F32)
        bsum = jnp.zeros((8, D), F32)
        for at, size in cuts(rows, 32):
            part = slice(at, at + size)
            xhat, rstd = normed(res_ref[part, :])
            dy_now = dy_ref[part, :].astype(F32)
            grad = gh_ref[part, :] + gi_ref[part, :].astype(F32)
            along = grad * xhat
            gsum = gsum + fold8(along, jnp.sum)
            bsum = bsum + fold8(dy_now, jnp.sum)
            u = grad * gain_row
            back = (
                u
                - jnp.mean(u, axis=1, keepdims=True)
                - xhat * jnp.mean(along * gain_row, axis=1, keepdims=True)
            )
            value = dy_now + back * rstd
            gres_ref[part, :] = value
            gproj_ref[part, :] = value.astype(BF)
        vec_ref[0:8, :] = gsum
        vec_ref[8:16, :] = bsum
        for k in range(groups):
            gm_refs[k][...] = dot_t(gproj_ref[...], w_ref[lax.rem(z + k, groups)]).astype(BF)

    ins = [gh_own, gh_in, residual, dy, gain, wout]
    out_shape = [
        jax.ShapeDtypeStruct((rows, D), F32),
        jax.ShapeDtypeStruct((rows, D), BF),
        jax.ShapeDtypeStruct((16, D), F32),
    ] + [jax.ShapeDtypeStruct((rows, hw), BF) for _ in range(groups)]
    made = pl.pallas_call(
        kernel,
        name="residual_backward",
        grid_spec=pltpu.PrefetchScalarGridSpec(
            num_scalar_prefetch=1,
            grid=(1,),
            in_specs=[whole(a.shape) for a in ins],
            out_specs=[whole(o.shape) for o in out_shape],
        ),
        out_shape=out_shape,
        compiler_params=params("arbitrary"),
        cost_estimate=cost(1e9, 4e6),
    )(place, *ins)
    return made[0], made[1], made[2], made[3:]


def input_backward(terms, x, gain, gres):
    rows = x.shape[0]
    count = len(terms)

    def kernel(*refs):
        x_ref, gain_ref, gres_ref, out_ref = refs[count:]
        for at, size in cuts(rows, 32):
            part = slice(at, at + size)
            grad = refs[0][part, :].astype(F32)
            for t in range(1, count):
                grad = grad + refs[t][part, :].astype(F32)
            xhat, rstd = normed(x_ref[part, :].astype(F32))
            u = grad * gain_ref[...]
            back = (
                u
                - jnp.mean(u, axis=1, keepdims=True)
                - xhat * jnp.mean(u * xhat, axis=1, keepdims=True)
            )
            out_ref[part, :] = (gres_ref[part, :] + back * rstd).astype(BF)

    ins = list(terms) + [x, gain, gres]
    return pl.pallas_call(
        kernel,
        name="input_backward",
        grid=(1,),
        in_specs=[whole(a.shape) for a in ins],
        out_specs=whole((rows, D)),
        out_shape=jax.ShapeDtypeStruct((rows, D), BF),
        compiler_params=params("arbitrary"),
        cost_estimate=cost(1e8, 3e6),
    )(*ins)


def add_low(a, b):
    return (a.astype(F32) + b.astype(F32)).astype(BF)


def pick(v, index):
    return lax.dynamic_index_in_dim(v, index, 0, keepdims=False)


def after(v, *others):
    return lax.optimization_barrier((v, others))[0]


class Links:
    def __init__(self, n_dp, n_seq):
        self.n_dp, self.n_seq, self.nz = n_dp, n_seq, n_seq // 2

    def core(self, v):
        return lax.ppermute(v, "seq", [(s, s ^ 1) for s in range(self.n_seq)])

    def flip(self, v, bit):
        return lax.ppermute(v, "dp", [(i, i ^ bit) for i in range(self.n_dp)])

    def shift(self, v, k):
        n = self.nz
        return lax.ppermute(
            v, "seq", [(s, 2 * ((s // 2 + k) % n) + s % 2) for s in range(self.n_seq)]
        )


def order_matrix(source, valid):
    rows = lax.broadcasted_iota(jnp.int32, (768, 768), 0)
    return jnp.where((rows == source[None, :]) & valid[None, :], 1.0, 0.0).astype(BF)


def per_device(
    n_dp,
    n_seq,
    inputs,
    row_segment,
    row_flag,
    row_block,
    norm1_scale,
    w_qkv,
    w_out,
    norm2_scale,
    w_fc1,
    b_fc1,
    w_fc2,
    b_fc2,
    cotangent,
):
    links = Links(n_dp, n_seq)
    nz = links.nz
    local = inputs.shape[2]
    chunk = 2 * local
    heads = -(-H // nz)
    hw = heads * HD
    lq = -(-hw // 128) * 128
    fast = n_dp == 4 and nz == 4 and H % nz == 0
    d = lax.axis_index("dp")
    s = lax.axis_index("seq")
    z = s // 2
    c = s % 2
    place = jnp.stack([d, z]).astype(jnp.int32)
    n1_w = D // n_seq
    b1_w = FF // n_seq

    x_loc = inputs[:, 0]
    x_keep = pick(x_loc, c)
    labels = jnp.stack([row_segment[:, 0], row_flag[:, 0], row_block[:, 0]], axis=1)
    labels = labels.astype(BF).reshape(2, 3 * local)
    vector = jnp.concatenate([norm1_scale, norm2_scale, b_fc2, b_fc1]).astype(BF)
    vector = jnp.pad(vector, (0, D - vector.shape[0]))
    lab_keep, lab_send = pick(labels, c), pick(labels, 1 - c)
    extra = jnp.stack([jnp.pad(lab_send, (0, D - 3 * local)), vector])
    message = jnp.concatenate([pick(x_loc, 1 - c), jnp.pad(extra, ((0, 14), (0, 0)))], axis=0)
    swapped = links.core(message)
    extra = jnp.stack(
        [
            jnp.concatenate([lab_keep, swapped[local, : 3 * local]]),
            vector,
            swapped[local + 1],
        ]
    )
    x_ext = jnp.concatenate(
        [x_keep, swapped[:local], jnp.pad(extra, ((0, 13), (0, 0)))], axis=0
    )

    def to_both(w):
        return jnp.where(c == 0, w[0], w[1]), jnp.where(c == 0, w[1], w[0])

    cot = cotangent[:, 0]
    if fast:
        two = w_fc2.astype(BF).T.reshape(96, 2, 384)
        two_keep, two_send = to_both((two[:, 0], two[:, 1]))
        both = jnp.concatenate([cot.reshape(chunk, D), jnp.pad(two_send, ((0, 0), (0, 384)))])
    else:
        both = cot.reshape(chunk, D)
    both_in = links.core(both)
    cot_in = both_in[:chunk].reshape(2, local, D)
    dy_own = jnp.concatenate([pick(cot, c), pick(cot_in, c)], axis=0)
    dy_other = jnp.concatenate([pick(cot_in, 1 - c), pick(cot, 1 - c)], axis=0)

    if nz == 4:
        x_before = links.shift(x_ext, 1)
        x_after = links.shift(x_ext, -1)
        x_low = links.shift(x_before[:144], 1)
        x_high = links.shift(x_after[144:], -1)
        gathered = [[x_ext], [x_after], [x_low, x_high], [x_before]]
        settled = (x_low, x_high)
    else:
        gathered = [[x_ext]] + [[links.shift(x_ext, -k)] for k in range(1, nz)]
        settled = (x_ext,)
    arrays, plan, extras = [], [], []
    for k, pieces in enumerate(gathered):
        at = 0
        for piece in pieces:
            rows = min(piece.shape[0], chunk - at)
            plan.append((len(arrays), 0, k * chunk + at, rows))
            at += rows
            arrays.append(piece)
        extras.append(pieces[-1][-16:])
    extras = jnp.stack(extras)
    labels_all = extras[:, 0].astype(F32).reshape(nz, 2, 3, local)
    segment = labels_all[:, :, 0].reshape(-1)
    flag = labels_all[:, :, 1].reshape(-1)
    block = labels_all[:, :, 2].reshape(-1)
    total = segment.shape[0]
    start = segment * 4096.0
    key_code = start + jnp.where(flag > 0.5, block, block + 2048.0)
    low = start
    high = start + block + flag
    same = jnp.where(flag > 0.5, -1.0, key_code)
    position = block * BLK + (jnp.arange(total, dtype=jnp.int32) % BLK).astype(F32)
    qrow = jnp.pad(jnp.stack([low, high, same]), ((0, 5), (0, 0)))
    kcol = jnp.pad(jnp.stack([key_code, position], axis=1), ((0, 0), (0, 6)))
    freq = np.tile(
        np.float32(10000.0) ** (np.float32(-2.0) * np.arange(32, dtype=np.float32) / HD), 4
    )
    freq = jnp.asarray(freq.astype(np.float32)[None, :])
    vectors = extras[:, 1:3]
    bias_rel = vectors[:, 0, 3 * n1_w : 3 * n1_w + b1_w]
    vectors = jnp.roll(jnp.where(c == 0, vectors, vectors[:, ::-1]), z, axis=0)
    gain_one = vectors[:, :, :n1_w].reshape(1, D).astype(F32)
    gain_two = vectors[:, :, n1_w : 2 * n1_w].reshape(1, D).astype(F32)
    bias_two = vectors[:, :, 2 * n1_w : 3 * n1_w].reshape(1, D).astype(F32)

    if fast:
        cols = jnp.arange(768, dtype=jnp.int32)
        half, at = cols // 384, cols % 384
        qkv_order = order_matrix(
            256 * (at // 96) + 96 * (c ^ half) + at % 96, at < 288
        )
        out_order = order_matrix(
            192 * ((z + at // 96) % 4) + 96 * (c ^ half) + at % 96, at < 384
        )
        wq_parts = w_qkv.astype(BF)
        parts = []
        for i in range(3):
            parts.append(
                lax.ppermute(
                    wq_parts[:, 96 * i : 96 * i + 96],
                    "seq",
                    [(q, (3 * q + i) % 8) for q in range(8)],
                )
            )
        parts = jnp.stack(parts)
        wq_own = jnp.concatenate(
            [pick(parts, (2 * t + s) % 3) for t in range(3)] + [w_out.astype(BF)], axis=1
        )
        wq_own = jnp.stack([wq_own, links.flip(wq_own, 1)])
        wq_own = jnp.stack([wq_own, links.flip(wq_own, 2)]).reshape(4, 192, 384)
        wq_in = links.core(wq_own)
        wq = reorder_columns(place, wq_own, wq_in, qkv_order)
        wo_own = jnp.concatenate([wq_own[j, :, 288:] for j in range(4)], axis=1)

        two = jnp.concatenate(to_both((two_keep, both_in[chunk:, :384])), axis=0)
        w12 = jnp.stack([w_fc1.astype(BF), two])
        w_before = links.shift(w12, 1)
        w_after = links.shift(w12, -1)
        w1_two = links.shift(w_before[0], 1)
        w2_two = links.shift(w_after[1], -1)
        w1 = jnp.stack([w12[0], w_after[0], w1_two, w_before[0]])
        w2 = jnp.stack([w12[1], w_after[1], w2_two, w_before[1]])
        kcol = after(kcol, w1, w2)
        w1_in = links.flip(w1, 2)
        w2_in = links.flip(w2, 1)
        bias_one = bias_rel.reshape(4, 1, 384)
        ff_place = place
    else:

        def everywhere(w):
            w = lax.all_gather(w.astype(BF), "seq", axis=1, tiled=True)
            return lax.all_gather(w, "dp", axis=0, tiled=True)

        wq = everywhere(w_qkv).reshape(D, 3, D)
        wq = jnp.pad(wq, ((0, 0), (0, 0), (0, nz * hw - D)))
        wq = lax.dynamic_slice_in_dim(wq, z * hw, hw, 2)
        wq = jnp.pad(wq, ((0, 0), (0, 0), (0, lq - hw))).reshape(D, 3 * lq)
        wout = jnp.pad(everywhere(w_out), ((0, nz * hw - D), (0, 0))).reshape(nz, hw, D)
        w1 = lax.dynamic_slice_in_dim(everywhere(w_fc1), c * (FF // 2), FF // 2, 1)
        w1 = w1.reshape(2, 2, 192, 4, 384).transpose(3, 1, 0, 2, 4)
        w2 = lax.dynamic_slice_in_dim(everywhere(w_fc2), c * (FF // 2), FF // 2, 0)
        w2 = w2.reshape(2, 2, 384, 4, 192).transpose(3, 1, 0, 4, 2)
        w1, w2 = w1.transpose(1, 2, 0, 3, 4), w2.transpose(2, 1, 0, 3, 4)
        weights = (w1[0], w1[1], w2[0], w2[1])
        bias_all = vectors[:, :, 3 * n1_w : 3 * n1_w + b1_w].reshape(FF)
        bias_one = lax.dynamic_slice_in_dim(bias_all, c * (FF // 2), FF // 2, 0).reshape(4, 1, 384)
        ff_place = jnp.zeros((2,), jnp.int32)

    far = sorted(range(1, nz), key=lambda k: -min(k, nz - k))
    first = far[: nz // 2]
    rest = far[nz // 2 :] + [0]
    saved, by = attention_first(
        arrays, plan, kcol, qrow, freq, wq, gain_one, heads, chunk, first
    )
    mixed = {k: links.shift(by[k][0], k) for k in first}
    rest_in = saved
    if fast:
        w1_in, w2_in, wo_own, _ = lax.optimization_barrier((w1_in, w2_in, wo_own, by[first[0]]))
        w1a = jnp.stack([w1, w1_in])
        w2a = jnp.stack([w2, w2_in])
        w1b = links.flip(w1a, 1)
        w2b = links.flip(w2a, 2)
        weights = (w1a, w1b, w2a, w2b)
        wo_own = jnp.stack([wo_own] + [links.shift(wo_own, -k) for k in range(1, 4)])
        rest_in = after(tuple(saved), w1a, w2a)
    by_rest = attention_rest(rest_in, kcol, qrow, heads, chunk, rest)
    by = {**by, **by_rest}
    for k in rest:
        mixed[k] = links.shift(by[k][0], k) if k else by[k][0]
    mixed = [mixed[k] for k in range(nz)]
    if fast:
        wo_own = after(wo_own, by[0][0])
        wout = reorder_out(place, wo_own, links.core(wo_own), out_order)
    x_own = x_ext[:chunk]
    residual, h2 = output_projection(place, mixed, wout, x_own, gain_two)
    h2_in = links.core(h2)
    (out_own, out_other, gh_own, gh_other, dw1a, dw1b, dw2a, dw2b, db1) = feed_forward(
        ff_place, h2, h2_in, dy_own, dy_other, weights, bias_one
    )
    gh_in = links.core(gh_other)
    if fast:
        dw1_in = links.flip(dw1b, 1)
        dw2_in = links.flip(dw2b, 2)
    gres, gproj, sums, gmixed = residual_backward(
        place, gh_own, gh_in, residual, dy_own, gain_two, wout
    )
    pulled = [gmixed[0]] + [links.shift(gmixed[k], k) for k in range(1, nz)]
    pulled = [pulled[(nz - k) % nz] for k in range(nz)]
    part = attention_backward(
        pulled, by, saved, kcol, qrow, wq, heads, chunk, [0], None, False
    )
    grad_gain_two = jnp.sum(sums[:8], axis=0)
    grad_bias_two = jnp.sum(sums[8:], axis=0)
    grad_bias_one = jnp.sum(db1, axis=1)
    if fast:
        wo_keep, wo_send = out_weight(place, mixed, gproj, out_order)
        wo_came = links.core(wo_send)
    out_other = after(out_other, part)
    out_in = links.core(out_other)
    out_rows = (residual + out_own + out_in.astype(F32) + bias_two).astype(BF)
    rows_in = links.core(out_rows[local:])
    if fast:
        dwo = add_low(wo_keep, wo_came)
        part, _ = lax.optimization_barrier((part, (dwo, out_rows, grad_bias_one, grad_bias_two)))
        dwo = sum(
            [dwo[..., :96].astype(F32)]
            + [
                links.shift(dwo[..., 96 * k : 96 * k + 96], k).astype(F32)
                for k in range(1, 4)
            ]
        )
    made = attention_backward(
        pulled, by, saved, kcol, qrow, wq, heads, chunk, list(range(1, nz)), part, True
    )
    gqkv, n1_sum, gh1 = made[0], made[1], made[2:]
    if nz == 4:
        low_in = links.shift(gh1[2][:local], 1)
        high_in = links.shift(gh1[2][local:], -1)
        up = jnp.concatenate([add_low(gh1[1][:local], low_in), gh1[1][local:]], axis=0)
        down = jnp.concatenate([gh1[3][:local], add_low(gh1[3][local:], high_in)], axis=0)
        terms = [gh1[0], links.shift(up, 1), links.shift(down, -1)]
    else:
        terms = [gh1[0]] + [links.shift(gh1[k], k) for k in range(1, nz)]
    grad_rows = input_backward(terms, x_own, gain_one, gres)
    grad_in = links.core(grad_rows[local:])

    def by_micro(own, other):
        return jnp.where(c == 0, jnp.stack([own, other]), jnp.stack([other, own]))[:, None]

    outputs = by_micro(out_rows[:local], rows_in)
    input_grad = by_micro(grad_rows[:local], grad_in)

    grad_gain_one = jnp.sum(n1_sum, axis=0) / gain_one[0]

    if fast:
        wq_keep, wq_send = qkv_weight(place, saved[0], after(gqkv, low_in, high_in), qkv_order)
        joint = jnp.concatenate(
            [add_low(wq_keep, links.core(wq_send)), dwo.astype(BF)], axis=2
        )
        joint = joint.reshape(2, 2, 192, 384)
        joint = add_low(joint[0], links.flip(joint[1], 2))
        joint = joint[0].astype(F32) + links.flip(joint[1], 1).astype(F32)
        g_out = joint[:, 288:]
        third = jnp.stack([joint[:, 96 * t : 96 * t + 96] for t in range(3)])
        g_qkv = jnp.concatenate(
            [
                lax.ppermute(
                    pick(third, lax.rem(2 * (i - s + 9), 3)),
                    "seq",
                    [((3 * q + i) % 8, q) for q in range(8)],
                )
                for i in range(3)
            ],
            axis=1,
        )
        dw1_in, dw2_in, _ = lax.optimization_barrier((dw1_in, dw2_in, gqkv))
        dw1_in = links.flip(add_low(dw1a[1], dw1_in[1]), 2), dw1_in[0]
        dw2_in = links.flip(add_low(dw2a[1], dw2_in[1]), 1), dw2_in[0]
        dw1 = dw1a[0].astype(F32) + dw1_in[0].astype(F32) + dw1_in[1].astype(F32)
        dw2 = dw2a[0].astype(F32) + dw2_in[0].astype(F32) + dw2_in[1].astype(F32)
        low_in = links.shift(dw1[2].astype(BF), 1)
        high_in = links.shift(dw2[2].astype(BF), -1)
        up = jnp.stack([dw1[1] + low_in.astype(F32), dw2[1]]).astype(BF)
        down = jnp.stack([dw1[3], dw2[3] + high_in.astype(F32)]).astype(BF)
        up_in = links.shift(up, 1).astype(F32)
        down_in = links.shift(down, -1).astype(F32)
        dw = jnp.stack([dw1[0], dw2[0]]) + up_in + down_in
        g_fc1 = dw[0]
        keep, send = to_both((dw[1, :96], dw[1, 96:]))
        came = links.core(send)
        g_fc2 = jnp.concatenate(to_both((keep, came)), axis=1).T
        three = jnp.stack([grad_gain_one, grad_gain_two, grad_bias_two]).reshape(3, 4, 2, 96)
        three = jnp.roll(three, -z, axis=1)
        keep, send = to_both((three[:, :, 0], three[:, :, 1]))
        three = (keep + links.core(send)).transpose(1, 0, 2).reshape(4, 288)
        vec = jnp.concatenate([three, grad_bias_one, jnp.zeros((4, 352), F32)], axis=1)
        vec = vec.reshape(4, 8, 128)
        vec = sum([vec[0]] + [links.shift(vec[k], k) for k in range(1, 4)])
        for bit in (1, 2):
            vec = vec + links.flip(vec, bit)
        vec = vec.reshape(1024)
        vecs = (vec[:96], vec[96:192], vec[288:672], vec[192:288])
    else:

        def owned(w):
            w = lax.psum_scatter(w.astype(BF), "seq", scatter_dimension=1, tiled=True)
            return lax.psum_scatter(w, "dp", scatter_dimension=0, tiled=True).astype(F32)

        dwq = jnp.einsum("rd,rj->dj", saved[0], gqkv, preferred_element_type=F32)
        spread = jnp.zeros((D, 3, nz * hw), F32)
        spread = lax.dynamic_update_slice_in_dim(
            spread, dwq.reshape(D, 3, lq)[..., :hw], z * hw, 2
        )
        g_qkv = owned(spread[..., :D].reshape(D, 3 * D))
        mixed_all = jnp.concatenate(mixed, axis=1)
        dwo = jnp.einsum("ri,ro->io", mixed_all, gproj, preferred_element_type=F32)
        dwo = dwo.reshape(nz, hw, D)
        dwo = jnp.roll(dwo[::-1], z + 1, axis=0).reshape(nz * hw, D)[:D]
        g_out = owned(dwo)
        half = jnp.stack([dw1a, dw1b]).transpose(1, 0, 3, 2, 4).reshape(D, FF // 2)
        full = lax.dynamic_update_slice_in_dim(
            jnp.zeros((D, FF), BF), half, c * (FF // 2), 1
        )
        g_fc1 = owned(full)
        half = jnp.stack([dw2a, dw2b]).transpose(0, 1, 4, 2, 3).reshape(FF // 2, D)
        full = lax.dynamic_update_slice_in_dim(
            jnp.zeros((FF, D), BF), half, c * (FF // 2), 0
        )
        g_fc2 = owned(full)
        bias_full = lax.dynamic_update_slice_in_dim(
            jnp.zeros((FF,), F32), grad_bias_one.reshape(-1), c * (FF // 2), 0
        )
        vecs = tuple(
            lax.psum(lax.psum_scatter(v, "seq", scatter_dimension=0, tiled=True), "dp")
            for v in (grad_gain_one, grad_gain_two, bias_full, grad_bias_two)
        )

    return (
        outputs,
        input_grad,
        vecs[0],
        g_qkv,
        g_out,
        vecs[1],
        g_fc1,
        vecs[2],
        g_fc2,
        vecs[3],
    )


def solution(mesh):
    rows = P(None, "dp", "seq", None)
    labels = P(None, "dp", "seq")
    matrix = P("dp", "seq")
    vector = P("seq")
    return jax.shard_map(
        functools.partial(per_device, mesh.shape["dp"], mesh.shape["seq"]),
        mesh=mesh,
        in_specs=(
            rows, labels, labels, labels, vector, matrix, matrix, vector, matrix, vector, matrix,
            vector, rows,
        ),
        out_specs=(
            rows, rows, vector, matrix, matrix, vector, matrix, vector, matrix, vector,
        ),
        check_vma=False,
    )
```

```python
import functools

import jax
import jax.numpy as jnp
import numpy as np
from jax import lax
from jax.experimental import pallas as pl
from jax.experimental.pallas import tpu as pltpu
from jax.sharding import PartitionSpec as P

D = 768
H = 12
HD = 64
FF = 3072
BLK = 16
F32 = jnp.float32
BF = jnp.bfloat16
NEG = -1e30
VMEM_LIMIT = 56 * 1024 * 1024


def cost(flops, nbytes):
    return pl.CostEstimate(flops=int(flops * 1e-3), bytes_accessed=int(nbytes * 1e-3), transcendentals=0)


def params(*semantics):
    return pltpu.CompilerParams(
        dimension_semantics=semantics or None, vmem_limit_bytes=VMEM_LIMIT
    )


def dot(a, b):
    return lax.dot_general(a, b, (((1,), (0,)), ((), ())), preferred_element_type=F32)


def dot_t(a, b):
    return lax.dot_general(a, b, (((1,), (1,)), ((), ())), preferred_element_type=F32)


def whole(shape):
    return pl.BlockSpec(shape, lambda *_: (0,) * len(shape))


def cuts(count, step):
    return [(at, min(step, count - at)) for at in range(0, count, step)]


def lane_mask(width, head):
    lanes = lax.broadcasted_iota(jnp.int32, (1, width), 1)
    return jnp.where(lanes // HD == head, 1.0, 0.0).astype(BF)


def per_head(block, heads):
    return jnp.concatenate([block * lane_mask(block.shape[1], h) for h in range(heads)], axis=0)


def swap_halves(v):
    out = []
    for at in range(0, v.shape[1], 128):
        part = v[:, at : at + 128]
        lanes = lax.broadcasted_iota(jnp.int32, part.shape, 1)
        out.append(
            jnp.where(
                lanes % HD < HD // 2,
                pltpu.roll(part, 128 - HD // 2, 1),
                pltpu.roll(part, HD // 2, 1),
            )
        )
    return jnp.concatenate(out, axis=1)


def widen(table, width):
    return jnp.concatenate([table] * (width // 128), axis=1)


def cos_sin(angle):
    turns = jnp.round(angle * np.float32(2.0 / np.pi))
    left = angle - turns * np.float32(1.5703125)
    left = left - turns * np.float32(4.837512969970703125e-4)
    left = left - turns * np.float32(7.54978995489188e-8)
    sq = left * left
    sine = left + left * sq * (
        np.float32(-1.6666654611e-1)
        + sq * (np.float32(8.3321608736e-3) + sq * np.float32(-1.9515295891e-4))
    )
    cosine = (
        1.0
        - 0.5 * sq
        + sq
        * sq
        * (
            np.float32(4.166664568298827e-2)
            + sq * (np.float32(-1.388731625493765e-3) + sq * np.float32(2.443315711809948e-5))
        )
    )
    quarter = jnp.bitwise_and(turns.astype(jnp.int32), 3)
    odd = jnp.bitwise_and(quarter, 1) == 1
    sin_out = jnp.where(odd, cosine, sine)
    cos_out = jnp.where(odd, sine, cosine)
    sin_out = jnp.where(quarter >= 2, -sin_out, sin_out)
    cos_out = jnp.where((quarter == 1) | (quarter == 2), -cos_out, cos_out)
    return cos_out, sin_out


def normed(v):
    centered = v - jnp.mean(v, axis=1, keepdims=True)
    var = jnp.mean(centered * centered, axis=1, keepdims=True)
    rstd = lax.rsqrt(var + 1e-05)
    return centered * rstd, rstd


def fold8(v, op):
    return op(v.reshape(v.shape[0] // 8, 8, v.shape[1]), axis=0)


def pair_mask(kcol_ref, rows, codes):
    key = kcol_ref[rows, 3:4]
    low, high, same = codes
    return ((key >= low) & (key < high)) | (key == same)


def query_codes(qrow_ref, at, count):
    cols = pl.ds(at, count)
    return qrow_ref[0:1, cols], qrow_ref[1:2, cols], qrow_ref[2:3, cols]


SUB = 64


def chosen(step, entries):
    value = jnp.int32(entries[0])
    for i, e in enumerate(entries[1:], 1):
        value = jnp.where(step == i, jnp.int32(e), value)
    return value


def attend(step, entries, q_ref, k_ref, vt_ref, kcol_ref, qrow_ref, s_scr, p_scr, heads, chunk):
    blocks = k_ref.shape[0] // chunk
    lq = k_ref.shape[1]
    at = pl.multiple_of(chosen(step, entries) * chunk, chunk)
    codes = query_codes(qrow_ref, at, chunk)
    query = per_head(q_ref[pl.ds(at, chunk), :], heads)

    def score(block, best):
        base = pl.multiple_of(block * chunk, chunk)
        s_scr[pl.ds(base, chunk), :] = dot_t(k_ref[pl.ds(base, chunk), :], query)
        best = list(best)
        for sub in range(0, chunk, SUB):
            rows = pl.ds(base + sub, SUB)
            mask = pair_mask(kcol_ref, rows, codes)
            for h in range(heads):
                cols = slice(h * chunk, (h + 1) * chunk)
                value = jnp.where(mask, s_scr[rows, cols], NEG)
                s_scr[rows, cols] = value
                best[h] = jnp.maximum(best[h], fold8(value, jnp.max))
        return tuple(best)

    best = lax.fori_loop(
        0, blocks, score, tuple(jnp.full((8, chunk), NEG, F32) for _ in range(heads))
    )
    best = [jnp.max(b, axis=0, keepdims=True) for b in best]

    def soften(block, sums):
        base = pl.multiple_of(block * chunk, chunk)
        sums = list(sums)
        for sub in range(0, chunk, SUB):
            rows = pl.ds(base + sub, SUB)
            for h in range(heads):
                cols = slice(h * chunk, (h + 1) * chunk)
                value = jnp.exp(s_scr[rows, cols] - best[h])
                sums[h] = sums[h] + fold8(value, jnp.sum)
                p_scr[rows, cols] = value.astype(BF)
        return tuple(sums)

    sums = lax.fori_loop(
        0, blocks, soften, tuple(jnp.zeros((8, chunk), F32) for _ in range(heads))
    )
    sums = [jnp.sum(s, axis=0, keepdims=True) for s in sums]
    tops = []
    for h in range(heads):
        made = dot(vt_ref[...], p_scr[:, h * chunk : (h + 1) * chunk])
        tops.append(made[h * HD : (h + 1) * HD, :] * (1.0 / sums[h]))
    if heads * HD < lq:
        tops.append(jnp.zeros((lq - heads * HD, chunk), F32))
    logs = [best[h] + jnp.log(sums[h]) for h in range(heads)]
    logs.append(jnp.zeros((8 - heads, chunk), F32))
    return jnp.concatenate(tops, axis=0), jnp.concatenate(logs, axis=0)


def block_outputs(entries, lq, hw, chunk):
    shapes = []
    for _ in entries:
        shapes += [
            jax.ShapeDtypeStruct((chunk, hw), BF),
            jax.ShapeDtypeStruct((lq, chunk), F32),
            jax.ShapeDtypeStruct((8, chunk), F32),
        ]
    return shapes


def store_block(step, entries, refs, joined, logs, hw):
    attended = joined.T[:, :hw].astype(BF)
    for i in range(len(entries)):

        @pl.when(step == i)
        def _(i=i):
            refs[3 * i][...] = attended
            refs[3 * i + 1][...] = joined
            refs[3 * i + 2][...] = logs


def by_block(entries, made):
    return {e: tuple(made[3 * i : 3 * i + 3]) for i, e in enumerate(entries)}


def fill_rows(scr, row, which, labels, vectors, at):
    local = labels[0].shape[1]
    for i, ref in enumerate(labels):
        value = jnp.where(which == 0, ref[0:1, :], ref[1:2, :]).astype(F32)
        scr[row : row + 1, at + local * i : at + local * (i + 1)] = value
    for i, ref in enumerate(vectors):
        scr[row + 1 : row + 2, 128 * i : 128 * i + ref.shape[1]] = ref[...]


def message_rows(place, x, labels, vectors):
    local = x.shape[1]

    def kernel(place_ref, x_ref, *refs):
        label_refs, vector_refs, out_ref, scr = refs[:3], refs[3:7], refs[7], refs[8]
        other = 1 - place_ref[2]
        out_ref[:local, :] = x_ref[other]
        scr[...] = jnp.zeros_like(scr)
        fill_rows(scr, 0, other, label_refs, vector_refs, 0)
        out_ref[local:, :] = scr[...].astype(BF)

    ins = [x] + list(labels) + list(vectors)
    return pl.pallas_call(
        kernel,
        name="message_rows",
        grid_spec=pltpu.PrefetchScalarGridSpec(
            num_scalar_prefetch=1,
            grid=(1,),
            in_specs=[whole(a.shape) for a in ins],
            out_specs=whole((local + 16, D)),
            scratch_shapes=[pltpu.VMEM((16, D), F32)],
        ),
        out_shape=jax.ShapeDtypeStruct((local + 16, D), BF),
        compiler_params=params("arbitrary"),
        cost_estimate=cost(1e6, 1e6),
    )(place, *ins)


def own_rows(place, x, labels, vectors, came):
    local = x.shape[1]

    def kernel(place_ref, x_ref, *refs):
        label_refs, vector_refs, came_ref, out_ref, scr = refs[:3], refs[3:7], *refs[7:]
        own = place_ref[2]
        out_ref[:local, :] = x_ref[own]
        out_ref[local : 2 * local, :] = came_ref[:local, :]
        scr[...] = jnp.zeros_like(scr)
        fill_rows(scr, 0, own, label_refs, vector_refs, 0)
        extra = came_ref[local:, :].astype(F32)
        scr[0:1, 3 * local : 6 * local] = extra[0:1, : 3 * local]
        scr[2:3, :] = extra[1:2, :]
        out_ref[2 * local :, :] = scr[...].astype(BF)

    ins = [x] + list(labels) + list(vectors) + [came]
    return pl.pallas_call(
        kernel,
        name="own_rows",
        grid_spec=pltpu.PrefetchScalarGridSpec(
            num_scalar_prefetch=1,
            grid=(1,),
            in_specs=[whole(a.shape) for a in ins],
            out_specs=whole((2 * local + 16, D)),
            scratch_shapes=[pltpu.VMEM((16, D), F32)],
        ),
        out_shape=jax.ShapeDtypeStruct((2 * local + 16, D), BF),
        compiler_params=params("arbitrary"),
        cost_estimate=cost(1e6, 1e6),
    )(place, *ins)


def attention_first(place, arrays, plan, extras, freq, wq, order, heads, chunk, entries, widths):
    blocks = len(extras)
    total = blocks * chunk
    local = chunk // 2
    hw = heads * HD
    lq = -(-hw // 128) * 128
    count = len(arrays)
    parts = len(wq)
    n_w, b_w = widths
    fixed = 11

    def kernel(place_ref, *refs):
        x_refs = refs[:count]
        freq_ref, order_ref = refs[count : count + 2]
        wq_refs = refs[count + 2 : count + 2 + parts]
        outs = refs[count + 2 + parts :]
        h1_ref, q_ref, k_ref, v_ref, vt_ref, cs_ref, sn_ref, kcol_ref, qrow_ref, gain_ref, wq_ref = (
            outs[:fixed]
        )
        bias_ref = outs[fixed]
        block_refs = outs[fixed + 1 : fixed + 1 + 3 * len(entries)]
        s_scr, p_scr, g_scr = outs[fixed + 1 + 3 * len(entries) :]
        step = pl.program_id(0)
        d, c = place_ref[0], place_ref[2]

        @pl.when(step == 0)
        def _():
            g_scr[...] = jnp.zeros_like(g_scr)
            bias_ref[...] = jnp.zeros_like(bias_ref)
            turn = lax.broadcasted_iota(jnp.int32, (1, chunk), 1) % BLK
            for k, (which, at) in enumerate(extras):
                rows = x_refs[which][at : at + 16, :].astype(F32)

                def label(i, rows=rows):
                    return jnp.concatenate(
                        [
                            rows[0:1, i * local : (i + 1) * local],
                            rows[0:1, (3 + i) * local : (4 + i) * local],
                        ],
                        axis=1,
                    )

                segment, flag, block = label(0), label(1), label(2)
                start = segment * 4096.0
                clean = flag > 0.5
                key = start + jnp.where(clean, block, block + 2048.0)
                place_now = block * BLK + turn.astype(F32)
                coded = jnp.concatenate(
                    [
                        start,
                        start + block + flag,
                        jnp.where(clean, -1.0, key),
                        key,
                        place_now,
                        jnp.zeros((3, chunk), F32),
                    ],
                    axis=0,
                )
                qrow_ref[:, k * chunk : (k + 1) * chunk] = coded
                kcol_ref[k * chunk : (k + 1) * chunk, :] = coded.T
                for half in range(2):
                    vector = rows[1 + half : 2 + half, :]
                    lane = 384 * half + n_w * k
                    for i in range(3):
                        g_scr[i : i + 1, lane : lane + n_w] = vector[:, 128 * i : 128 * i + n_w]
                if parts == 2:
                    bias_ref[k : k + 1, :b_w] = rows[1:2, 384 : 384 + b_w]
            gain_ref[...] = dot_t(g_scr[...].astype(BF), order_ref[...])
            if parts == 2:
                for half in range(2):

                    @pl.when(c == half)
                    def _(half=half):
                        for j in range(4):
                            rows = slice(192 * j, 192 * j + 192)
                            for t in range(3):
                                for i in range(2):
                                    at = lq * t + 96 * (i ^ half)
                                    wq_ref[rows, at : at + 96] = wq_refs[i][
                                        d ^ j, :, 96 * t : 96 * t + 96
                                    ]

                for t in range(3):
                    if hw < lq:
                        wq_ref[:, lq * t + hw : lq * (t + 1)] = jnp.zeros((D, lq - hw), BF)
            else:
                wq_ref[...] = wq_refs[0][...]
            gain_row = gain_ref[0:1, :]
            for which, src, dst, rows in plan:
                for at, size in cuts(rows, 64):
                    xhat, _ = normed(x_refs[which][src + at : src + at + size, :].astype(F32))
                    h1_ref[dst + at : dst + at + size, :] = (xhat * gain_row).astype(BF)
            lanes = lax.broadcasted_iota(jnp.int32, (1, 128), 1)
            sign = jnp.where(lanes % HD < HD // 2, -1.0, 1.0)

            def project(block, carry):
                rows = pl.ds(pl.multiple_of(block * chunk, chunk), chunk)
                cosine, sine = cos_sin(kcol_ref[rows, 4:5] * freq_ref[...])
                sine = sine * sign
                cs_ref[rows, :] = cosine
                sn_ref[rows, :] = sine
                cosine = widen(cosine, lq)
                sine = widen(sine, lq)
                made = dot(h1_ref[rows, :], wq_ref[...])
                q = made[:, :lq]
                q_ref[rows, :] = ((q * cosine + swap_halves(q) * sine).astype(BF) * 0.125).astype(
                    BF
                )
                k = made[:, lq : 2 * lq]
                k_ref[rows, :] = (k * cosine + swap_halves(k) * sine).astype(BF)
                v = made[:, 2 * lq :]
                v_ref[rows, :] = v.astype(BF)
                vt_ref[:, rows] = v.T.astype(BF)
                return carry

            lax.fori_loop(0, blocks, project, 0)

        joined, logs = attend(
            step, entries, q_ref, k_ref, vt_ref, kcol_ref, qrow_ref, s_scr, p_scr, heads, chunk
        )
        store_block(step, entries, block_refs, joined, logs, hw)

    ins = list(arrays) + [freq, order] + list(wq)
    out_shape = [
        jax.ShapeDtypeStruct((total, D), BF),
        jax.ShapeDtypeStruct((total, lq), BF),
        jax.ShapeDtypeStruct((total, lq), BF),
        jax.ShapeDtypeStruct((total, lq), BF),
        jax.ShapeDtypeStruct((lq, total), BF),
        jax.ShapeDtypeStruct((total, 128), F32),
        jax.ShapeDtypeStruct((total, 128), F32),
        jax.ShapeDtypeStruct((total, 8), F32),
        jax.ShapeDtypeStruct((8, total), F32),
        jax.ShapeDtypeStruct((16, D), F32),
        jax.ShapeDtypeStruct((D, 3 * lq), BF),
        jax.ShapeDtypeStruct((-(-blocks // 8) * 8, 384), F32),
    ] + block_outputs(entries, lq, hw, chunk)
    made = pl.pallas_call(
        kernel,
        name="attention_first",
        grid_spec=pltpu.PrefetchScalarGridSpec(
            num_scalar_prefetch=1,
            grid=(len(entries),),
            in_specs=[whole(v.shape) for v in ins],
            out_specs=[whole(o.shape) for o in out_shape],
            scratch_shapes=[
                pltpu.VMEM((total, heads * chunk), F32),
                pltpu.VMEM((total, heads * chunk), BF),
                pltpu.VMEM((16, D), F32),
            ],
        ),
        out_shape=out_shape,
        compiler_params=params("arbitrary"),
        cost_estimate=cost(8e9, 8e6),
    )(place, *ins)
    return made[:12], by_block(entries, made[12:])


def attention_rest(saved, heads, chunk, entries):
    q, k, vt, kcol, qrow = saved
    total, lq = k.shape
    hw = heads * HD

    def kernel(q_ref, k_ref, vt_ref, kcol_ref, qrow_ref, *refs):
        step = pl.program_id(0)
        s_scr, p_scr = refs[3 * len(entries) :]
        joined, logs = attend(
            step, entries, q_ref, k_ref, vt_ref, kcol_ref, qrow_ref, s_scr, p_scr, heads, chunk
        )
        store_block(step, entries, refs, joined, logs, hw)

    ins = [q, k, vt, kcol, qrow]
    out_shape = block_outputs(entries, lq, hw, chunk)
    made = pl.pallas_call(
        kernel,
        name="attention_rest",
        grid=(len(entries),),
        in_specs=[whole(v.shape) for v in ins],
        out_specs=[whole(o.shape) for o in out_shape],
        out_shape=out_shape,
        scratch_shapes=[
            pltpu.VMEM((total, heads * chunk), F32),
            pltpu.VMEM((total, heads * chunk), BF),
        ],
        compiler_params=params("arbitrary"),
        cost_estimate=cost(5e9, 4e6),
    )(*ins)
    return by_block(entries, made)


def attention_backward(pulls, by, saved, heads, chunk, entries, before, finish):
    h1, q, k, v, _, cs, sn, kcol, qrow, gains, wq = saved[:11]
    last = finish is not None
    total, lq = k.shape
    blocks = total // chunk
    hw = heads * HD
    n = len(entries)
    halves = blocks == 4
    pieces = blocks + 1 if halves else blocks

    def kernel(*refs):
        g_refs, att_refs, lse_refs = refs[:n], refs[n : 2 * n], refs[2 * n : 3 * n]
        q_ref, k_ref, v_ref, cs_ref, sn_ref, kcol_ref, qrow_ref = refs[3 * n : 3 * n + 7]
        refs = refs[3 * n + 7 :]
        if last:
            dq_in, dk_in, dv_in, wq_ref, h1_ref, gains_ref, sums_ref, order_ref = refs[:8]
            gqkv_ref, keep_ref, send_ref = refs[8:11]
            gh_refs = refs[11 : 11 + pieces]
            scr = refs[11 + pieces :]
        else:
            dq_out, dk_out, dv_out = refs[:3]
            scr = refs[3:]
        g_scr, row_scr, kt_scr, dk_scr, dv_scr, s_scr, dp_scr, pb_scr, ds_scr, dst_scr = scr
        step = pl.program_id(0)

        @pl.when(step == 0)
        def _():
            for i in range(n):
                g_scr[i, :, :hw] = g_refs[i][...]
                if hw < lq:
                    g_scr[i, :, hw:] = jnp.zeros((chunk, lq - hw), BF)
                product = g_scr[i].astype(F32).T * att_refs[i][...]
                for h in range(heads):
                    row_scr[i, h : h + 1, :] = jnp.sum(
                        product[h * HD : (h + 1) * HD, :], axis=0, keepdims=True
                    )
                row_scr[i, 8:16, :] = lse_refs[i][...]
            if last:
                dk_scr[...] = dk_in[...]
                dv_scr[...] = dv_in[...]
            else:
                dk_scr[...] = jnp.zeros_like(dk_scr)
                dv_scr[...] = jnp.zeros_like(dv_scr)

            def turn(block, carry):
                rows = pl.ds(pl.multiple_of(block * chunk, chunk), chunk)
                flat = k_ref[rows, :].astype(F32).T
                line = lax.broadcasted_iota(jnp.int32, (lq, 1), 0) // HD
                for h in range(heads):
                    kt_scr[block, :, h * chunk : (h + 1) * chunk] = jnp.where(
                        line == h, flat, 0.0
                    ).astype(BF)
                return carry

            lax.fori_loop(0, blocks, turn, 0)

        at = pl.multiple_of(chosen(step, entries) * chunk, chunk)
        own = pl.ds(at, chunk)
        codes = query_codes(qrow_ref, at, chunk)
        query = per_head(q_ref[own, :], heads)
        pull = per_head(g_scr[step], heads)
        delta = [row_scr[step, h : h + 1, :] for h in range(heads)]
        top = [row_scr[step, 8 + h : 9 + h, :] for h in range(heads)]

        def keys(block, dq_t):
            base = pl.multiple_of(block * chunk, chunk)
            rows = pl.ds(base, chunk)
            s_scr[...] = dot_t(k_ref[rows, :], query)
            dp_scr[...] = dot_t(v_ref[rows, :], pull)
            for sub in range(0, chunk, SUB):
                part = slice(sub, sub + SUB)
                mask = pair_mask(kcol_ref, pl.ds(base + sub, SUB), codes)
                for h in range(heads):
                    cols = slice(h * chunk, (h + 1) * chunk)
                    prob = jnp.exp(jnp.where(mask, s_scr[part, cols] - top[h], NEG))
                    slope = (prob * (dp_scr[part, cols] - delta[h])).astype(BF)
                    pb_scr[part, cols] = prob.astype(BF)
                    ds_scr[part, cols] = slope
                    dst_scr[h * chunk + sub : h * chunk + sub + SUB, :] = slope
            dv_scr[rows, :] += dot(pb_scr[...], pull)
            dk_scr[rows, :] += dot(ds_scr[...], query)
            return dq_t + dot(kt_scr[block], dst_scr[...])

        dq_t = lax.fori_loop(0, blocks, keys, jnp.zeros((lq, chunk), F32))

        def unrotate(value, rows):
            return value * widen(cs_ref[rows, :], lq) - swap_halves(value) * widen(
                sn_ref[rows, :], lq
            )

        dq = unrotate(dq_t.T * 0.125, own).astype(BF)
        if not last:
            dq_out[...] = dq

            @pl.when(step == n - 1)
            def _():
                dk_out[...] = dk_scr[...]
                dv_out[...] = dv_scr[...]

        else:
            gqkv_ref[own, :lq] = dq

            @pl.when(step == n - 1)
            def _():
                gqkv_ref[0:chunk, :lq] = dq_in[...]
                n1 = jnp.zeros((8, D), F32)
                for b in range(blocks):
                    rows = slice(b * chunk, (b + 1) * chunk)
                    gqkv_ref[rows, lq : 2 * lq] = unrotate(dk_scr[rows, :], rows).astype(BF)
                    gqkv_ref[rows, 2 * lq :] = dv_scr[rows, :].astype(BF)
                    gh = dot_t(gqkv_ref[rows, :], wq_ref[...])
                    if halves and b == 2:
                        gh_refs[2][...] = gh[: chunk // 2, :].astype(BF)
                        gh_refs[4][...] = gh[chunk // 2 :, :].astype(BF)
                    else:
                        gh_refs[b][...] = gh.astype(gh_refs[b].dtype)
                    n1 = n1 + fold8(gh * h1_ref[rows, :].astype(F32), jnp.sum)
                lines = [
                    jnp.sum(n1, axis=0, keepdims=True) / gains_ref[0:1, :],
                    jnp.sum(sums_ref[0:8, :], axis=0, keepdims=True),
                    jnp.sum(sums_ref[8:16, :], axis=0, keepdims=True),
                    jnp.zeros((13, D), F32),
                ]
                lines = jnp.concatenate(lines, axis=0)
                high = lines.astype(BF)
                rest = (lines - high.astype(F32)).astype(BF)
                lines = dot(high, order_ref[...]) + dot(rest, order_ref[...])
                keep_ref[...] = lines[:, :384]
                send_ref[...] = lines[:, 384:]

    ins = [pulls[e] for e in entries] + [by[e][1] for e in entries] + [by[e][2] for e in entries]
    ins += [q, k, v, cs, sn, kcol, qrow]
    if last:
        ins += list(before) + [wq, h1, gains] + list(finish)
        out_shape = [
            jax.ShapeDtypeStruct((total, 3 * lq), BF),
            jax.ShapeDtypeStruct((16, 384), F32),
            jax.ShapeDtypeStruct((16, 384), F32),
        ]
        for b in range(pieces):
            rows = chunk // 2 if halves and b in (2, 4) else chunk
            out_shape.append(jax.ShapeDtypeStruct((rows, D), F32 if b == 0 else BF))
    else:
        out_shape = [
            jax.ShapeDtypeStruct((chunk, lq), BF),
            jax.ShapeDtypeStruct((total, lq), F32),
            jax.ShapeDtypeStruct((total, lq), F32),
        ]
    return pl.pallas_call(
        kernel,
        name="attention_backward_last" if last else "attention_backward_own",
        grid=(n,),
        in_specs=[whole(a.shape) for a in ins],
        out_specs=[whole(o.shape) for o in out_shape],
        out_shape=out_shape,
        scratch_shapes=[
            pltpu.VMEM((n, chunk, lq), BF),
            pltpu.VMEM((n, 16, chunk), F32),
            pltpu.VMEM((blocks, lq, heads * chunk), BF),
            pltpu.VMEM((total, lq), F32),
            pltpu.VMEM((total, lq), F32),
            pltpu.VMEM((chunk, heads * chunk), F32),
            pltpu.VMEM((chunk, heads * chunk), F32),
            pltpu.VMEM((chunk, heads * chunk), BF),
            pltpu.VMEM((chunk, heads * chunk), BF),
            pltpu.VMEM((heads * chunk, chunk), BF),
        ],
        compiler_params=params("arbitrary"),
        cost_estimate=cost(3e9 * n, 1e7),
    )(*ins)


def dot_first(a, b):
    return lax.dot_general(a, b, (((0,), (0,)), ((), ())), preferred_element_type=F32)


def reorder_out(place, own, other, order):
    def kernel(place_ref, own_ref, other_ref, order_ref, out_ref, scr):
        d = place_ref[0]
        for j in range(4):
            for k in range(4):
                at = 96 * k
                part = slice(96 * j, 96 * j + 96)
                scr[j, :, at : at + 96] = own_ref[k, :, part]
                scr[j, :, 384 + at : 384 + at + 96] = other_ref[k, :, part]
        for j in range(4):
            out_ref[j] = dot_t(scr[d ^ j], order_ref[...]).astype(BF)

    return pl.pallas_call(
        kernel,
        name="reorder_out",
        grid_spec=pltpu.PrefetchScalarGridSpec(
            num_scalar_prefetch=1,
            grid=(1,),
            in_specs=[whole(own.shape), whole(other.shape), whole(order.shape)],
            out_specs=whole((4, 192, D)),
            scratch_shapes=[pltpu.VMEM((4, 192, 768), BF)],
        ),
        out_shape=jax.ShapeDtypeStruct((4, 192, D), BF),
        compiler_params=params("arbitrary"),
        cost_estimate=cost(1e9, 3e6),
    )(place, own, other, order)


def qkv_weight(place, h1_t, gqkv, order):
    def kernel(place_ref, h_ref, g_ref, order_ref, keep_ref, send_ref):
        d = place_ref[0]
        made = dot(h_ref[...], g_ref[...]).astype(BF)
        made = dot(made, order_ref[...]).astype(BF)
        for j in range(4):
            rows = slice(192 * j, 192 * j + 192)
            keep_ref[d ^ j] = made[rows, :288]
            send_ref[d ^ j] = made[rows, 384:672]

    shape = jax.ShapeDtypeStruct((4, 192, 288), BF)
    return pl.pallas_call(
        kernel,
        name="qkv_weight",
        grid_spec=pltpu.PrefetchScalarGridSpec(
            num_scalar_prefetch=1,
            grid=(1,),
            in_specs=[whole(h1_t.shape), whole(gqkv.shape), whole(order.shape)],
            out_specs=[whole(shape.shape)] * 2,
        ),
        out_shape=[shape, shape],
        compiler_params=params("arbitrary"),
        cost_estimate=cost(2e9, 5e6),
    )(place, h1_t, gqkv, order)


def out_weight(place, mixed, gproj, order):
    groups = len(mixed)

    def kernel(place_ref, *refs):
        m_refs = refs[:groups]
        g_ref, order_ref, keep_ref, send_ref = refs[groups:]
        d, z = place_ref[0], place_ref[1]
        for k in range(groups):
            made = dot_first(m_refs[k][...], g_ref[...]).astype(BF)
            made = dot(made, order_ref[...]).astype(BF)
            row = d ^ lax.rem(z + (groups - k), groups)
            keep_ref[row] = made[:, :384]
            send_ref[row] = made[:, 384:]

    ins = list(mixed) + [gproj, order]
    shape = jax.ShapeDtypeStruct((4, 192, 384), BF)
    return pl.pallas_call(
        kernel,
        name="out_weight",
        grid_spec=pltpu.PrefetchScalarGridSpec(
            num_scalar_prefetch=1,
            grid=(1,),
            in_specs=[whole(a.shape) for a in ins],
            out_specs=[whole(shape.shape)] * 2,
        ),
        out_shape=[shape, shape],
        compiler_params=params("arbitrary"),
        cost_estimate=cost(1e9, 4e6),
    )(place, *ins)


def output_projection(place, mixed, wout, x, gain):
    groups = len(mixed)
    rows = mixed[0].shape[0]

    def kernel(place_ref, *refs):
        m_refs = refs[:groups]
        w_ref, x_ref, gain_ref, res_ref, h2_ref = refs[groups:]
        z = place_ref[1]
        total = x_ref[:rows, :].astype(F32)
        for k in range(groups):
            total = total + dot(m_refs[k][...], w_ref[lax.rem(z + (groups - k), groups)])
        res_ref[...] = total
        for at, size in cuts(rows, 64):
            xhat, _ = normed(res_ref[at : at + size, :])
            h2_ref[at : at + size, :] = (xhat * gain_ref[1:2, :]).astype(BF)

    ins = list(mixed) + [wout, x, gain]
    return pl.pallas_call(
        kernel,
        name="output_projection",
        grid_spec=pltpu.PrefetchScalarGridSpec(
            num_scalar_prefetch=1,
            grid=(1,),
            in_specs=[whole(a.shape) for a in ins],
            out_specs=[whole((rows, D)), whole((rows, D))],
        ),
        out_shape=[jax.ShapeDtypeStruct((rows, D), F32), jax.ShapeDtypeStruct((rows, D), BF)],
        compiler_params=params("arbitrary"),
        cost_estimate=cost(1e9, 3e6),
    )(place, *ins)


def feed_forward(place, h2_own, h2_other, cot, cot_in, weights, bias):
    rows = h2_own.shape[0]
    both = 2 * rows
    width = 384

    def kernel(
        place_ref, ho_ref, hp_ref, go_ref, gp_ref, w1a_ref, w1b_ref, w2a_ref, w2b_ref, b_ref,
        out_own, out_other, gh_own, gh_other, d1a_ref, d1b_ref, d2a_ref, d2b_ref, db_ref,
        h_scr, g_scr, ht_scr, gt_scr, w1_scr, w2_scr, pre_scr, ga_scr, act_scr, slope_scr, out_scr,
        gh_scr, dw_scr,
    ):
        step = pl.program_id(0)
        d = place_ref[0]
        z = place_ref[1]
        c = place_ref[2]

        @pl.when(step == 0)
        def _():
            h_scr[:rows, :] = ho_ref[...]
            h_scr[rows:, :] = hp_ref[...]
            local = rows // 2
            g_scr[:local, :] = go_ref[c]
            g_scr[local:rows, :] = gp_ref[c]
            g_scr[rows : rows + local, :] = gp_ref[1 - c]
            g_scr[rows + local :, :] = go_ref[1 - c]
            for at in range(0, both, 256):
                part = slice(at, at + 256)
                ht_scr[:, part] = h_scr[part, :].astype(F32).T.astype(BF)
                gt_scr[:, part] = g_scr[part, :].astype(F32).T.astype(BF)

        near = lax.rem(step - z + 4, 4)
        hidden = step ^ d
        for odd in range(2):

            @pl.when(d % 2 == odd)
            def _(odd=odd):
                for j in range(4):
                    src = (w1a_ref, w1b_ref)[odd ^ (j % 2)]
                    w1_scr[192 * j : 192 * j + 192, :] = src[(d ^ j) // 2, near]

            @pl.when(hidden // 2 == odd)
            def _(odd=odd):
                for j in range(4):
                    src = (w2a_ref, w2b_ref)[odd]
                    w2_scr[192 * j : 192 * j + 192, :] = src[hidden % 2, lax.rem(j - z + 4, 4)]

        pre_scr[...] = dot(h_scr[...], w1_scr[...])
        ga_scr[...] = dot(g_scr[...], w2_scr[...])
        bias_row = b_ref[pl.ds(near, 1), :]
        total = jnp.zeros((8, width), F32)
        for at in range(0, both, 32):
            part = slice(at, at + 32)
            u = pre_scr[part, :] + bias_row
            usq = u * u
            c = np.float32(np.sqrt(2.0 / np.pi))
            t = jnp.tanh(c * (u + np.float32(0.044715) * (usq * u)))
            half = 0.5 * (1.0 + t)
            act_scr[part, :] = (u * half).astype(BF)
            rise = half + 0.5 * u * (1.0 - t * t) * (c * (1.0 + np.float32(0.134145) * usq))
            slope = (ga_scr[part, :] * rise).astype(BF)
            slope_scr[part, :] = slope
            total = total + fold8(slope.astype(F32), jnp.sum)
        db_ref[0] = jnp.sum(total, axis=0, keepdims=True)

        out_now = dot_t(act_scr[...], w2_scr[...])
        gh_now = dot_t(slope_scr[...], w1_scr[...])

        @pl.when(step == 0)
        def _():
            out_scr[...] = out_now
            gh_scr[...] = gh_now

        @pl.when(step > 0)
        def _():
            out_scr[...] += out_now
            gh_scr[...] += gh_now

        dw_scr[0] = dot(ht_scr[...], slope_scr[...]).astype(BF)
        dw_scr[1] = dot(gt_scr[...], act_scr[...]).astype(BF)
        for odd in range(2):

            @pl.when(d % 2 == odd)
            def _(odd=odd):
                for j in range(4):
                    dst = (d1a_ref, d1b_ref)[odd ^ (j % 2)]
                    dst[(d ^ j) // 2, near] = dw_scr[0, 192 * j : 192 * j + 192, :]

            @pl.when(hidden // 2 == odd)
            def _(odd=odd):
                for j in range(4):
                    dst = (d2a_ref, d2b_ref)[odd]
                    dst[hidden % 2, lax.rem(j - z + 4, 4)] = dw_scr[1, 192 * j : 192 * j + 192, :]

        @pl.when(step == 3)
        def _():
            out_own[...] = out_scr[:rows, :]
            out_other[...] = out_scr[rows:, :].astype(BF)
            gh_own[...] = gh_scr[:rows, :]
            gh_other[...] = gh_scr[rows:, :].astype(BF)

    def by_z(i, place_ref):
        return (lax.rem(i - place_ref[1] + 4, 4), 0, 0)

    ins = [h2_own, h2_other, cot, cot_in] + list(weights) + [bias]
    full = jax.ShapeDtypeStruct((2, 4, 192, width), BF)
    out_shape = [
        jax.ShapeDtypeStruct((rows, D), F32),
        jax.ShapeDtypeStruct((rows, D), BF),
        jax.ShapeDtypeStruct((rows, D), F32),
        jax.ShapeDtypeStruct((rows, D), BF),
        full,
        full,
        full,
        full,
        jax.ShapeDtypeStruct((4, 1, width), F32),
    ]
    return pl.pallas_call(
        kernel,
        name="feed_forward",
        grid_spec=pltpu.PrefetchScalarGridSpec(
            num_scalar_prefetch=1,
            grid=(4,),
            in_specs=[whole(a.shape) for a in ins],
            out_specs=[whole(o.shape) for o in out_shape[:-1]]
            + [pl.BlockSpec((1, 1, width), by_z)],
            scratch_shapes=[
                pltpu.VMEM((both, D), BF),
                pltpu.VMEM((both, D), BF),
                pltpu.VMEM((D, both), BF),
                pltpu.VMEM((D, both), BF),
                pltpu.VMEM((D, width), BF),
                pltpu.VMEM((D, width), BF),
                pltpu.VMEM((both, width), F32),
                pltpu.VMEM((both, width), F32),
                pltpu.VMEM((both, width), BF),
                pltpu.VMEM((both, width), BF),
                pltpu.VMEM((both, D), F32),
                pltpu.VMEM((both, D), F32),
                pltpu.VMEM((2, D, width), BF),
            ],
        ),
        out_shape=out_shape,
        compiler_params=params("arbitrary"),
        cost_estimate=cost(7.2e9, 1.5e7),
    )(place, *ins)


def residual_backward(place, gh_own, gh_in, residual, cot, cot_in, gain, wout):
    rows, local = residual.shape[0], cot.shape[1]
    groups, hw = wout.shape[0], wout.shape[1]

    def kernel(place_ref, gh_ref, gi_ref, res_ref, ca_ref, cb_ref, gain_ref, w_ref, *outs):
        gres_ref, gproj_ref, vec_ref = outs[:3]
        gm_refs = outs[3:]
        z, c = place_ref[1], place_ref[2]
        gain_row = gain_ref[1:2, :]
        gsum = jnp.zeros((8, D), F32)
        bsum = jnp.zeros((8, D), F32)
        for at, size in cuts(rows, 32):
            part = slice(at, at + size)
            xhat, rstd = normed(res_ref[part, :])
            dy_now = (ca_ref, cb_ref)[at // local][c, at % local : at % local + size, :].astype(F32)
            grad = gh_ref[part, :] + gi_ref[part, :].astype(F32)
            along = grad * xhat
            gsum = gsum + fold8(along, jnp.sum)
            bsum = bsum + fold8(dy_now, jnp.sum)
            u = grad * gain_row
            back = (
                u
                - jnp.mean(u, axis=1, keepdims=True)
                - xhat * jnp.mean(along * gain_row, axis=1, keepdims=True)
            )
            value = dy_now + back * rstd
            gres_ref[part, :] = value
            gproj_ref[part, :] = value.astype(BF)
        vec_ref[0:8, :] = gsum
        vec_ref[8:16, :] = bsum
        for k in range(groups):
            gm_refs[k][...] = dot_t(gproj_ref[...], w_ref[lax.rem(z + k, groups)]).astype(BF)

    ins = [gh_own, gh_in, residual, cot, cot_in, gain, wout]
    out_shape = [
        jax.ShapeDtypeStruct((rows, D), F32),
        jax.ShapeDtypeStruct((rows, D), BF),
        jax.ShapeDtypeStruct((16, D), F32),
    ] + [jax.ShapeDtypeStruct((rows, hw), BF) for _ in range(groups)]
    made = pl.pallas_call(
        kernel,
        name="residual_backward",
        grid_spec=pltpu.PrefetchScalarGridSpec(
            num_scalar_prefetch=1,
            grid=(1,),
            in_specs=[whole(a.shape) for a in ins],
            out_specs=[whole(o.shape) for o in out_shape],
        ),
        out_shape=out_shape,
        compiler_params=params("arbitrary"),
        cost_estimate=cost(1e9, 4e6),
    )(place, *ins)
    return made[0], made[1], made[2], made[3:]


def input_backward(terms, x, gain, gres):
    rows = gres.shape[0]
    count = len(terms)

    def kernel(*refs):
        x_ref, gain_ref, gres_ref, out_ref = refs[count:]
        for at, size in cuts(rows, 32):
            part = slice(at, at + size)
            grad = refs[0][part, :].astype(F32)
            for t in range(1, count):
                grad = grad + refs[t][part, :].astype(F32)
            xhat, rstd = normed(x_ref[part, :].astype(F32))
            u = grad * gain_ref[0:1, :]
            back = (
                u
                - jnp.mean(u, axis=1, keepdims=True)
                - xhat * jnp.mean(u * xhat, axis=1, keepdims=True)
            )
            out_ref[part, :] = (gres_ref[part, :] + back * rstd).astype(BF)

    ins = list(terms) + [x, gain, gres]
    return pl.pallas_call(
        kernel,
        name="input_backward",
        grid=(1,),
        in_specs=[whole(a.shape) for a in ins],
        out_specs=whole((rows, D)),
        out_shape=jax.ShapeDtypeStruct((rows, D), BF),
        compiler_params=params("arbitrary"),
        cost_estimate=cost(1e8, 3e6),
    )(*ins)


def add_low(a, b):
    return (a.astype(F32) + b.astype(F32)).astype(BF)


def pick(v, index):
    return lax.dynamic_index_in_dim(v, index, 0, keepdims=False)


def after(v, *others):
    return lax.optimization_barrier((v, others))[0]


class Links:
    def __init__(self, n_dp, n_seq):
        self.n_dp, self.n_seq, self.nz = n_dp, n_seq, n_seq // 2

    def core(self, v):
        return lax.ppermute(v, "seq", [(s, s ^ 1) for s in range(self.n_seq)])

    def flip(self, v, bit):
        return lax.ppermute(v, "dp", [(i, i ^ bit) for i in range(self.n_dp)])

    def shift(self, v, k):
        n = self.nz
        return lax.ppermute(
            v, "seq", [(s, 2 * ((s // 2 + k) % n) + s % 2) for s in range(self.n_seq)]
        )


def order_matrix(source, valid):
    rows = lax.broadcasted_iota(jnp.int32, (768, 768), 0)
    return jnp.where((rows == source[None, :]) & valid[None, :], 1.0, 0.0).astype(BF)


def per_device(
    n_dp,
    n_seq,
    inputs,
    row_segment,
    row_flag,
    row_block,
    norm1_scale,
    w_qkv,
    w_out,
    norm2_scale,
    w_fc1,
    b_fc1,
    w_fc2,
    b_fc2,
    cotangent,
):
    links = Links(n_dp, n_seq)
    nz = links.nz
    local = inputs.shape[2]
    chunk = 2 * local
    heads = -(-H // nz)
    hw = heads * HD
    lq = -(-hw // 128) * 128
    fast = n_dp == 4 and nz == 4 and H % nz == 0
    d = lax.axis_index("dp")
    s = lax.axis_index("seq")
    z = s // 2
    c = s % 2
    place = jnp.stack([d, z, c]).astype(jnp.int32)
    n_w, b_w = D // n_seq, FF // n_seq
    cols = jnp.arange(768, dtype=jnp.int32)
    side, at = cols // 384, cols % 384
    out_order = order_matrix(
        n_w * (2 * ((z + at // n_w) % nz) + (c ^ side)) + at % n_w, at < 384
    )

    def to_both(w):
        return jnp.where(c == 0, w[0], w[1]), jnp.where(c == 0, w[1], w[0])

    x_loc = inputs[:, 0]
    labels = (row_segment[:, 0], row_flag[:, 0], row_block[:, 0])
    vectors = tuple(v.reshape(1, -1) for v in (norm1_scale, norm2_scale, b_fc2, b_fc1))
    came = links.core(message_rows(place, x_loc, labels, vectors))
    x_ext = own_rows(place, x_loc, labels, vectors, came)
    if nz == 4:
        x_before = links.shift(x_ext, 1)
        x_after = links.shift(x_ext, -1)
        x_low = links.shift(x_before[:144], 1)
        x_high = links.shift(x_after[144:], -1)
        gathered = [[x_ext], [x_after], [x_low, x_high], [x_before]]
    else:
        gathered = [[x_ext]] + [[links.shift(x_ext, -k)] for k in range(1, nz)]
    arrays, plan, extras = [], [], []
    for k, pieces in enumerate(gathered):
        at = 0
        for piece in pieces:
            rows = min(piece.shape[0], chunk - at)
            plan.append((len(arrays), 0, k * chunk + at, rows))
            at += rows
            arrays.append(piece)
        extras.append((len(arrays) - 1, pieces[-1].shape[0] - 16))
    freq = np.tile(
        np.float32(10000.0) ** (np.float32(-2.0) * np.arange(32, dtype=np.float32) / HD), 4
    )
    freq = jnp.asarray(freq.astype(np.float32)[None, :])
    cot = cotangent[:, 0]

    if fast:
        two = w_fc2.astype(BF).T.reshape(96, 2, 384)
        two_keep, two_send = to_both((two[:, 0], two[:, 1]))
        two = jnp.concatenate(to_both((two_keep, links.core(two_send))), axis=0)
        w12 = jnp.stack([w_fc1.astype(BF), two])
        w_before = links.shift(w12, 1)
        w_after = links.shift(w12, -1)
        w1_two = links.shift(w_before[0], 1)
        w2_two = links.shift(w_after[1], -1)
        w1 = jnp.stack([w12[0], w_after[0], w1_two, w_before[0]])
        w2 = jnp.stack([w12[1], w_after[1], w2_two, w_before[1]])

        qkv_order = order_matrix(
            256 * (cols % 384 // 96) + 96 * (c ^ side) + cols % 96, cols % 384 < 288
        )
        wq_parts = after(w_qkv.astype(BF), x_ext)
        parts = []
        for i in range(3):
            parts.append(
                lax.ppermute(
                    wq_parts[:, 96 * i : 96 * i + 96],
                    "seq",
                    [(q, (3 * q + i) % 8) for q in range(8)],
                )
            )
        parts = jnp.stack(parts)
        wq_own = jnp.concatenate(
            [pick(parts, (2 * t + s) % 3) for t in range(3)] + [w_out.astype(BF)], axis=1
        )
        wq_own = jnp.stack([wq_own, links.flip(wq_own, 1)])
        wq_own = jnp.stack([wq_own, links.flip(wq_own, 2)]).reshape(4, 192, 384)
        wq = (wq_own, links.core(wq_own))
        wo_own = jnp.concatenate([wq_own[j, :, 288:] for j in range(4)], axis=1)

        x_ext_late, _ = lax.optimization_barrier((arrays[0], (w1, w2, wo_own)))
        arrays[0] = x_ext_late
        w1_in = links.flip(w1, 2)
        w2_in = links.flip(w2, 1)
        wo_all = [wo_own] + [links.shift(wo_own, -k) for k in range(1, 4)]
        ff_place = place
    else:

        def everywhere(w):
            w = lax.all_gather(w.astype(BF), "seq", axis=1, tiled=True)
            return lax.all_gather(w, "dp", axis=0, tiled=True)

        wq = everywhere(w_qkv).reshape(D, 3, D)
        wq = jnp.pad(wq, ((0, 0), (0, 0), (0, nz * hw - D)))
        wq = lax.dynamic_slice_in_dim(wq, z * hw, hw, 2)
        wq = (jnp.pad(wq, ((0, 0), (0, 0), (0, lq - hw))).reshape(D, 3 * lq),)
        wout = jnp.pad(everywhere(w_out), ((0, nz * hw - D), (0, 0))).reshape(nz, hw, D)
        w1 = lax.dynamic_slice_in_dim(everywhere(w_fc1), c * (FF // 2), FF // 2, 1)
        w1 = w1.reshape(2, 2, 192, 4, 384).transpose(3, 1, 0, 2, 4)
        w2 = lax.dynamic_slice_in_dim(everywhere(w_fc2), c * (FF // 2), FF // 2, 0)
        w2 = w2.reshape(2, 2, 384, 4, 192).transpose(3, 1, 0, 4, 2)
        w1, w2 = w1.transpose(1, 2, 0, 3, 4), w2.transpose(2, 1, 0, 3, 4)
        weights = (w1[0], w1[1], w2[0], w2[1])
        bias_all = lax.all_gather(b_fc1.astype(BF), "seq", axis=0, tiled=True).astype(F32)
        bias = lax.dynamic_slice_in_dim(bias_all, c * (FF // 2), FF // 2, 0).reshape(4, 384)
        bias = jnp.pad(bias, ((0, 4), (0, 0)))
        ff_place = jnp.stack([0 * d, 0 * z, c]).astype(jnp.int32)
    cot_in = links.core(after(cot, x_ext))

    far = sorted(range(1, nz), key=lambda k: -min(k, nz - k))
    first = far[: nz // 2]
    rest = far[nz // 2 :] + [0]
    saved, by = attention_first(
        place, arrays, plan, extras, freq, wq, out_order, heads, chunk, first, (n_w, b_w)
    )
    h1, gains = saved[0], saved[9]
    rest_in = tuple(saved[i] for i in (1, 2, 4, 7, 8))
    if fast:
        bias = saved[11]
        w1_in, w2_in, wo_all, _ = lax.optimization_barrier((w1_in, w2_in, wo_all, h1))
        w1a = jnp.stack([w1, w1_in])
        w2a = jnp.stack([w2, w2_in])
        wo_all = jnp.stack(wo_all)
        wo_in = links.core(wo_all)
        w1b = links.flip(w1a, 1)
        w2b = links.flip(w2a, 2)
        weights = (w1a, w1b, w2a, w2b)
        rest_in = after(rest_in, w1a, w2a, wo_all)
    mixed = {k: links.shift(by[k][0], k) for k in first}
    by = {**by, **attention_rest(rest_in, heads, chunk, rest)}
    for k in rest:
        mixed[k] = links.shift(by[k][0], k) if k else by[k][0]
    mixed = [mixed[k] for k in range(nz)]
    h1_t = after(h1, by[0][0]).T
    if fast:
        wout = reorder_out(place, after(wo_all, by[0][0]), wo_in, out_order)
    residual, h2 = output_projection(place, mixed, wout, after(x_ext, h1_t), gains)
    h2_in = links.core(h2)
    (out_own, out_other, gh_own, gh_other, dw1a, dw1b, dw2a, dw2b, db1) = feed_forward(
        ff_place, h2, h2_in, cot, cot_in, weights, bias
    )
    gh_in = links.core(gh_other)
    out_in = links.core(out_other)
    gres, gproj, sums, gmixed = residual_backward(
        place, gh_own, gh_in, residual, cot, cot_in, gains, wout
    )
    if fast:
        dw1_in = links.flip(dw1b, 1)
        dw2_in = links.flip(dw2b, 2)
    pulled = [gmixed[0]] + [links.shift(gmixed[k], k) for k in range(1, nz)]
    pulled = [pulled[(nz - k) % nz] for k in range(nz)]
    part = attention_backward(pulled, by, saved, heads, chunk, [0], None, None)
    out_rows = (residual + out_own + out_in.astype(F32) + gains[2:3]).astype(BF)
    rows_in = links.core(out_rows[local:])
    if fast:
        wo_keep, wo_send = out_weight(place, mixed, gproj, out_order)
        wo_came = links.core(wo_send)
        dwo = [
            add_low(wo_keep[..., 96 * k : 96 * k + 96], wo_came[..., 96 * k : 96 * k + 96])
            for k in range(4)
        ]
        part, _ = lax.optimization_barrier((part, (dwo, out_rows)))
        dwo = [dwo[0]] + [links.shift(dwo[k], k) for k in range(1, 4)]
    made = attention_backward(
        pulled, by, saved, heads, chunk, list(range(1, nz)), part, (sums, out_order)
    )
    if fast:
        made, dwo, dw1_in, dw2_in, rows_in = lax.optimization_barrier(
            (made, dwo, dw1_in, dw2_in, rows_in)
        )
    gqkv, vec_keep, vec_send, gh1 = made[0], made[1], made[2], made[3:]
    if nz == 4:
        low_in = links.shift(gh1[2], 1)
        high_in = links.shift(gh1[4], -1)
        up = jnp.concatenate([add_low(gh1[1][:local], low_in), gh1[1][local:]], axis=0)
        down = jnp.concatenate([gh1[3][:local], add_low(gh1[3][local:], high_in)], axis=0)
        terms = [gh1[0], links.shift(up, 1), links.shift(down, -1)]
    else:
        terms = [gh1[0]] + [links.shift(gh1[k], k) for k in range(1, nz)]
    grad_rows = input_backward(terms, x_ext, gains, gres)
    grad_in = links.core(grad_rows[local:])

    def by_micro(own, other):
        return jnp.where(c == 0, jnp.stack([own, other]), jnp.stack([other, own]))[:, None]

    outputs = by_micro(out_rows[:local], rows_in)
    input_grad = by_micro(grad_rows[:local], grad_in)
    vec = vec_keep + links.core(vec_send)

    if fast:
        dw1_in = links.flip(add_low(dw1a[1], dw1_in[1]), 2), dw1_in[0]
        dw2_in = links.flip(add_low(dw2a[1], dw2_in[1]), 1), dw2_in[0]
        wq_keep, wq_send = qkv_weight(place, h1_t, after(gqkv, low_in, high_in), qkv_order)
        dwo = sum(t.astype(F32) for t in dwo)
        joint = jnp.concatenate(
            [add_low(wq_keep, links.core(wq_send)), dwo.astype(BF)], axis=2
        )
        joint = joint.reshape(2, 384, 384)
        vec = jnp.concatenate([vec[:3], db1[:, 0], jnp.zeros((9, 384), F32)], axis=0)
        came = links.flip(jnp.concatenate([joint[1], vec.astype(BF)], axis=0), 2)
        joint = add_low(joint[0], came[:384]).reshape(2, 192, 384)
        vec = vec + came[384:].astype(F32)
        came = links.flip(jnp.concatenate([joint[1], vec.astype(BF)], axis=0), 1)
        joint = joint[0].astype(F32) + came[:192].astype(F32)
        vec = vec + came[192:].astype(F32)
        vec = [
            jnp.concatenate(
                [jnp.pad(vec[:3, 96 * k : 96 * k + 96], ((0, 0), (0, 288))), vec[3 + k : 4 + k]],
                axis=0,
            )
            for k in range(4)
        ]
        vec = sum([vec[0]] + [links.shift(vec[k], k) for k in range(1, 4)])
        vecs = (vec[0, :96], vec[1, :96], vec[3], vec[2, :96])
        g_out = joint[:, 288:]
        third = jnp.stack([joint[:, 96 * t : 96 * t + 96] for t in range(3)])
        g_qkv = jnp.concatenate(
            [
                lax.ppermute(
                    pick(third, lax.rem(2 * (i - s + 9), 3)),
                    "seq",
                    [((3 * q + i) % 8, q) for q in range(8)],
                )
                for i in range(3)
            ],
            axis=1,
        )
        dw1 = dw1a[0].astype(F32) + dw1_in[0].astype(F32) + dw1_in[1].astype(F32)
        dw2 = dw2a[0].astype(F32) + dw2_in[0].astype(F32) + dw2_in[1].astype(F32)
        low_in = links.shift(dw1[2].astype(BF), 1)
        high_in = links.shift(dw2[2].astype(BF), -1)
        up = jnp.stack([dw1[1] + low_in.astype(F32), dw2[1]]).astype(BF)
        down = jnp.stack([dw1[3], dw2[3] + high_in.astype(F32)]).astype(BF)
        up_in = links.shift(up, 1).astype(F32)
        down_in = links.shift(down, -1).astype(F32)
        dw = jnp.stack([dw1[0], dw2[0]]) + up_in + down_in
        g_fc1 = dw[0]
        keep, send = to_both((dw[1, :96], dw[1, 96:]))
        g_fc2 = jnp.concatenate(to_both((keep, links.core(send))), axis=1).T
    else:

        def owned(w):
            w = lax.psum_scatter(w.astype(BF), "seq", scatter_dimension=1, tiled=True)
            return lax.psum_scatter(w, "dp", scatter_dimension=0, tiled=True).astype(F32)

        dwq = jnp.einsum("rd,rj->dj", h1, gqkv, preferred_element_type=F32)
        spread = jnp.zeros((D, 3, nz * hw), F32)
        spread = lax.dynamic_update_slice_in_dim(
            spread, dwq.reshape(D, 3, lq)[..., :hw], z * hw, 2
        )
        g_qkv = owned(spread[..., :D].reshape(D, 3 * D))
        mixed_all = jnp.concatenate(mixed, axis=1)
        dwo = jnp.einsum("ri,ro->io", mixed_all, gproj, preferred_element_type=F32)
        dwo = dwo.reshape(nz, hw, D)
        dwo = jnp.roll(dwo[::-1], z + 1, axis=0).reshape(nz * hw, D)[:D]
        g_out = owned(dwo)
        half = jnp.stack([dw1a, dw1b]).transpose(1, 0, 3, 2, 4).reshape(D, FF // 2)
        full = lax.dynamic_update_slice_in_dim(
            jnp.zeros((D, FF), BF), half, c * (FF // 2), 1
        )
        g_fc1 = owned(full)
        half = jnp.stack([dw2a, dw2b]).transpose(0, 1, 4, 2, 3).reshape(FF // 2, D)
        full = lax.dynamic_update_slice_in_dim(
            jnp.zeros((FF, D), BF), half, c * (FF // 2), 0
        )
        g_fc2 = owned(full)
        bias_full = lax.dynamic_update_slice_in_dim(
            jnp.zeros((FF,), F32), db1.reshape(-1), c * (FF // 2), 0
        )
        bias_full = lax.psum(
            lax.psum_scatter(bias_full, "seq", scatter_dimension=0, tiled=True), "dp"
        )
        vec = vec[:3].reshape(3, nz, n_w)
        vec = sum([vec[:, 0]] + [links.shift(vec[:, k], k) for k in range(1, nz)])
        vec = lax.psum(vec, "dp")
        vecs = (vec[0], vec[1], bias_full, vec[2])

    return (
        outputs,
        input_grad,
        vecs[0],
        g_qkv,
        g_out,
        vecs[1],
        g_fc1,
        vecs[2],
        g_fc2,
        vecs[3],
    )


def solution(mesh):
    rows = P(None, "dp", "seq", None)
    labels = P(None, "dp", "seq")
    matrix = P("dp", "seq")
    vector = P("seq")
    return jax.shard_map(
        functools.partial(per_device, mesh.shape["dp"], mesh.shape["seq"]),
        mesh=mesh,
        in_specs=(
            rows, labels, labels, labels, vector, matrix, matrix, vector, matrix, vector, matrix,
            vector, rows,
        ),
        out_specs=(
            rows, rows, vector, matrix, matrix, vector, matrix, vector, matrix, vector,
        ),
        check_vma=False,
    )
```

```python
import functools

import jax
import jax.numpy as jnp
import numpy as np
from jax import lax
from jax.experimental import pallas as pl
from jax.experimental.pallas import tpu as pltpu
from jax.sharding import PartitionSpec as P

D = 768
H = 12
HD = 64
FF = 3072
BLK = 16
F32 = jnp.float32
BF = jnp.bfloat16
NEG = -1e30
VMEM_LIMIT = 56 * 1024 * 1024


def cost(flops, nbytes, scale=1e-3):
    return pl.CostEstimate(
        flops=int(flops * scale), bytes_accessed=int(nbytes * scale), transcendentals=0
    )


def params(*semantics):
    return pltpu.CompilerParams(
        dimension_semantics=semantics or None, vmem_limit_bytes=VMEM_LIMIT
    )


def dot(a, b):
    return lax.dot_general(a, b, (((1,), (0,)), ((), ())), preferred_element_type=F32)


def dot_t(a, b):
    return lax.dot_general(a, b, (((1,), (1,)), ((), ())), preferred_element_type=F32)


def whole(shape):
    return pl.BlockSpec(shape, lambda *_: (0,) * len(shape))


def cuts(count, step):
    return [(at, min(step, count - at)) for at in range(0, count, step)]


def lane_mask(width, head):
    lanes = lax.broadcasted_iota(jnp.int32, (1, width), 1)
    return jnp.where(lanes // HD == head, 1.0, 0.0).astype(BF)


def per_head(block, heads):
    return jnp.concatenate([block * lane_mask(block.shape[1], h) for h in range(heads)], axis=0)


def swap_halves(v):
    out = []
    for at in range(0, v.shape[1], 128):
        part = v[:, at : at + 128]
        lanes = lax.broadcasted_iota(jnp.int32, part.shape, 1)
        out.append(
            jnp.where(
                lanes % HD < HD // 2,
                pltpu.roll(part, 128 - HD // 2, 1),
                pltpu.roll(part, HD // 2, 1),
            )
        )
    return jnp.concatenate(out, axis=1)


def widen(table, width):
    return jnp.concatenate([table] * (width // 128), axis=1)


def cos_sin(angle):
    turns = jnp.round(angle * np.float32(2.0 / np.pi))
    left = angle - turns * np.float32(1.5703125)
    left = left - turns * np.float32(4.837512969970703125e-4)
    left = left - turns * np.float32(7.54978995489188e-8)
    sq = left * left
    sine = left + left * sq * (
        np.float32(-1.6666654611e-1)
        + sq * (np.float32(8.3321608736e-3) + sq * np.float32(-1.9515295891e-4))
    )
    cosine = (
        1.0
        - 0.5 * sq
        + sq
        * sq
        * (
            np.float32(4.166664568298827e-2)
            + sq * (np.float32(-1.388731625493765e-3) + sq * np.float32(2.443315711809948e-5))
        )
    )
    quarter = jnp.bitwise_and(turns.astype(jnp.int32), 3)
    odd = jnp.bitwise_and(quarter, 1) == 1
    sin_out = jnp.where(odd, cosine, sine)
    cos_out = jnp.where(odd, sine, cosine)
    sin_out = jnp.where(quarter >= 2, -sin_out, sin_out)
    cos_out = jnp.where((quarter == 1) | (quarter == 2), -cos_out, cos_out)
    return cos_out, sin_out


def normed(v):
    centered = v - jnp.mean(v, axis=1, keepdims=True)
    var = jnp.mean(centered * centered, axis=1, keepdims=True)
    rstd = lax.rsqrt(var + 1e-05)
    return centered * rstd, rstd


def fold8(v, op):
    return op(v.reshape(v.shape[0] // 8, 8, v.shape[1]), axis=0)


def pair_mask(kcol_ref, rows, codes):
    key = kcol_ref[rows, 3:4]
    low, high, same = codes
    return ((key >= low) & (key < high)) | (key == same)


def query_codes(qrow_ref, at, count):
    cols = pl.ds(at, count)
    return qrow_ref[0:1, cols], qrow_ref[1:2, cols], qrow_ref[2:3, cols]


SUB = 64


def chosen(step, entries):
    value = jnp.int32(entries[0])
    for i, e in enumerate(entries[1:], 1):
        value = jnp.where(step == i, jnp.int32(e), value)
    return value


def attend(step, entries, q_ref, k_ref, vt_ref, kcol_ref, qrow_ref, s_scr, p_scr, heads, chunk):
    blocks = k_ref.shape[0] // chunk
    lq = k_ref.shape[1]
    at = pl.multiple_of(chosen(step, entries) * chunk, chunk)
    codes = query_codes(qrow_ref, at, chunk)
    query = per_head(q_ref[pl.ds(at, chunk), :], heads)

    def score(block, best):
        base = pl.multiple_of(block * chunk, chunk)
        s_scr[pl.ds(base, chunk), :] = dot_t(k_ref[pl.ds(base, chunk), :], query)
        best = list(best)
        for sub in range(0, chunk, SUB):
            rows = pl.ds(base + sub, SUB)
            mask = pair_mask(kcol_ref, rows, codes)
            for h in range(heads):
                cols = slice(h * chunk, (h + 1) * chunk)
                value = jnp.where(mask, s_scr[rows, cols], NEG)
                s_scr[rows, cols] = value
                best[h] = jnp.maximum(best[h], fold8(value, jnp.max))
        return tuple(best)

    best = lax.fori_loop(
        0, blocks, score, tuple(jnp.full((8, chunk), NEG, F32) for _ in range(heads))
    )
    best = [jnp.max(b, axis=0, keepdims=True) for b in best]

    def soften(block, sums):
        base = pl.multiple_of(block * chunk, chunk)
        sums = list(sums)
        for sub in range(0, chunk, SUB):
            rows = pl.ds(base + sub, SUB)
            for h in range(heads):
                cols = slice(h * chunk, (h + 1) * chunk)
                value = jnp.exp(s_scr[rows, cols] - best[h])
                sums[h] = sums[h] + fold8(value, jnp.sum)
                p_scr[rows, cols] = value.astype(BF)
        return tuple(sums)

    sums = lax.fori_loop(
        0, blocks, soften, tuple(jnp.zeros((8, chunk), F32) for _ in range(heads))
    )
    sums = [jnp.sum(s, axis=0, keepdims=True) for s in sums]
    tops = []
    for h in range(heads):
        made = dot(vt_ref[...], p_scr[:, h * chunk : (h + 1) * chunk])
        tops.append(made[h * HD : (h + 1) * HD, :] * (1.0 / sums[h]))
    if heads * HD < lq:
        tops.append(jnp.zeros((lq - heads * HD, chunk), F32))
    logs = [best[h] + jnp.log(sums[h]) for h in range(heads)]
    logs.append(jnp.zeros((8 - heads, chunk), F32))
    return jnp.concatenate(tops, axis=0), jnp.concatenate(logs, axis=0)


def block_outputs(entries, lq, hw, chunk):
    shapes = []
    for _ in entries:
        shapes += [
            jax.ShapeDtypeStruct((chunk, hw), BF),
            jax.ShapeDtypeStruct((lq, chunk), F32),
            jax.ShapeDtypeStruct((8, chunk), F32),
        ]
    return shapes


def store_block(step, entries, refs, joined, logs, hw):
    attended = joined.T[:, :hw].astype(BF)
    for i in range(len(entries)):

        @pl.when(step == i)
        def _(i=i):
            refs[3 * i][...] = attended
            refs[3 * i + 1][...] = joined
            refs[3 * i + 2][...] = logs


def by_block(entries, made):
    return {e: tuple(made[3 * i : 3 * i + 3]) for i, e in enumerate(entries)}


def fill_rows(scr, row, which, labels, vectors, at):
    local = labels[0].shape[1]
    for i, ref in enumerate(labels):
        value = jnp.where(which == 0, ref[0:1, :], ref[1:2, :]).astype(F32)
        scr[row : row + 1, at + local * i : at + local * (i + 1)] = value
    for i, ref in enumerate(vectors):
        scr[row + 1 : row + 2, 128 * i : 128 * i + ref.shape[1]] = ref[...]


def message_rows(place, x, labels, vectors):
    local = x.shape[1]

    def kernel(place_ref, x_ref, *refs):
        label_refs, vector_refs, out_ref, scr = refs[:3], refs[3:7], refs[7], refs[8]
        other = 1 - place_ref[2]
        out_ref[:local, :] = x_ref[other]
        scr[...] = jnp.zeros_like(scr)
        fill_rows(scr, 0, other, label_refs, vector_refs, 0)
        out_ref[local:, :] = scr[...].astype(BF)

    ins = [x] + list(labels) + list(vectors)
    return pl.pallas_call(
        kernel,
        name="message_rows",
        grid_spec=pltpu.PrefetchScalarGridSpec(
            num_scalar_prefetch=1,
            grid=(1,),
            in_specs=[whole(a.shape) for a in ins],
            out_specs=whole((local + 16, D)),
            scratch_shapes=[pltpu.VMEM((16, D), F32)],
        ),
        out_shape=jax.ShapeDtypeStruct((local + 16, D), BF),
        compiler_params=params("arbitrary"),
        cost_estimate=cost(1e6, 1e6),
    )(place, *ins)


def own_rows(place, x, labels, vectors, came):
    local = x.shape[1]

    def kernel(place_ref, x_ref, *refs):
        label_refs, vector_refs, came_ref, out_ref, scr = refs[:3], refs[3:7], *refs[7:]
        own = place_ref[2]
        out_ref[:local, :] = x_ref[own]
        out_ref[local : 2 * local, :] = came_ref[:local, :]
        scr[...] = jnp.zeros_like(scr)
        fill_rows(scr, 0, own, label_refs, vector_refs, 0)
        extra = came_ref[local:, :].astype(F32)
        scr[0:1, 3 * local : 6 * local] = extra[0:1, : 3 * local]
        scr[2:3, :] = extra[1:2, :]
        out_ref[2 * local :, :] = scr[...].astype(BF)

    ins = [x] + list(labels) + list(vectors) + [came]
    return pl.pallas_call(
        kernel,
        name="own_rows",
        grid_spec=pltpu.PrefetchScalarGridSpec(
            num_scalar_prefetch=1,
            grid=(1,),
            in_specs=[whole(a.shape) for a in ins],
            out_specs=whole((2 * local + 16, D)),
            scratch_shapes=[pltpu.VMEM((16, D), F32)],
        ),
        out_shape=jax.ShapeDtypeStruct((2 * local + 16, D), BF),
        compiler_params=params("arbitrary"),
        cost_estimate=cost(1e6, 1e6),
    )(place, *ins)


def attention_first(place, arrays, plan, extras, freq, wq, order, heads, chunk, entries, widths):
    blocks = len(extras)
    total = blocks * chunk
    local = chunk // 2
    hw = heads * HD
    lq = -(-hw // 128) * 128
    count = len(arrays)
    parts = len(wq)
    n_w, b_w = widths
    fixed = 11

    def kernel(place_ref, *refs):
        x_refs = refs[:count]
        freq_ref, order_ref = refs[count : count + 2]
        wq_refs = refs[count + 2 : count + 2 + parts]
        outs = refs[count + 2 + parts :]
        h1_ref, q_ref, k_ref, v_ref, vt_ref, cs_ref, sn_ref, kcol_ref, qrow_ref, gain_ref, wq_ref = (
            outs[:fixed]
        )
        bias_ref = outs[fixed]
        block_refs = outs[fixed + 1 : fixed + 1 + 3 * len(entries)]
        s_scr, p_scr, g_scr = outs[fixed + 1 + 3 * len(entries) :]
        step = pl.program_id(0)
        d, c = place_ref[0], place_ref[2]

        @pl.when(step == 0)
        def _():
            g_scr[...] = jnp.zeros_like(g_scr)
            bias_ref[...] = jnp.zeros_like(bias_ref)
            turn = lax.broadcasted_iota(jnp.int32, (1, chunk), 1) % BLK
            for k, (which, at) in enumerate(extras):
                rows = x_refs[which][at : at + 16, :].astype(F32)

                def label(i, rows=rows):
                    return jnp.concatenate(
                        [
                            rows[0:1, i * local : (i + 1) * local],
                            rows[0:1, (3 + i) * local : (4 + i) * local],
                        ],
                        axis=1,
                    )

                segment, flag, block = label(0), label(1), label(2)
                start = segment * 4096.0
                clean = flag > 0.5
                key = start + jnp.where(clean, block, block + 2048.0)
                place_now = block * BLK + turn.astype(F32)
                coded = jnp.concatenate(
                    [
                        start,
                        start + block + flag,
                        jnp.where(clean, -1.0, key),
                        key,
                        place_now,
                        jnp.zeros((3, chunk), F32),
                    ],
                    axis=0,
                )
                qrow_ref[:, k * chunk : (k + 1) * chunk] = coded
                kcol_ref[k * chunk : (k + 1) * chunk, :] = coded.T
                for half in range(2):
                    vector = rows[1 + half : 2 + half, :]
                    lane = 384 * half + n_w * k
                    for i in range(3):
                        g_scr[i : i + 1, lane : lane + n_w] = vector[:, 128 * i : 128 * i + n_w]
                if parts == 2:
                    bias_ref[k : k + 1, :b_w] = rows[1:2, 384 : 384 + b_w]
            gain_ref[...] = dot_t(g_scr[...].astype(BF), order_ref[...])
            if parts == 2:
                for half in range(2):

                    @pl.when(c == half)
                    def _(half=half):
                        for j in range(4):
                            rows = slice(192 * j, 192 * j + 192)
                            for t in range(3):
                                for i in range(2):
                                    at = lq * t + 96 * (i ^ half)
                                    wq_ref[rows, at : at + 96] = wq_refs[i][
                                        d ^ j, :, 96 * t : 96 * t + 96
                                    ]

                for t in range(3):
                    if hw < lq:
                        wq_ref[:, lq * t + hw : lq * (t + 1)] = jnp.zeros((D, lq - hw), BF)
            else:
                wq_ref[...] = wq_refs[0][...]
            gain_row = gain_ref[0:1, :]
            for which, src, dst, rows in plan:
                for at, size in cuts(rows, 64):
                    xhat, _ = normed(x_refs[which][src + at : src + at + size, :].astype(F32))
                    h1_ref[dst + at : dst + at + size, :] = (xhat * gain_row).astype(BF)
            lanes = lax.broadcasted_iota(jnp.int32, (1, 128), 1)
            sign = jnp.where(lanes % HD < HD // 2, -1.0, 1.0)

            def project(block, carry):
                rows = pl.ds(pl.multiple_of(block * chunk, chunk), chunk)
                cosine, sine = cos_sin(kcol_ref[rows, 4:5] * freq_ref[...])
                sine = sine * sign
                cs_ref[rows, :] = cosine
                sn_ref[rows, :] = sine
                cosine = widen(cosine, lq)
                sine = widen(sine, lq)
                made = dot(h1_ref[rows, :], wq_ref[...])
                q = made[:, :lq]
                q_ref[rows, :] = ((q * cosine + swap_halves(q) * sine).astype(BF) * 0.125).astype(
                    BF
                )
                k = made[:, lq : 2 * lq]
                k_ref[rows, :] = (k * cosine + swap_halves(k) * sine).astype(BF)
                v = made[:, 2 * lq :]
                v_ref[rows, :] = v.astype(BF)
                vt_ref[:, rows] = v.T.astype(BF)
                return carry

            lax.fori_loop(0, blocks, project, 0)

        joined, logs = attend(
            step, entries, q_ref, k_ref, vt_ref, kcol_ref, qrow_ref, s_scr, p_scr, heads, chunk
        )
        store_block(step, entries, block_refs, joined, logs, hw)

    ins = list(arrays) + [freq, order] + list(wq)
    out_shape = [
        jax.ShapeDtypeStruct((total, D), BF),
        jax.ShapeDtypeStruct((total, lq), BF),
        jax.ShapeDtypeStruct((total, lq), BF),
        jax.ShapeDtypeStruct((total, lq), BF),
        jax.ShapeDtypeStruct((lq, total), BF),
        jax.ShapeDtypeStruct((total, 128), F32),
        jax.ShapeDtypeStruct((total, 128), F32),
        jax.ShapeDtypeStruct((total, 8), F32),
        jax.ShapeDtypeStruct((8, total), F32),
        jax.ShapeDtypeStruct((16, D), F32),
        jax.ShapeDtypeStruct((D, 3 * lq), BF),
        jax.ShapeDtypeStruct((-(-blocks // 8) * 8, 384), F32),
    ] + block_outputs(entries, lq, hw, chunk)
    made = pl.pallas_call(
        kernel,
        name="attention_first",
        grid_spec=pltpu.PrefetchScalarGridSpec(
            num_scalar_prefetch=1,
            grid=(len(entries),),
            in_specs=[whole(v.shape) for v in ins],
            out_specs=[whole(o.shape) for o in out_shape],
            scratch_shapes=[
                pltpu.VMEM((total, heads * chunk), F32),
                pltpu.VMEM((total, heads * chunk), BF),
                pltpu.VMEM((16, D), F32),
            ],
        ),
        out_shape=out_shape,
        compiler_params=params("arbitrary"),
        cost_estimate=cost(8e9, 8e6),
    )(place, *ins)
    return made[:12], by_block(entries, made[12:])


def attention_rest(saved, heads, chunk, entries):
    q, k, vt, kcol, qrow = saved
    total, lq = k.shape
    hw = heads * HD

    def kernel(q_ref, k_ref, vt_ref, kcol_ref, qrow_ref, *refs):
        step = pl.program_id(0)
        s_scr, p_scr = refs[3 * len(entries) :]
        joined, logs = attend(
            step, entries, q_ref, k_ref, vt_ref, kcol_ref, qrow_ref, s_scr, p_scr, heads, chunk
        )
        store_block(step, entries, refs, joined, logs, hw)

    ins = [q, k, vt, kcol, qrow]
    out_shape = block_outputs(entries, lq, hw, chunk)
    made = pl.pallas_call(
        kernel,
        name="attention_rest",
        grid=(len(entries),),
        in_specs=[whole(v.shape) for v in ins],
        out_specs=[whole(o.shape) for o in out_shape],
        out_shape=out_shape,
        scratch_shapes=[
            pltpu.VMEM((total, heads * chunk), F32),
            pltpu.VMEM((total, heads * chunk), BF),
        ],
        compiler_params=params("arbitrary"),
        cost_estimate=cost(5e9, 4e6),
    )(*ins)
    return by_block(entries, made)


def attention_backward(pulls, by, saved, heads, chunk, entries, before, finish):
    h1, q, k, v, _, cs, sn, kcol, qrow, gains, wq = saved[:11]
    last = finish is not None
    total, lq = k.shape
    blocks = total // chunk
    hw = heads * HD
    n = len(entries)
    halves = blocks == 4
    pieces = blocks + 1 if halves else blocks

    def kernel(*refs):
        g_refs, att_refs, lse_refs = refs[:n], refs[n : 2 * n], refs[2 * n : 3 * n]
        q_ref, k_ref, v_ref, cs_ref, sn_ref, kcol_ref, qrow_ref = refs[3 * n : 3 * n + 7]
        refs = refs[3 * n + 7 :]
        if last:
            dq_in, dk_in, dv_in, wq_ref, h1_ref, gains_ref, sums_ref, order_ref = refs[:8]
            gqkv_ref, keep_ref, send_ref = refs[8:11]
            gh_refs = refs[11 : 11 + pieces]
            scr = refs[11 + pieces :]
        else:
            dq_out, dk_out, dv_out = refs[:3]
            scr = refs[3:]
        g_scr, row_scr, kt_scr, dk_scr, dv_scr, s_scr, dp_scr, pb_scr, ds_scr, dst_scr = scr
        step = pl.program_id(0)

        @pl.when(step == 0)
        def _():
            for i in range(n):
                g_scr[i, :, :hw] = g_refs[i][...]
                if hw < lq:
                    g_scr[i, :, hw:] = jnp.zeros((chunk, lq - hw), BF)
                product = g_scr[i].astype(F32).T * att_refs[i][...]
                for h in range(heads):
                    row_scr[i, h : h + 1, :] = jnp.sum(
                        product[h * HD : (h + 1) * HD, :], axis=0, keepdims=True
                    )
                row_scr[i, 8:16, :] = lse_refs[i][...]
            if last:
                dk_scr[...] = dk_in[...]
                dv_scr[...] = dv_in[...]
            else:
                dk_scr[...] = jnp.zeros_like(dk_scr)
                dv_scr[...] = jnp.zeros_like(dv_scr)

            def turn(block, carry):
                rows = pl.ds(pl.multiple_of(block * chunk, chunk), chunk)
                flat = k_ref[rows, :].astype(F32).T
                line = lax.broadcasted_iota(jnp.int32, (lq, 1), 0) // HD
                for h in range(heads):
                    kt_scr[block, :, h * chunk : (h + 1) * chunk] = jnp.where(
                        line == h, flat, 0.0
                    ).astype(BF)
                return carry

            lax.fori_loop(0, blocks, turn, 0)

        at = pl.multiple_of(chosen(step, entries) * chunk, chunk)
        own = pl.ds(at, chunk)
        codes = query_codes(qrow_ref, at, chunk)
        query = per_head(q_ref[own, :], heads)
        pull = per_head(g_scr[step], heads)
        delta = [row_scr[step, h : h + 1, :] for h in range(heads)]
        top = [row_scr[step, 8 + h : 9 + h, :] for h in range(heads)]

        def keys(block, dq_t):
            base = pl.multiple_of(block * chunk, chunk)
            rows = pl.ds(base, chunk)
            s_scr[...] = dot_t(k_ref[rows, :], query)
            dp_scr[...] = dot_t(v_ref[rows, :], pull)
            for sub in range(0, chunk, SUB):
                part = slice(sub, sub + SUB)
                mask = pair_mask(kcol_ref, pl.ds(base + sub, SUB), codes)
                for h in range(heads):
                    cols = slice(h * chunk, (h + 1) * chunk)
                    prob = jnp.exp(jnp.where(mask, s_scr[part, cols] - top[h], NEG))
                    slope = (prob * (dp_scr[part, cols] - delta[h])).astype(BF)
                    pb_scr[part, cols] = prob.astype(BF)
                    ds_scr[part, cols] = slope
                    dst_scr[h * chunk + sub : h * chunk + sub + SUB, :] = slope
            dv_scr[rows, :] += dot(pb_scr[...], pull)
            dk_scr[rows, :] += dot(ds_scr[...], query)
            return dq_t + dot(kt_scr[block], dst_scr[...])

        dq_t = lax.fori_loop(0, blocks, keys, jnp.zeros((lq, chunk), F32))

        def unrotate(value, rows):
            return value * widen(cs_ref[rows, :], lq) - swap_halves(value) * widen(
                sn_ref[rows, :], lq
            )

        dq = unrotate(dq_t.T * 0.125, own).astype(BF)
        if not last:
            dq_out[...] = dq

            @pl.when(step == n - 1)
            def _():
                dk_out[...] = dk_scr[...]
                dv_out[...] = dv_scr[...]

        else:
            gqkv_ref[own, :lq] = dq

            @pl.when(step == n - 1)
            def _():
                gqkv_ref[0:chunk, :lq] = dq_in[...]
                n1 = jnp.zeros((8, D), F32)
                for b in range(blocks):
                    rows = slice(b * chunk, (b + 1) * chunk)
                    gqkv_ref[rows, lq : 2 * lq] = unrotate(dk_scr[rows, :], rows).astype(BF)
                    gqkv_ref[rows, 2 * lq :] = dv_scr[rows, :].astype(BF)
                    gh = dot_t(gqkv_ref[rows, :], wq_ref[...])
                    if halves and b == 2:
                        gh_refs[2][...] = gh[: chunk // 2, :].astype(BF)
                        gh_refs[4][...] = gh[chunk // 2 :, :].astype(BF)
                    else:
                        gh_refs[b][...] = gh.astype(gh_refs[b].dtype)
                    n1 = n1 + fold8(gh * h1_ref[rows, :].astype(F32), jnp.sum)
                lines = [
                    jnp.sum(n1, axis=0, keepdims=True) / gains_ref[0:1, :],
                    jnp.sum(sums_ref[0:8, :], axis=0, keepdims=True),
                    jnp.sum(sums_ref[8:16, :], axis=0, keepdims=True),
                    jnp.zeros((13, D), F32),
                ]
                lines = jnp.concatenate(lines, axis=0)
                high = lines.astype(BF)
                rest = (lines - high.astype(F32)).astype(BF)
                lines = dot(high, order_ref[...]) + dot(rest, order_ref[...])
                keep_ref[...] = lines[:, :384]
                send_ref[...] = lines[:, 384:]

    ins = [pulls[e] for e in entries] + [by[e][1] for e in entries] + [by[e][2] for e in entries]
    ins += [q, k, v, cs, sn, kcol, qrow]
    if last:
        ins += list(before) + [wq, h1, gains] + list(finish)
        out_shape = [
            jax.ShapeDtypeStruct((total, 3 * lq), BF),
            jax.ShapeDtypeStruct((16, 384), F32),
            jax.ShapeDtypeStruct((16, 384), F32),
        ]
        for b in range(pieces):
            rows = chunk // 2 if halves and b in (2, 4) else chunk
            out_shape.append(jax.ShapeDtypeStruct((rows, D), F32 if b == 0 else BF))
    else:
        out_shape = [
            jax.ShapeDtypeStruct((chunk, lq), BF),
            jax.ShapeDtypeStruct((total, lq), F32),
            jax.ShapeDtypeStruct((total, lq), F32),
        ]
    return pl.pallas_call(
        kernel,
        name="attention_backward_last" if last else "attention_backward_own",
        grid=(n,),
        in_specs=[whole(a.shape) for a in ins],
        out_specs=[whole(o.shape) for o in out_shape],
        out_shape=out_shape,
        scratch_shapes=[
            pltpu.VMEM((n, chunk, lq), BF),
            pltpu.VMEM((n, 16, chunk), F32),
            pltpu.VMEM((blocks, lq, heads * chunk), BF),
            pltpu.VMEM((total, lq), F32),
            pltpu.VMEM((total, lq), F32),
            pltpu.VMEM((chunk, heads * chunk), F32),
            pltpu.VMEM((chunk, heads * chunk), F32),
            pltpu.VMEM((chunk, heads * chunk), BF),
            pltpu.VMEM((chunk, heads * chunk), BF),
            pltpu.VMEM((heads * chunk, chunk), BF),
        ],
        compiler_params=params("arbitrary"),
        cost_estimate=cost(3e9 * n, 1e7),
    )(*ins)


def dot_first(a, b):
    return lax.dot_general(a, b, (((0,), (0,)), ((), ())), preferred_element_type=F32)


def reorder_out(place, own, other, order):
    def kernel(place_ref, own_ref, other_ref, order_ref, out_ref, scr):
        d = place_ref[0]
        for j in range(4):
            for k in range(4):
                at = 96 * k
                part = slice(96 * j, 96 * j + 96)
                scr[j, :, at : at + 96] = own_ref[k, :, part]
                scr[j, :, 384 + at : 384 + at + 96] = other_ref[k, :, part]
        for j in range(4):
            out_ref[j] = dot_t(scr[d ^ j], order_ref[...]).astype(BF)

    return pl.pallas_call(
        kernel,
        name="reorder_out",
        grid_spec=pltpu.PrefetchScalarGridSpec(
            num_scalar_prefetch=1,
            grid=(1,),
            in_specs=[whole(own.shape), whole(other.shape), whole(order.shape)],
            out_specs=whole((4, 192, D)),
            scratch_shapes=[pltpu.VMEM((4, 192, 768), BF)],
        ),
        out_shape=jax.ShapeDtypeStruct((4, 192, D), BF),
        compiler_params=params("arbitrary"),
        cost_estimate=cost(1e9, 3e6),
    )(place, own, other, order)


def qkv_weight(place, h1_t, gqkv, order):
    def kernel(place_ref, h_ref, g_ref, order_ref, keep_ref, send_ref):
        d = place_ref[0]
        made = dot(h_ref[...], g_ref[...]).astype(BF)
        made = dot(made, order_ref[...]).astype(BF)
        for j in range(4):
            rows = slice(192 * j, 192 * j + 192)
            keep_ref[d ^ j] = made[rows, :288]
            send_ref[d ^ j] = made[rows, 384:672]

    shape = jax.ShapeDtypeStruct((4, 192, 288), BF)
    return pl.pallas_call(
        kernel,
        name="qkv_weight",
        grid_spec=pltpu.PrefetchScalarGridSpec(
            num_scalar_prefetch=1,
            grid=(1,),
            in_specs=[whole(h1_t.shape), whole(gqkv.shape), whole(order.shape)],
            out_specs=[whole(shape.shape)] * 2,
        ),
        out_shape=[shape, shape],
        compiler_params=params("arbitrary"),
        cost_estimate=cost(2e9, 5e6),
    )(place, h1_t, gqkv, order)


def out_weight(place, mixed, gproj, order):
    groups = len(mixed)

    def kernel(place_ref, *refs):
        m_refs = refs[:groups]
        g_ref, order_ref, keep_ref, send_ref = refs[groups:]
        d, z = place_ref[0], place_ref[1]
        for k in range(groups):
            made = dot_first(m_refs[k][...], g_ref[...]).astype(BF)
            made = dot(made, order_ref[...]).astype(BF)
            row = d ^ lax.rem(z + (groups - k), groups)
            keep_ref[row] = made[:, :384]
            send_ref[row] = made[:, 384:]

    ins = list(mixed) + [gproj, order]
    shape = jax.ShapeDtypeStruct((4, 192, 384), BF)
    return pl.pallas_call(
        kernel,
        name="out_weight",
        grid_spec=pltpu.PrefetchScalarGridSpec(
            num_scalar_prefetch=1,
            grid=(1,),
            in_specs=[whole(a.shape) for a in ins],
            out_specs=[whole(shape.shape)] * 2,
        ),
        out_shape=[shape, shape],
        compiler_params=params("arbitrary"),
        cost_estimate=cost(1e9, 4e6),
    )(place, *ins)


def output_projection(place, mixed, wout, x, gain):
    groups = len(mixed)
    rows = mixed[0].shape[0]

    def kernel(place_ref, *refs):
        m_refs = refs[:groups]
        w_ref, x_ref, gain_ref, res_ref, h2_ref = refs[groups:]
        z = place_ref[1]
        total = x_ref[:rows, :].astype(F32)
        for k in range(groups):
            total = total + dot(m_refs[k][...], w_ref[lax.rem(z + (groups - k), groups)])
        res_ref[...] = total
        for at, size in cuts(rows, 64):
            xhat, _ = normed(res_ref[at : at + size, :])
            h2_ref[at : at + size, :] = (xhat * gain_ref[1:2, :]).astype(BF)

    ins = list(mixed) + [wout, x, gain]
    return pl.pallas_call(
        kernel,
        name="output_projection",
        grid_spec=pltpu.PrefetchScalarGridSpec(
            num_scalar_prefetch=1,
            grid=(1,),
            in_specs=[whole(a.shape) for a in ins],
            out_specs=[whole((rows, D)), whole((rows, D))],
        ),
        out_shape=[jax.ShapeDtypeStruct((rows, D), F32), jax.ShapeDtypeStruct((rows, D), BF)],
        compiler_params=params("arbitrary"),
        cost_estimate=cost(1e9, 3e6),
    )(place, *ins)


def feed_forward(place, h2_own, h2_other, cot, cot_in, weights, bias):
    rows = h2_own.shape[0]
    both = 2 * rows
    width = 384

    def kernel(
        place_ref, ho_ref, hp_ref, go_ref, gp_ref, w1a_ref, w1b_ref, w2a_ref, w2b_ref, b_ref,
        out_own, out_other, gh_own, gh_other, d1a_ref, d1b_ref, d2a_ref, d2b_ref, db_ref,
        h_scr, g_scr, ht_scr, gt_scr, w1_scr, w2_scr, pre_scr, ga_scr, act_scr, slope_scr, out_scr,
        gh_scr, dw_scr,
    ):
        step = pl.program_id(0)
        d = place_ref[0]
        z = place_ref[1]
        c = place_ref[2]

        @pl.when(step == 0)
        def _():
            h_scr[:rows, :] = ho_ref[...]
            h_scr[rows:, :] = hp_ref[...]
            local = rows // 2
            g_scr[:local, :] = go_ref[c]
            g_scr[local:rows, :] = gp_ref[c]
            g_scr[rows : rows + local, :] = gp_ref[1 - c]
            g_scr[rows + local :, :] = go_ref[1 - c]
            for at in range(0, both, 256):
                part = slice(at, at + 256)
                ht_scr[:, part] = h_scr[part, :].astype(F32).T.astype(BF)
                gt_scr[:, part] = g_scr[part, :].astype(F32).T.astype(BF)

        near = lax.rem(step - z + 4, 4)
        hidden = step ^ d
        for odd in range(2):

            @pl.when(d % 2 == odd)
            def _(odd=odd):
                for j in range(4):
                    src = (w1a_ref, w1b_ref)[odd ^ (j % 2)]
                    w1_scr[192 * j : 192 * j + 192, :] = src[(d ^ j) // 2, near]

            @pl.when(hidden // 2 == odd)
            def _(odd=odd):
                for j in range(4):
                    src = (w2a_ref, w2b_ref)[odd]
                    w2_scr[192 * j : 192 * j + 192, :] = src[hidden % 2, lax.rem(j - z + 4, 4)]

        pre_scr[...] = dot(h_scr[...], w1_scr[...])
        ga_scr[...] = dot(g_scr[...], w2_scr[...])
        bias_row = b_ref[pl.ds(near, 1), :]
        total = jnp.zeros((8, width), F32)
        for at in range(0, both, 32):
            part = slice(at, at + 32)
            u = pre_scr[part, :] + bias_row
            usq = u * u
            c = np.float32(np.sqrt(2.0 / np.pi))
            t = jnp.tanh(c * (u + np.float32(0.044715) * (usq * u)))
            half = 0.5 * (1.0 + t)
            act_scr[part, :] = (u * half).astype(BF)
            rise = half + 0.5 * u * (1.0 - t * t) * (c * (1.0 + np.float32(0.134145) * usq))
            slope = (ga_scr[part, :] * rise).astype(BF)
            slope_scr[part, :] = slope
            total = total + fold8(slope.astype(F32), jnp.sum)
        db_ref[0] = jnp.sum(total, axis=0, keepdims=True)

        out_now = dot_t(act_scr[...], w2_scr[...])
        gh_now = dot_t(slope_scr[...], w1_scr[...])

        @pl.when(step == 0)
        def _():
            out_scr[...] = out_now
            gh_scr[...] = gh_now

        @pl.when(step > 0)
        def _():
            out_scr[...] += out_now
            gh_scr[...] += gh_now

        dw_scr[0] = dot(ht_scr[...], slope_scr[...]).astype(BF)
        dw_scr[1] = dot(gt_scr[...], act_scr[...]).astype(BF)
        for odd in range(2):

            @pl.when(d % 2 == odd)
            def _(odd=odd):
                for j in range(4):
                    dst = (d1a_ref, d1b_ref)[odd ^ (j % 2)]
                    dst[(d ^ j) // 2, near] = dw_scr[0, 192 * j : 192 * j + 192, :]

            @pl.when(hidden // 2 == odd)
            def _(odd=odd):
                for j in range(4):
                    dst = (d2a_ref, d2b_ref)[odd]
                    dst[hidden % 2, lax.rem(j - z + 4, 4)] = dw_scr[1, 192 * j : 192 * j + 192, :]

        @pl.when(step == 3)
        def _():
            out_own[...] = out_scr[:rows, :]
            out_other[...] = out_scr[rows:, :].astype(BF)
            gh_own[...] = gh_scr[:rows, :]
            gh_other[...] = gh_scr[rows:, :].astype(BF)

    def by_z(i, place_ref):
        return (lax.rem(i - place_ref[1] + 4, 4), 0, 0)

    ins = [h2_own, h2_other, cot, cot_in] + list(weights) + [bias]
    full = jax.ShapeDtypeStruct((2, 4, 192, width), BF)
    out_shape = [
        jax.ShapeDtypeStruct((rows, D), F32),
        jax.ShapeDtypeStruct((rows, D), BF),
        jax.ShapeDtypeStruct((rows, D), F32),
        jax.ShapeDtypeStruct((rows, D), BF),
        full,
        full,
        full,
        full,
        jax.ShapeDtypeStruct((4, 1, width), F32),
    ]
    return pl.pallas_call(
        kernel,
        name="feed_forward",
        grid_spec=pltpu.PrefetchScalarGridSpec(
            num_scalar_prefetch=1,
            grid=(4,),
            in_specs=[whole(a.shape) for a in ins],
            out_specs=[whole(o.shape) for o in out_shape[:-1]]
            + [pl.BlockSpec((1, 1, width), by_z)],
            scratch_shapes=[
                pltpu.VMEM((both, D), BF),
                pltpu.VMEM((both, D), BF),
                pltpu.VMEM((D, both), BF),
                pltpu.VMEM((D, both), BF),
                pltpu.VMEM((D, width), BF),
                pltpu.VMEM((D, width), BF),
                pltpu.VMEM((both, width), F32),
                pltpu.VMEM((both, width), F32),
                pltpu.VMEM((both, width), BF),
                pltpu.VMEM((both, width), BF),
                pltpu.VMEM((both, D), F32),
                pltpu.VMEM((both, D), F32),
                pltpu.VMEM((2, D, width), BF),
            ],
        ),
        out_shape=out_shape,
        compiler_params=params("arbitrary"),
        cost_estimate=cost(7.2e9, 1.5e7),
    )(place, *ins)


def residual_backward(place, gh_own, gh_in, residual, cot, cot_in, gain, wout):
    rows, local = residual.shape[0], cot.shape[1]
    groups, hw = wout.shape[0], wout.shape[1]

    def kernel(place_ref, gh_ref, gi_ref, res_ref, ca_ref, cb_ref, gain_ref, w_ref, *outs):
        gres_ref, gproj_ref, vec_ref = outs[:3]
        gm_refs = outs[3:]
        z, c = place_ref[1], place_ref[2]
        gain_row = gain_ref[1:2, :]
        gsum = jnp.zeros((8, D), F32)
        bsum = jnp.zeros((8, D), F32)
        for at, size in cuts(rows, 32):
            part = slice(at, at + size)
            xhat, rstd = normed(res_ref[part, :])
            dy_now = (ca_ref, cb_ref)[at // local][c, at % local : at % local + size, :].astype(F32)
            grad = gh_ref[part, :] + gi_ref[part, :].astype(F32)
            along = grad * xhat
            gsum = gsum + fold8(along, jnp.sum)
            bsum = bsum + fold8(dy_now, jnp.sum)
            u = grad * gain_row
            back = (
                u
                - jnp.mean(u, axis=1, keepdims=True)
                - xhat * jnp.mean(along * gain_row, axis=1, keepdims=True)
            )
            value = dy_now + back * rstd
            gres_ref[part, :] = value
            gproj_ref[part, :] = value.astype(BF)
        vec_ref[0:8, :] = gsum
        vec_ref[8:16, :] = bsum
        for k in range(groups):
            gm_refs[k][...] = dot_t(gproj_ref[...], w_ref[lax.rem(z + k, groups)]).astype(BF)

    ins = [gh_own, gh_in, residual, cot, cot_in, gain, wout]
    out_shape = [
        jax.ShapeDtypeStruct((rows, D), F32),
        jax.ShapeDtypeStruct((rows, D), BF),
        jax.ShapeDtypeStruct((16, D), F32),
    ] + [jax.ShapeDtypeStruct((rows, hw), BF) for _ in range(groups)]
    made = pl.pallas_call(
        kernel,
        name="residual_backward",
        grid_spec=pltpu.PrefetchScalarGridSpec(
            num_scalar_prefetch=1,
            grid=(1,),
            in_specs=[whole(a.shape) for a in ins],
            out_specs=[whole(o.shape) for o in out_shape],
        ),
        out_shape=out_shape,
        compiler_params=params("arbitrary"),
        cost_estimate=cost(1e9, 4e6),
    )(place, *ins)
    return made[0], made[1], made[2], made[3:]


def input_backward(terms, x, gain, gres):
    rows = gres.shape[0]
    count = len(terms)

    def kernel(*refs):
        x_ref, gain_ref, gres_ref, out_ref = refs[count:]
        for at, size in cuts(rows, 32):
            part = slice(at, at + size)
            grad = refs[0][part, :].astype(F32)
            for t in range(1, count):
                grad = grad + refs[t][part, :].astype(F32)
            xhat, rstd = normed(x_ref[part, :].astype(F32))
            u = grad * gain_ref[0:1, :]
            back = (
                u
                - jnp.mean(u, axis=1, keepdims=True)
                - xhat * jnp.mean(u * xhat, axis=1, keepdims=True)
            )
            out_ref[part, :] = (gres_ref[part, :] + back * rstd).astype(BF)

    ins = list(terms) + [x, gain, gres]
    return pl.pallas_call(
        kernel,
        name="input_backward",
        grid=(1,),
        in_specs=[whole(a.shape) for a in ins],
        out_specs=whole((rows, D)),
        out_shape=jax.ShapeDtypeStruct((rows, D), BF),
        compiler_params=params("arbitrary"),
        cost_estimate=cost(1e8, 3e6),
    )(*ins)


def add_low(a, b):
    return (a.astype(F32) + b.astype(F32)).astype(BF)


def pick(v, index):
    return lax.dynamic_index_in_dim(v, index, 0, keepdims=False)


def after(v, *others):
    return lax.optimization_barrier((v, others))[0]


class Links:
    def __init__(self, n_dp, n_seq):
        self.n_dp, self.n_seq, self.nz = n_dp, n_seq, n_seq // 2

    def core(self, v):
        return lax.ppermute(v, "seq", [(s, s ^ 1) for s in range(self.n_seq)])

    def flip(self, v, bit):
        return lax.ppermute(v, "dp", [(i, i ^ bit) for i in range(self.n_dp)])

    def shift(self, v, k):
        n = self.nz
        return lax.ppermute(
            v, "seq", [(s, 2 * ((s // 2 + k) % n) + s % 2) for s in range(self.n_seq)]
        )


def order_matrix(source, valid):
    rows = lax.broadcasted_iota(jnp.int32, (768, 768), 0)
    return jnp.where((rows == source[None, :]) & valid[None, :], 1.0, 0.0).astype(BF)


def per_device(
    n_dp,
    n_seq,
    inputs,
    row_segment,
    row_flag,
    row_block,
    norm1_scale,
    w_qkv,
    w_out,
    norm2_scale,
    w_fc1,
    b_fc1,
    w_fc2,
    b_fc2,
    cotangent,
):
    links = Links(n_dp, n_seq)
    nz = links.nz
    local = inputs.shape[2]
    chunk = 2 * local
    heads = -(-H // nz)
    hw = heads * HD
    lq = -(-hw // 128) * 128
    fast = n_dp == 4 and nz == 4 and H % nz == 0
    d = lax.axis_index("dp")
    s = lax.axis_index("seq")
    z = s // 2
    c = s % 2
    place = jnp.stack([d, z, c]).astype(jnp.int32)
    n_w, b_w = D // n_seq, FF // n_seq
    cols = jnp.arange(768, dtype=jnp.int32)
    side, at = cols // 384, cols % 384
    out_order = order_matrix(
        n_w * (2 * ((z + at // n_w) % nz) + (c ^ side)) + at % n_w, at < 384
    )

    def to_both(w):
        return jnp.where(c == 0, w[0], w[1]), jnp.where(c == 0, w[1], w[0])

    x_loc = inputs[:, 0]
    labels = (row_segment[:, 0], row_flag[:, 0], row_block[:, 0])
    vectors = tuple(v.reshape(1, -1) for v in (norm1_scale, norm2_scale, b_fc2, b_fc1))
    came = links.core(message_rows(place, x_loc, labels, vectors))
    x_ext = own_rows(place, x_loc, labels, vectors, came)
    if nz == 4:
        x_before = links.shift(x_ext, 1)
        x_after = links.shift(x_ext, -1)
        x_low = links.shift(x_before[:144], 1)
        x_high = links.shift(x_after[144:], -1)
        gathered = [[x_ext], [x_after], [x_low, x_high], [x_before]]
    else:
        gathered = [[x_ext]] + [[links.shift(x_ext, -k)] for k in range(1, nz)]
    arrays, plan, extras = [], [], []
    for k, pieces in enumerate(gathered):
        at = 0
        for piece in pieces:
            rows = min(piece.shape[0], chunk - at)
            plan.append((len(arrays), 0, k * chunk + at, rows))
            at += rows
            arrays.append(piece)
        extras.append((len(arrays) - 1, pieces[-1].shape[0] - 16))
    freq = np.tile(
        np.float32(10000.0) ** (np.float32(-2.0) * np.arange(32, dtype=np.float32) / HD), 4
    )
    freq = jnp.asarray(freq.astype(np.float32)[None, :])
    cot = cotangent[:, 0]

    if fast:
        two = w_fc2.astype(BF).T.reshape(96, 2, 384)
        two_keep, two_send = to_both((two[:, 0], two[:, 1]))
        two = jnp.concatenate(to_both((two_keep, links.core(two_send))), axis=0)
        w12 = jnp.stack([w_fc1.astype(BF), two])
        w_before = links.shift(w12, 1)
        w_after = links.shift(w12, -1)
        w1_two = links.shift(w_before[0], 1)
        w2_two = links.shift(w_after[1], -1)
        w1 = jnp.stack([w12[0], w_after[0], w1_two, w_before[0]])
        w2 = jnp.stack([w12[1], w_after[1], w2_two, w_before[1]])

        qkv_order = order_matrix(
            256 * (cols % 384 // 96) + 96 * (c ^ side) + cols % 96, cols % 384 < 288
        )
        wq_parts = after(w_qkv.astype(BF), x_ext)
        parts = []
        for i in range(3):
            parts.append(
                lax.ppermute(
                    wq_parts[:, 96 * i : 96 * i + 96],
                    "seq",
                    [(q, (3 * q + i) % 8) for q in range(8)],
                )
            )
        parts = jnp.stack(parts)
        wq_own = jnp.concatenate(
            [pick(parts, (2 * t + s) % 3) for t in range(3)] + [w_out.astype(BF)], axis=1
        )
        wq_own = jnp.stack([wq_own, links.flip(wq_own, 1)])
        wq_own = jnp.stack([wq_own, links.flip(wq_own, 2)]).reshape(4, 192, 384)
        wq_own, qkv_order = lax.optimization_barrier((wq_own, qkv_order))
        wq = (wq_own, links.core(wq_own))
        wo_own = jnp.concatenate([wq_own[j, :, 288:] for j in range(4)], axis=1)

        arrays, w1, w2, wo_own = lax.optimization_barrier((arrays, w1, w2, wo_own))
        w1_in = links.flip(w1, 2)
        w2_in = links.flip(w2, 1)
        wo_all = [wo_own] + [links.shift(wo_own, -k) for k in range(1, 4)]
        ff_place = place
    else:

        def everywhere(w):
            w = lax.all_gather(w.astype(BF), "seq", axis=1, tiled=True)
            return lax.all_gather(w, "dp", axis=0, tiled=True)

        wq = everywhere(w_qkv).reshape(D, 3, D)
        wq = jnp.pad(wq, ((0, 0), (0, 0), (0, nz * hw - D)))
        wq = lax.dynamic_slice_in_dim(wq, z * hw, hw, 2)
        wq = (jnp.pad(wq, ((0, 0), (0, 0), (0, lq - hw))).reshape(D, 3 * lq),)
        wout = jnp.pad(everywhere(w_out), ((0, nz * hw - D), (0, 0))).reshape(nz, hw, D)
        w1 = lax.dynamic_slice_in_dim(everywhere(w_fc1), c * (FF // 2), FF // 2, 1)
        w1 = w1.reshape(2, 2, 192, 4, 384).transpose(3, 1, 0, 2, 4)
        w2 = lax.dynamic_slice_in_dim(everywhere(w_fc2), c * (FF // 2), FF // 2, 0)
        w2 = w2.reshape(2, 2, 384, 4, 192).transpose(3, 1, 0, 4, 2)
        w1, w2 = w1.transpose(1, 2, 0, 3, 4), w2.transpose(2, 1, 0, 3, 4)
        weights = (w1[0], w1[1], w2[0], w2[1])
        bias_all = lax.all_gather(b_fc1.astype(BF), "seq", axis=0, tiled=True).astype(F32)
        bias = lax.dynamic_slice_in_dim(bias_all, c * (FF // 2), FF // 2, 0).reshape(4, 384)
        bias = jnp.pad(bias, ((0, 4), (0, 0)))
        ff_place = jnp.stack([0 * d, 0 * z, c]).astype(jnp.int32)
    cot_in = links.core(after(cot, arrays))

    far = sorted(range(1, nz), key=lambda k: -min(k, nz - k))
    first = far[: nz // 2]
    rest = far[nz // 2 :] + [0]
    saved, by = attention_first(
        place, arrays, plan, extras, freq, wq, out_order, heads, chunk, first, (n_w, b_w)
    )
    h1, gains = saved[0], saved[9]
    rest_in = tuple(saved[i] for i in (1, 2, 4, 7, 8))
    if fast:
        bias = saved[11]
        w1_in, w2_in, wo_all, _ = lax.optimization_barrier((w1_in, w2_in, wo_all, h1))
        w1a = jnp.stack([w1, w1_in])
        w2a = jnp.stack([w2, w2_in])
        wo_all = jnp.stack(wo_all)
        wo_in = links.core(wo_all)
        w1b = links.flip(w1a, 1)
        w2b = links.flip(w2a, 2)
        weights = (w1a, w1b, w2a, w2b)
        rest_in = after(rest_in, w1a, w2a, wo_all)
    mixed = {k: links.shift(by[k][0], k) for k in first}
    by = {**by, **attention_rest(rest_in, heads, chunk, rest)}
    for k in rest:
        mixed[k] = links.shift(by[k][0], k) if k else by[k][0]
    mixed = [mixed[k] for k in range(nz)]
    h1_t = after(h1, by[0][0]).T
    if fast:
        wout = reorder_out(place, after(wo_all, by[0][0]), wo_in, out_order)
    residual, h2 = output_projection(place, mixed, wout, after(x_ext, h1_t), gains)
    h2_in = links.core(h2)
    (out_own, out_other, gh_own, gh_other, dw1a, dw1b, dw2a, dw2b, db1) = feed_forward(
        ff_place, h2, h2_in, cot, cot_in, weights, bias
    )
    gh_in = links.core(gh_other)
    out_in = links.core(out_other)
    gres, gproj, sums, gmixed = residual_backward(
        place, gh_own, gh_in, residual, cot, cot_in, gains, wout
    )
    if fast:
        dw1_in = links.flip(dw1b, 1)
        dw2_in = links.flip(dw2b, 2)
    pulled = [gmixed[0]] + [links.shift(gmixed[k], k) for k in range(1, nz)]
    pulled = [pulled[(nz - k) % nz] for k in range(nz)]
    part = attention_backward(pulled, by, saved, heads, chunk, [0], None, None)
    if fast:
        part, pulled, gproj = lax.optimization_barrier((part, pulled, gproj))
    out_rows = (residual + out_own + out_in.astype(F32) + gains[2:3]).astype(BF)
    rows_in = links.core(out_rows[local:])
    if fast:
        wo_keep, wo_send = out_weight(place, mixed, gproj, out_order)
        wo_came = links.core(wo_send)
        dw1_in, dw2_in, _ = lax.optimization_barrier((dw1_in, dw2_in, wo_keep))
        dw1_sum = add_low(dw1a[1], dw1_in[1])
        dw2_sum = add_low(dw2a[1], dw2_in[1])
        dwo = [
            add_low(wo_keep[..., 96 * k : 96 * k + 96], wo_came[..., 96 * k : 96 * k + 96])
            for k in range(4)
        ]
        dw1 = dw1a[0].astype(F32) + dw1_in[0].astype(F32)
        dw2 = dw2a[0].astype(F32) + dw2_in[0].astype(F32)
        part, dwo, dw1_sum, dw2_sum, dw1, dw2, _ = lax.optimization_barrier(
            (part, dwo, dw1_sum, dw2_sum, dw1, dw2, out_rows)
        )
        dw1_in = links.flip(dw1_sum, 2)
        dw2_in = links.flip(dw2_sum, 1)
        dwo = [dwo[0]] + [links.shift(dwo[k], k) for k in range(1, 4)]
    made = attention_backward(
        pulled, by, saved, heads, chunk, list(range(1, nz)), part, (sums, out_order)
    )
    if fast:
        made, dwo, dw1_in, dw2_in, rows_in = lax.optimization_barrier(
            (made, dwo, dw1_in, dw2_in, rows_in)
        )
    gqkv, vec_keep, vec_send, gh1 = made[0], made[1], made[2], made[3:]
    if nz == 4:
        low_in = links.shift(gh1[2], 1)
        high_in = links.shift(gh1[4], -1)
        if fast:
            wq_keep, wq_send = qkv_weight(place, h1_t, gqkv, qkv_order)
            low_in, high_in, wq_keep, wq_send = lax.optimization_barrier(
                (low_in, high_in, wq_keep, wq_send)
            )
        up = jnp.concatenate([add_low(gh1[1][:local], low_in), gh1[1][local:]], axis=0)
        down = jnp.concatenate([gh1[3][:local], add_low(gh1[3][local:], high_in)], axis=0)
        terms = [gh1[0], links.shift(up, 1), links.shift(down, -1)]
    else:
        terms = [gh1[0]] + [links.shift(gh1[k], k) for k in range(1, nz)]
    if fast:
        dw1_in, dw2_in, dwo, wq_send = lax.optimization_barrier((dw1_in, dw2_in, dwo, wq_send))
        dw1 = dw1 + dw1_in.astype(F32)
        dw2 = dw2 + dw2_in.astype(F32)
        dw = after(jnp.stack([dw1, dw2], axis=1).astype(BF), up, down)
        dw_came = (
            links.shift(dw[1], 1),
            links.shift(dw[3], -1),
            links.shift(dw[2], 2),
        )
        dwo = sum(t.astype(F32) for t in dwo)
        joint = jnp.concatenate(
            [add_low(wq_keep, links.core(wq_send)), dwo.astype(BF)], axis=2
        )
        joint = joint.reshape(2, 384, 384)
        vec = vec_keep + links.core(vec_send)
        vec = jnp.concatenate([vec[:3], db1[:, 0], jnp.zeros((9, 384), F32)], axis=0)
        came = links.flip(jnp.concatenate([joint[1], vec.astype(BF)], axis=0), 2)
        terms, came = lax.optimization_barrier((terms, came))
    grad_rows = input_backward(terms, x_ext, gains, gres)
    grad_in = links.core(grad_rows[local:])

    def by_micro(own, other):
        return jnp.where(c == 0, jnp.stack([own, other]), jnp.stack([other, own]))[:, None]

    outputs = by_micro(*after((out_rows[:local], rows_in), terms))
    input_grad = by_micro(grad_rows[:local], grad_in)
    if fast:
        joint = add_low(joint[0], came[:384]).reshape(2, 192, 384)
        vec = vec + came[384:].astype(F32)
        came = links.flip(jnp.concatenate([joint[1], vec.astype(BF)], axis=0), 1)
        joint = joint[0].astype(F32) + came[:192].astype(F32)
        vec = vec + came[192:].astype(F32)
        vec = [
            jnp.concatenate(
                [jnp.pad(vec[:3, 96 * k : 96 * k + 96], ((0, 0), (0, 288))), vec[3 + k : 4 + k]],
                axis=0,
            )
            for k in range(4)
        ]
        vec = sum([vec[0]] + [links.shift(vec[k], k) for k in range(1, 4)])
        vecs = (vec[0, :96], vec[1, :96], vec[3], vec[2, :96])
        g_out = joint[:, 288:]
        third = jnp.stack([joint[:, 96 * t : 96 * t + 96] for t in range(3)])
        g_qkv = jnp.concatenate(
            [
                lax.ppermute(
                    pick(third, lax.rem(2 * (i - s + 9), 3)),
                    "seq",
                    [((3 * q + i) % 8, q) for q in range(8)],
                )
                for i in range(3)
            ],
            axis=1,
        )
        dw_came, _ = lax.optimization_barrier((dw_came, (vecs, g_qkv, grad_rows)))
        dw_came = [v.astype(F32) for v in dw_came]
        dw = jnp.stack([dw1[0], dw2[0]]) + dw_came[0] + dw_came[1] + dw_came[2]
        g_fc1 = dw[0]
        keep, send = to_both((dw[1, :96], dw[1, 96:]))
        g_fc2 = jnp.concatenate(to_both((keep, links.core(send))), axis=1).T
    else:

        def owned(w):
            w = lax.psum_scatter(w.astype(BF), "seq", scatter_dimension=1, tiled=True)
            return lax.psum_scatter(w, "dp", scatter_dimension=0, tiled=True).astype(F32)

        dwq = jnp.einsum("rd,rj->dj", h1, gqkv, preferred_element_type=F32)
        spread = jnp.zeros((D, 3, nz * hw), F32)
        spread = lax.dynamic_update_slice_in_dim(
            spread, dwq.reshape(D, 3, lq)[..., :hw], z * hw, 2
        )
        g_qkv = owned(spread[..., :D].reshape(D, 3 * D))
        mixed_all = jnp.concatenate(mixed, axis=1)
        dwo = jnp.einsum("ri,ro->io", mixed_all, gproj, preferred_element_type=F32)
        dwo = dwo.reshape(nz, hw, D)
        dwo = jnp.roll(dwo[::-1], z + 1, axis=0).reshape(nz * hw, D)[:D]
        g_out = owned(dwo)
        half = jnp.stack([dw1a, dw1b]).transpose(1, 0, 3, 2, 4).reshape(D, FF // 2)
        full = lax.dynamic_update_slice_in_dim(
            jnp.zeros((D, FF), BF), half, c * (FF // 2), 1
        )
        g_fc1 = owned(full)
        half = jnp.stack([dw2a, dw2b]).transpose(0, 1, 4, 2, 3).reshape(FF // 2, D)
        full = lax.dynamic_update_slice_in_dim(
            jnp.zeros((FF, D), BF), half, c * (FF // 2), 0
        )
        g_fc2 = owned(full)
        bias_full = lax.dynamic_update_slice_in_dim(
            jnp.zeros((FF,), F32), db1.reshape(-1), c * (FF // 2), 0
        )
        bias_full = lax.psum(
            lax.psum_scatter(bias_full, "seq", scatter_dimension=0, tiled=True), "dp"
        )
        vec = vec_keep + links.core(vec_send)
        vec = vec[:3].reshape(3, nz, n_w)
        vec = sum([vec[:, 0]] + [links.shift(vec[:, k], k) for k in range(1, nz)])
        vec = lax.psum(vec, "dp")
        vecs = (vec[0], vec[1], bias_full, vec[2])

    return (
        outputs,
        input_grad,
        vecs[0],
        g_qkv,
        g_out,
        vecs[1],
        g_fc1,
        vecs[2],
        g_fc2,
        vecs[3],
    )


def solution(mesh):
    rows = P(None, "dp", "seq", None)
    labels = P(None, "dp", "seq")
    matrix = P("dp", "seq")
    vector = P("seq")
    return jax.shard_map(
        functools.partial(per_device, mesh.shape["dp"], mesh.shape["seq"]),
        mesh=mesh,
        in_specs=(
            rows, labels, labels, labels, vector, matrix, matrix, vector, matrix, vector, matrix,
            vector, rows,
        ),
        out_specs=(
            rows, rows, vector, matrix, matrix, vector, matrix, vector, matrix, vector,
        ),
        check_vma=False,
    )
```

```python
import functools

import jax
import jax.numpy as jnp
import numpy as np
from jax import lax
from jax.experimental import pallas as pl
from jax.experimental.pallas import tpu as pltpu
from jax.sharding import PartitionSpec as P

D = 768
H = 12
HD = 64
FF = 3072
BLK = 16
F32 = jnp.float32
BF = jnp.bfloat16
NEG = -1e30
VMEM_LIMIT = 56 * 1024 * 1024


def cost(flops, nbytes, scale=1e-3):
    return pl.CostEstimate(
        flops=int(flops * scale), bytes_accessed=int(nbytes * scale), transcendentals=0
    )


def params(*semantics):
    return pltpu.CompilerParams(
        dimension_semantics=semantics or None, vmem_limit_bytes=VMEM_LIMIT
    )


def dot(a, b):
    return lax.dot_general(a, b, (((1,), (0,)), ((), ())), preferred_element_type=F32)


def dot_t(a, b):
    return lax.dot_general(a, b, (((1,), (1,)), ((), ())), preferred_element_type=F32)


def whole(shape):
    return pl.BlockSpec(shape, lambda *_: (0,) * len(shape))


def cuts(count, step):
    return [(at, min(step, count - at)) for at in range(0, count, step)]


def lane_mask(width, head):
    lanes = lax.broadcasted_iota(jnp.int32, (1, width), 1)
    return jnp.where(lanes // HD == head, 1.0, 0.0).astype(BF)


def per_head(block, heads):
    return jnp.concatenate([block * lane_mask(block.shape[1], h) for h in range(heads)], axis=0)


def swap_halves(v):
    out = []
    for at in range(0, v.shape[1], 128):
        part = v[:, at : at + 128]
        lanes = lax.broadcasted_iota(jnp.int32, part.shape, 1)
        out.append(
            jnp.where(
                lanes % HD < HD // 2,
                pltpu.roll(part, 128 - HD // 2, 1),
                pltpu.roll(part, HD // 2, 1),
            )
        )
    return jnp.concatenate(out, axis=1)


def widen(table, width):
    return jnp.concatenate([table] * (width // 128), axis=1)


def cos_sin(angle):
    turns = jnp.round(angle * np.float32(2.0 / np.pi))
    left = angle - turns * np.float32(1.5703125)
    left = left - turns * np.float32(4.837512969970703125e-4)
    left = left - turns * np.float32(7.54978995489188e-8)
    sq = left * left
    sine = left + left * sq * (
        np.float32(-1.6666654611e-1)
        + sq * (np.float32(8.3321608736e-3) + sq * np.float32(-1.9515295891e-4))
    )
    cosine = (
        1.0
        - 0.5 * sq
        + sq
        * sq
        * (
            np.float32(4.166664568298827e-2)
            + sq * (np.float32(-1.388731625493765e-3) + sq * np.float32(2.443315711809948e-5))
        )
    )
    quarter = jnp.bitwise_and(turns.astype(jnp.int32), 3)
    odd = jnp.bitwise_and(quarter, 1) == 1
    sin_out = jnp.where(odd, cosine, sine)
    cos_out = jnp.where(odd, sine, cosine)
    sin_out = jnp.where(quarter >= 2, -sin_out, sin_out)
    cos_out = jnp.where((quarter == 1) | (quarter == 2), -cos_out, cos_out)
    return cos_out, sin_out


def normed(v):
    centered = v - jnp.mean(v, axis=1, keepdims=True)
    var = jnp.mean(centered * centered, axis=1, keepdims=True)
    rstd = lax.rsqrt(var + 1e-05)
    return centered * rstd, rstd


def fold8(v, op):
    return op(v.reshape(v.shape[0] // 8, 8, v.shape[1]), axis=0)


def pair_mask(kcol_ref, rows, codes):
    key = kcol_ref[rows, 3:4]
    low, high, same = codes
    return ((key >= low) & (key < high)) | (key == same)


def query_codes(qrow_ref, at, count):
    cols = pl.ds(at, count)
    return qrow_ref[0:1, cols], qrow_ref[1:2, cols], qrow_ref[2:3, cols]


SUB = 64


def chosen(step, entries):
    value = jnp.int32(entries[0])
    for i, e in enumerate(entries[1:], 1):
        value = jnp.where(step == i, jnp.int32(e), value)
    return value


def attend(step, entries, q_ref, k_ref, vt_ref, kcol_ref, qrow_ref, s_scr, p_scr, heads, chunk):
    blocks = k_ref.shape[0] // chunk
    lq = k_ref.shape[1]
    at = pl.multiple_of(chosen(step, entries) * chunk, chunk)
    codes = query_codes(qrow_ref, at, chunk)
    query = per_head(q_ref[pl.ds(at, chunk), :], heads)

    def score(block, best):
        base = pl.multiple_of(block * chunk, chunk)
        s_scr[pl.ds(base, chunk), :] = dot_t(k_ref[pl.ds(base, chunk), :], query)
        best = list(best)
        for sub in range(0, chunk, SUB):
            rows = pl.ds(base + sub, SUB)
            mask = pair_mask(kcol_ref, rows, codes)
            for h in range(heads):
                cols = slice(h * chunk, (h + 1) * chunk)
                value = jnp.where(mask, s_scr[rows, cols], NEG)
                s_scr[rows, cols] = value
                best[h] = jnp.maximum(best[h], fold8(value, jnp.max))
        return tuple(best)

    best = lax.fori_loop(
        0, blocks, score, tuple(jnp.full((8, chunk), NEG, F32) for _ in range(heads))
    )
    best = [jnp.max(b, axis=0, keepdims=True) for b in best]

    def soften(block, sums):
        base = pl.multiple_of(block * chunk, chunk)
        sums = list(sums)
        for sub in range(0, chunk, SUB):
            rows = pl.ds(base + sub, SUB)
            for h in range(heads):
                cols = slice(h * chunk, (h + 1) * chunk)
                value = jnp.exp(s_scr[rows, cols] - best[h])
                sums[h] = sums[h] + fold8(value, jnp.sum)
                p_scr[rows, cols] = value.astype(BF)
        return tuple(sums)

    sums = lax.fori_loop(
        0, blocks, soften, tuple(jnp.zeros((8, chunk), F32) for _ in range(heads))
    )
    sums = [jnp.sum(s, axis=0, keepdims=True) for s in sums]
    tops = []
    for h in range(heads):
        made = dot(vt_ref[...], p_scr[:, h * chunk : (h + 1) * chunk])
        tops.append(made[h * HD : (h + 1) * HD, :] * (1.0 / sums[h]))
    if heads * HD < lq:
        tops.append(jnp.zeros((lq - heads * HD, chunk), F32))
    logs = [best[h] + jnp.log(sums[h]) for h in range(heads)]
    logs.append(jnp.zeros((8 - heads, chunk), F32))
    return jnp.concatenate(tops, axis=0), jnp.concatenate(logs, axis=0)


def block_outputs(entries, lq, hw, chunk):
    shapes = []
    for _ in entries:
        shapes += [
            jax.ShapeDtypeStruct((chunk, hw), BF),
            jax.ShapeDtypeStruct((lq, chunk), F32),
            jax.ShapeDtypeStruct((8, chunk), F32),
        ]
    return shapes


def store_block(step, entries, refs, joined, logs, hw):
    attended = joined.T[:, :hw].astype(BF)
    for i in range(len(entries)):

        @pl.when(step == i)
        def _(i=i):
            refs[3 * i][...] = attended
            refs[3 * i + 1][...] = joined
            refs[3 * i + 2][...] = logs


def by_block(entries, made):
    return {e: tuple(made[3 * i : 3 * i + 3]) for i, e in enumerate(entries)}


def fill_rows(scr, row, which, labels, vectors, at):
    local = labels[0].shape[1]
    for i, ref in enumerate(labels):
        value = jnp.where(which == 0, ref[0:1, :], ref[1:2, :]).astype(F32)
        scr[row : row + 1, at + local * i : at + local * (i + 1)] = value
    for i, ref in enumerate(vectors):
        scr[row + 1 : row + 2, 128 * i : 128 * i + ref.shape[1]] = ref[...]


def message_rows(place, x, labels, vectors):
    local = x.shape[1]

    def kernel(place_ref, x_ref, *refs):
        label_refs, vector_refs, out_ref, scr = refs[:3], refs[3:7], refs[7], refs[8]
        other = 1 - place_ref[2]
        out_ref[:local, :] = x_ref[other]
        scr[...] = jnp.zeros_like(scr)
        fill_rows(scr, 0, other, label_refs, vector_refs, 0)
        out_ref[local:, :] = scr[...].astype(BF)

    ins = [x] + list(labels) + list(vectors)
    return pl.pallas_call(
        kernel,
        name="message_rows",
        grid_spec=pltpu.PrefetchScalarGridSpec(
            num_scalar_prefetch=1,
            grid=(1,),
            in_specs=[whole(a.shape) for a in ins],
            out_specs=whole((local + 16, D)),
            scratch_shapes=[pltpu.VMEM((16, D), F32)],
        ),
        out_shape=jax.ShapeDtypeStruct((local + 16, D), BF),
        compiler_params=params("arbitrary"),
        cost_estimate=cost(1e6, 1e6),
    )(place, *ins)


def own_rows(place, x, labels, vectors, came):
    local = x.shape[1]

    def kernel(place_ref, x_ref, *refs):
        label_refs, vector_refs, came_ref, out_ref, scr = refs[:3], refs[3:7], *refs[7:]
        own = place_ref[2]
        out_ref[:local, :] = x_ref[own]
        out_ref[local : 2 * local, :] = came_ref[:local, :]
        scr[...] = jnp.zeros_like(scr)
        fill_rows(scr, 0, own, label_refs, vector_refs, 0)
        extra = came_ref[local:, :].astype(F32)
        scr[0:1, 3 * local : 6 * local] = extra[0:1, : 3 * local]
        scr[2:3, :] = extra[1:2, :]
        out_ref[2 * local :, :] = scr[...].astype(BF)

    ins = [x] + list(labels) + list(vectors) + [came]
    return pl.pallas_call(
        kernel,
        name="own_rows",
        grid_spec=pltpu.PrefetchScalarGridSpec(
            num_scalar_prefetch=1,
            grid=(1,),
            in_specs=[whole(a.shape) for a in ins],
            out_specs=whole((2 * local + 16, D)),
            scratch_shapes=[pltpu.VMEM((16, D), F32)],
        ),
        out_shape=jax.ShapeDtypeStruct((2 * local + 16, D), BF),
        compiler_params=params("arbitrary"),
        cost_estimate=cost(1e6, 1e6),
    )(place, *ins)


def attention_first(place, arrays, plan, extras, freq, wq, order, heads, chunk, entries, widths):
    blocks = len(extras)
    total = blocks * chunk
    local = chunk // 2
    hw = heads * HD
    lq = -(-hw // 128) * 128
    count = len(arrays)
    parts = len(wq)
    n_w, b_w = widths
    fixed = 11

    def kernel(place_ref, *refs):
        x_refs = refs[:count]
        freq_ref, order_ref = refs[count : count + 2]
        wq_refs = refs[count + 2 : count + 2 + parts]
        outs = refs[count + 2 + parts :]
        h1_ref, q_ref, k_ref, v_ref, vt_ref, cs_ref, sn_ref, kcol_ref, qrow_ref, gain_ref, wq_ref = (
            outs[:fixed]
        )
        bias_ref = outs[fixed]
        block_refs = outs[fixed + 1 : fixed + 1 + 3 * len(entries)]
        s_scr, p_scr, g_scr = outs[fixed + 1 + 3 * len(entries) :]
        step = pl.program_id(0)
        d, c = place_ref[0], place_ref[2]

        @pl.when(step == 0)
        def _():
            g_scr[...] = jnp.zeros_like(g_scr)
            bias_ref[...] = jnp.zeros_like(bias_ref)
            turn = lax.broadcasted_iota(jnp.int32, (1, chunk), 1) % BLK
            for k, (which, at) in enumerate(extras):
                rows = x_refs[which][at : at + 16, :].astype(F32)

                def label(i, rows=rows):
                    return jnp.concatenate(
                        [
                            rows[0:1, i * local : (i + 1) * local],
                            rows[0:1, (3 + i) * local : (4 + i) * local],
                        ],
                        axis=1,
                    )

                segment, flag, block = label(0), label(1), label(2)
                start = segment * 4096.0
                clean = flag > 0.5
                key = start + jnp.where(clean, block, block + 2048.0)
                place_now = block * BLK + turn.astype(F32)
                coded = jnp.concatenate(
                    [
                        start,
                        start + block + flag,
                        jnp.where(clean, -1.0, key),
                        key,
                        place_now,
                        jnp.zeros((3, chunk), F32),
                    ],
                    axis=0,
                )
                qrow_ref[:, k * chunk : (k + 1) * chunk] = coded
                kcol_ref[k * chunk : (k + 1) * chunk, :] = coded.T
                for half in range(2):
                    vector = rows[1 + half : 2 + half, :]
                    lane = 384 * half + n_w * k
                    for i in range(3):
                        g_scr[i : i + 1, lane : lane + n_w] = vector[:, 128 * i : 128 * i + n_w]
                if parts == 2:
                    bias_ref[k : k + 1, :b_w] = rows[1:2, 384 : 384 + b_w]
            gain_ref[...] = dot_t(g_scr[...].astype(BF), order_ref[...])
            if parts == 2:
                for half in range(2):

                    @pl.when(c == half)
                    def _(half=half):
                        for j in range(4):
                            rows = slice(192 * j, 192 * j + 192)
                            for t in range(3):
                                for i in range(2):
                                    at = lq * t + 96 * (i ^ half)
                                    wq_ref[rows, at : at + 96] = wq_refs[i][
                                        d ^ j, :, 96 * t : 96 * t + 96
                                    ]

                for t in range(3):
                    if hw < lq:
                        wq_ref[:, lq * t + hw : lq * (t + 1)] = jnp.zeros((D, lq - hw), BF)
            else:
                wq_ref[...] = wq_refs[0][...]
            gain_row = gain_ref[0:1, :]
            for which, src, dst, rows in plan:
                for at, size in cuts(rows, 64):
                    xhat, _ = normed(x_refs[which][src + at : src + at + size, :].astype(F32))
                    h1_ref[dst + at : dst + at + size, :] = (xhat * gain_row).astype(BF)
            lanes = lax.broadcasted_iota(jnp.int32, (1, 128), 1)
            sign = jnp.where(lanes % HD < HD // 2, -1.0, 1.0)

            def project(block, carry):
                rows = pl.ds(pl.multiple_of(block * chunk, chunk), chunk)
                cosine, sine = cos_sin(kcol_ref[rows, 4:5] * freq_ref[...])
                sine = sine * sign
                cs_ref[rows, :] = cosine
                sn_ref[rows, :] = sine
                cosine = widen(cosine, lq)
                sine = widen(sine, lq)
                made = dot(h1_ref[rows, :], wq_ref[...])
                q = made[:, :lq]
                q_ref[rows, :] = ((q * cosine + swap_halves(q) * sine).astype(BF) * 0.125).astype(
                    BF
                )
                k = made[:, lq : 2 * lq]
                k_ref[rows, :] = (k * cosine + swap_halves(k) * sine).astype(BF)
                v = made[:, 2 * lq :]
                v_ref[rows, :] = v.astype(BF)
                vt_ref[:, rows] = v.T.astype(BF)
                return carry

            lax.fori_loop(0, blocks, project, 0)

        joined, logs = attend(
            step, entries, q_ref, k_ref, vt_ref, kcol_ref, qrow_ref, s_scr, p_scr, heads, chunk
        )
        store_block(step, entries, block_refs, joined, logs, hw)

    ins = list(arrays) + [freq, order] + list(wq)
    out_shape = [
        jax.ShapeDtypeStruct((total, D), BF),
        jax.ShapeDtypeStruct((total, lq), BF),
        jax.ShapeDtypeStruct((total, lq), BF),
        jax.ShapeDtypeStruct((total, lq), BF),
        jax.ShapeDtypeStruct((lq, total), BF),
        jax.ShapeDtypeStruct((total, 128), F32),
        jax.ShapeDtypeStruct((total, 128), F32),
        jax.ShapeDtypeStruct((total, 8), F32),
        jax.ShapeDtypeStruct((8, total), F32),
        jax.ShapeDtypeStruct((16, D), F32),
        jax.ShapeDtypeStruct((D, 3 * lq), BF),
        jax.ShapeDtypeStruct((-(-blocks // 8) * 8, 384), F32),
    ] + block_outputs(entries, lq, hw, chunk)
    made = pl.pallas_call(
        kernel,
        name="attention_first",
        grid_spec=pltpu.PrefetchScalarGridSpec(
            num_scalar_prefetch=1,
            grid=(len(entries),),
            in_specs=[whole(v.shape) for v in ins],
            out_specs=[whole(o.shape) for o in out_shape],
            scratch_shapes=[
                pltpu.VMEM((total, heads * chunk), F32),
                pltpu.VMEM((total, heads * chunk), BF),
                pltpu.VMEM((16, D), F32),
            ],
        ),
        out_shape=out_shape,
        compiler_params=params("arbitrary"),
        cost_estimate=cost(8e9, 8e6),
    )(place, *ins)
    return made[:12], by_block(entries, made[12:])


def attention_rest(saved, heads, chunk, entries):
    q, k, vt, kcol, qrow = saved
    total, lq = k.shape
    hw = heads * HD

    def kernel(q_ref, k_ref, vt_ref, kcol_ref, qrow_ref, *refs):
        step = pl.program_id(0)
        s_scr, p_scr = refs[3 * len(entries) :]
        joined, logs = attend(
            step, entries, q_ref, k_ref, vt_ref, kcol_ref, qrow_ref, s_scr, p_scr, heads, chunk
        )
        store_block(step, entries, refs, joined, logs, hw)

    ins = [q, k, vt, kcol, qrow]
    out_shape = block_outputs(entries, lq, hw, chunk)
    made = pl.pallas_call(
        kernel,
        name="attention_rest",
        grid=(len(entries),),
        in_specs=[whole(v.shape) for v in ins],
        out_specs=[whole(o.shape) for o in out_shape],
        out_shape=out_shape,
        scratch_shapes=[
            pltpu.VMEM((total, heads * chunk), F32),
            pltpu.VMEM((total, heads * chunk), BF),
        ],
        compiler_params=params("arbitrary"),
        cost_estimate=cost(5e9, 4e6),
    )(*ins)
    return by_block(entries, made)


def attention_backward(pulls, by, saved, heads, chunk, entries, before, finish):
    h1, q, k, v, _, cs, sn, kcol, qrow, gains, wq = saved[:11]
    last = finish is not None
    total, lq = k.shape
    blocks = total // chunk
    hw = heads * HD
    n = len(entries)
    halves = blocks == 4
    pieces = blocks + 1 if halves else blocks

    def kernel(*refs):
        g_refs, att_refs, lse_refs = refs[:n], refs[n : 2 * n], refs[2 * n : 3 * n]
        q_ref, k_ref, v_ref, cs_ref, sn_ref, kcol_ref, qrow_ref = refs[3 * n : 3 * n + 7]
        refs = refs[3 * n + 7 :]
        if last:
            dq_in, dk_in, dv_in, wq_ref, h1_ref, gains_ref, sums_ref, order_ref = refs[:8]
            gqkv_ref, keep_ref, send_ref = refs[8:11]
            gh_refs = refs[11 : 11 + pieces]
            scr = refs[11 + pieces :]
        else:
            dq_out, dk_out, dv_out = refs[:3]
            scr = refs[3:]
        g_scr, row_scr, kt_scr, dk_scr, dv_scr, s_scr, dp_scr, pb_scr, ds_scr, dst_scr = scr
        step = pl.program_id(0)

        @pl.when(step == 0)
        def _():
            for i in range(n):
                g_scr[i, :, :hw] = g_refs[i][...]
                if hw < lq:
                    g_scr[i, :, hw:] = jnp.zeros((chunk, lq - hw), BF)
                product = g_scr[i].astype(F32).T * att_refs[i][...]
                for h in range(heads):
                    row_scr[i, h : h + 1, :] = jnp.sum(
                        product[h * HD : (h + 1) * HD, :], axis=0, keepdims=True
                    )
                row_scr[i, 8:16, :] = lse_refs[i][...]
            if last:
                dk_scr[...] = dk_in[...]
                dv_scr[...] = dv_in[...]
            else:
                dk_scr[...] = jnp.zeros_like(dk_scr)
                dv_scr[...] = jnp.zeros_like(dv_scr)

            def turn(block, carry):
                rows = pl.ds(pl.multiple_of(block * chunk, chunk), chunk)
                flat = k_ref[rows, :].astype(F32).T
                line = lax.broadcasted_iota(jnp.int32, (lq, 1), 0) // HD
                for h in range(heads):
                    kt_scr[block, :, h * chunk : (h + 1) * chunk] = jnp.where(
                        line == h, flat, 0.0
                    ).astype(BF)
                return carry

            lax.fori_loop(0, blocks, turn, 0)

        at = pl.multiple_of(chosen(step, entries) * chunk, chunk)
        own = pl.ds(at, chunk)
        codes = query_codes(qrow_ref, at, chunk)
        query = per_head(q_ref[own, :], heads)
        pull = per_head(g_scr[step], heads)
        delta = [row_scr[step, h : h + 1, :] for h in range(heads)]
        top = [row_scr[step, 8 + h : 9 + h, :] for h in range(heads)]

        def keys(block, dq_t):
            base = pl.multiple_of(block * chunk, chunk)
            rows = pl.ds(base, chunk)
            s_scr[...] = dot_t(k_ref[rows, :], query)
            dp_scr[...] = dot_t(v_ref[rows, :], pull)
            for sub in range(0, chunk, SUB):
                part = slice(sub, sub + SUB)
                mask = pair_mask(kcol_ref, pl.ds(base + sub, SUB), codes)
                for h in range(heads):
                    cols = slice(h * chunk, (h + 1) * chunk)
                    prob = jnp.exp(jnp.where(mask, s_scr[part, cols] - top[h], NEG))
                    slope = (prob * (dp_scr[part, cols] - delta[h])).astype(BF)
                    pb_scr[part, cols] = prob.astype(BF)
                    ds_scr[part, cols] = slope
                    dst_scr[h * chunk + sub : h * chunk + sub + SUB, :] = slope
            dv_scr[rows, :] += dot(pb_scr[...], pull)
            dk_scr[rows, :] += dot(ds_scr[...], query)
            return dq_t + dot(kt_scr[block], dst_scr[...])

        dq_t = lax.fori_loop(0, blocks, keys, jnp.zeros((lq, chunk), F32))

        def unrotate(value, rows):
            return value * widen(cs_ref[rows, :], lq) - swap_halves(value) * widen(
                sn_ref[rows, :], lq
            )

        dq = unrotate(dq_t.T * 0.125, own).astype(BF)
        if not last:
            dq_out[...] = dq

            @pl.when(step == n - 1)
            def _():
                dk_out[...] = dk_scr[...]
                dv_out[...] = dv_scr[...]

        else:
            gqkv_ref[own, :lq] = dq

            @pl.when(step == n - 1)
            def _():
                gqkv_ref[0:chunk, :lq] = dq_in[...]
                n1 = jnp.zeros((8, D), F32)
                for b in range(blocks):
                    rows = slice(b * chunk, (b + 1) * chunk)
                    gqkv_ref[rows, lq : 2 * lq] = unrotate(dk_scr[rows, :], rows).astype(BF)
                    gqkv_ref[rows, 2 * lq :] = dv_scr[rows, :].astype(BF)
                    gh = dot_t(gqkv_ref[rows, :], wq_ref[...])
                    if halves and b == 2:
                        gh_refs[2][...] = gh[: chunk // 2, :].astype(BF)
                        gh_refs[4][...] = gh[chunk // 2 :, :].astype(BF)
                    else:
                        gh_refs[b][...] = gh.astype(gh_refs[b].dtype)
                    n1 = n1 + fold8(gh * h1_ref[rows, :].astype(F32), jnp.sum)
                lines = [
                    jnp.sum(n1, axis=0, keepdims=True) / gains_ref[0:1, :],
                    jnp.sum(sums_ref[0:8, :], axis=0, keepdims=True),
                    jnp.sum(sums_ref[8:16, :], axis=0, keepdims=True),
                    jnp.zeros((13, D), F32),
                ]
                lines = jnp.concatenate(lines, axis=0)
                high = lines.astype(BF)
                rest = (lines - high.astype(F32)).astype(BF)
                lines = dot(high, order_ref[...]) + dot(rest, order_ref[...])
                keep_ref[...] = lines[:, :384]
                send_ref[...] = lines[:, 384:]

    ins = [pulls[e] for e in entries] + [by[e][1] for e in entries] + [by[e][2] for e in entries]
    ins += [q, k, v, cs, sn, kcol, qrow]
    if last:
        ins += list(before) + [wq, h1, gains] + list(finish)
        out_shape = [
            jax.ShapeDtypeStruct((total, 3 * lq), BF),
            jax.ShapeDtypeStruct((16, 384), F32),
            jax.ShapeDtypeStruct((16, 384), F32),
        ]
        for b in range(pieces):
            rows = chunk // 2 if halves and b in (2, 4) else chunk
            out_shape.append(jax.ShapeDtypeStruct((rows, D), F32 if b == 0 else BF))
    else:
        out_shape = [
            jax.ShapeDtypeStruct((chunk, lq), BF),
            jax.ShapeDtypeStruct((total, lq), F32),
            jax.ShapeDtypeStruct((total, lq), F32),
        ]
    return pl.pallas_call(
        kernel,
        name="attention_backward_last" if last else "attention_backward_own",
        grid=(n,),
        in_specs=[whole(a.shape) for a in ins],
        out_specs=[whole(o.shape) for o in out_shape],
        out_shape=out_shape,
        scratch_shapes=[
            pltpu.VMEM((n, chunk, lq), BF),
            pltpu.VMEM((n, 16, chunk), F32),
            pltpu.VMEM((blocks, lq, heads * chunk), BF),
            pltpu.VMEM((total, lq), F32),
            pltpu.VMEM((total, lq), F32),
            pltpu.VMEM((chunk, heads * chunk), F32),
            pltpu.VMEM((chunk, heads * chunk), F32),
            pltpu.VMEM((chunk, heads * chunk), BF),
            pltpu.VMEM((chunk, heads * chunk), BF),
            pltpu.VMEM((heads * chunk, chunk), BF),
        ],
        compiler_params=params("arbitrary"),
        cost_estimate=cost(3e9 * n, 1e7),
    )(*ins)


def dot_first(a, b):
    return lax.dot_general(a, b, (((0,), (0,)), ((), ())), preferred_element_type=F32)


def reorder_out(place, own, other, order):
    def kernel(place_ref, own_ref, other_ref, order_ref, out_ref, scr):
        d = place_ref[0]
        for j in range(4):
            for k in range(4):
                at = 96 * k
                part = slice(96 * j, 96 * j + 96)
                scr[j, :, at : at + 96] = own_ref[k, :, part]
                scr[j, :, 384 + at : 384 + at + 96] = other_ref[k, :, part]
        for j in range(4):
            out_ref[j] = dot_t(scr[d ^ j], order_ref[...]).astype(BF)

    return pl.pallas_call(
        kernel,
        name="reorder_out",
        grid_spec=pltpu.PrefetchScalarGridSpec(
            num_scalar_prefetch=1,
            grid=(1,),
            in_specs=[whole(own.shape), whole(other.shape), whole(order.shape)],
            out_specs=whole((4, 192, D)),
            scratch_shapes=[pltpu.VMEM((4, 192, 768), BF)],
        ),
        out_shape=jax.ShapeDtypeStruct((4, 192, D), BF),
        compiler_params=params("arbitrary"),
        cost_estimate=cost(1e9, 3e6),
    )(place, own, other, order)


def qkv_weight(place, h1_t, gqkv, order):
    def kernel(place_ref, h_ref, g_ref, order_ref, keep_ref, send_ref):
        d = place_ref[0]
        made = dot(h_ref[...], g_ref[...]).astype(BF)
        made = dot(made, order_ref[...]).astype(BF)
        for j in range(4):
            rows = slice(192 * j, 192 * j + 192)
            keep_ref[d ^ j] = made[rows, :288]
            send_ref[d ^ j] = made[rows, 384:672]

    shape = jax.ShapeDtypeStruct((4, 192, 288), BF)
    return pl.pallas_call(
        kernel,
        name="qkv_weight",
        grid_spec=pltpu.PrefetchScalarGridSpec(
            num_scalar_prefetch=1,
            grid=(1,),
            in_specs=[whole(h1_t.shape), whole(gqkv.shape), whole(order.shape)],
            out_specs=[whole(shape.shape)] * 2,
        ),
        out_shape=[shape, shape],
        compiler_params=params("arbitrary"),
        cost_estimate=cost(2e9, 5e6),
    )(place, h1_t, gqkv, order)


def out_weight(place, mixed, gproj, order):
    groups = len(mixed)

    def kernel(place_ref, *refs):
        m_refs = refs[:groups]
        g_ref, order_ref, keep_ref, send_ref = refs[groups:]
        d, z = place_ref[0], place_ref[1]
        for k in range(groups):
            made = dot_first(m_refs[k][...], g_ref[...]).astype(BF)
            made = dot(made, order_ref[...]).astype(BF)
            row = d ^ lax.rem(z + (groups - k), groups)
            keep_ref[row] = made[:, :384]
            send_ref[row] = made[:, 384:]

    ins = list(mixed) + [gproj, order]
    shape = jax.ShapeDtypeStruct((4, 192, 384), BF)
    return pl.pallas_call(
        kernel,
        name="out_weight",
        grid_spec=pltpu.PrefetchScalarGridSpec(
            num_scalar_prefetch=1,
            grid=(1,),
            in_specs=[whole(a.shape) for a in ins],
            out_specs=[whole(shape.shape)] * 2,
        ),
        out_shape=[shape, shape],
        compiler_params=params("arbitrary"),
        cost_estimate=cost(1e9, 4e6),
    )(place, *ins)


def output_projection(place, mixed, wout, x, gain):
    groups = len(mixed)
    rows = mixed[0].shape[0]

    def kernel(place_ref, *refs):
        m_refs = refs[:groups]
        w_ref, x_ref, gain_ref, res_ref, h2_ref = refs[groups:]
        z = place_ref[1]
        total = x_ref[:rows, :].astype(F32)
        for k in range(groups):
            total = total + dot(m_refs[k][...], w_ref[lax.rem(z + (groups - k), groups)])
        res_ref[...] = total
        for at, size in cuts(rows, 64):
            xhat, _ = normed(res_ref[at : at + size, :])
            h2_ref[at : at + size, :] = (xhat * gain_ref[1:2, :]).astype(BF)

    ins = list(mixed) + [wout, x, gain]
    return pl.pallas_call(
        kernel,
        name="output_projection",
        grid_spec=pltpu.PrefetchScalarGridSpec(
            num_scalar_prefetch=1,
            grid=(1,),
            in_specs=[whole(a.shape) for a in ins],
            out_specs=[whole((rows, D)), whole((rows, D))],
        ),
        out_shape=[jax.ShapeDtypeStruct((rows, D), F32), jax.ShapeDtypeStruct((rows, D), BF)],
        compiler_params=params("arbitrary"),
        cost_estimate=cost(1e9, 3e6),
    )(place, *ins)


def feed_forward(place, h2_own, h2_other, cot, cot_in, weights, bias):
    rows = h2_own.shape[0]
    both = 2 * rows
    width = 384

    def kernel(
        place_ref, ho_ref, hp_ref, go_ref, gp_ref, w1a_ref, w1b_ref, w2a_ref, w2b_ref, b_ref,
        out_own, out_other, gh_own, gh_other, d1a_ref, d1b_ref, d2a_ref, d2b_ref, db_ref,
        h_scr, g_scr, ht_scr, gt_scr, w1_scr, w2_scr, pre_scr, ga_scr, act_scr, slope_scr, out_scr,
        gh_scr, dw_scr,
    ):
        step = pl.program_id(0)
        d = place_ref[0]
        z = place_ref[1]
        c = place_ref[2]

        @pl.when(step == 0)
        def _():
            h_scr[:rows, :] = ho_ref[...]
            h_scr[rows:, :] = hp_ref[...]
            local = rows // 2
            g_scr[:local, :] = go_ref[c]
            g_scr[local:rows, :] = gp_ref[c]
            g_scr[rows : rows + local, :] = gp_ref[1 - c]
            g_scr[rows + local :, :] = go_ref[1 - c]
            for at in range(0, both, 256):
                part = slice(at, at + 256)
                ht_scr[:, part] = h_scr[part, :].astype(F32).T.astype(BF)
                gt_scr[:, part] = g_scr[part, :].astype(F32).T.astype(BF)

        near = lax.rem(step - z + 4, 4)
        hidden = step ^ d
        for odd in range(2):

            @pl.when(d % 2 == odd)
            def _(odd=odd):
                for j in range(4):
                    src = (w1a_ref, w1b_ref)[odd ^ (j % 2)]
                    w1_scr[192 * j : 192 * j + 192, :] = src[(d ^ j) // 2, near]

            @pl.when(hidden // 2 == odd)
            def _(odd=odd):
                for j in range(4):
                    src = (w2a_ref, w2b_ref)[odd]
                    w2_scr[192 * j : 192 * j + 192, :] = src[hidden % 2, lax.rem(j - z + 4, 4)]

        pre_scr[...] = dot(h_scr[...], w1_scr[...])
        ga_scr[...] = dot(g_scr[...], w2_scr[...])
        bias_row = b_ref[pl.ds(near, 1), :]
        total = jnp.zeros((8, width), F32)
        for at in range(0, both, 32):
            part = slice(at, at + 32)
            u = pre_scr[part, :] + bias_row
            usq = u * u
            c = np.float32(np.sqrt(2.0 / np.pi))
            t = jnp.tanh(c * (u + np.float32(0.044715) * (usq * u)))
            half = 0.5 * (1.0 + t)
            act_scr[part, :] = (u * half).astype(BF)
            rise = half + 0.5 * u * (1.0 - t * t) * (c * (1.0 + np.float32(0.134145) * usq))
            slope = (ga_scr[part, :] * rise).astype(BF)
            slope_scr[part, :] = slope
            total = total + fold8(slope.astype(F32), jnp.sum)
        db_ref[0] = jnp.sum(total, axis=0, keepdims=True)

        out_now = dot_t(act_scr[...], w2_scr[...])
        gh_now = dot_t(slope_scr[...], w1_scr[...])

        @pl.when(step == 0)
        def _():
            out_scr[...] = out_now
            gh_scr[...] = gh_now

        @pl.when(step > 0)
        def _():
            out_scr[...] += out_now
            gh_scr[...] += gh_now

        dw_scr[0] = dot(ht_scr[...], slope_scr[...]).astype(BF)
        dw_scr[1] = dot(gt_scr[...], act_scr[...]).astype(BF)
        for odd in range(2):

            @pl.when(d % 2 == odd)
            def _(odd=odd):
                for j in range(4):
                    dst = (d1a_ref, d1b_ref)[odd ^ (j % 2)]
                    dst[(d ^ j) // 2, near] = dw_scr[0, 192 * j : 192 * j + 192, :]

            @pl.when(hidden // 2 == odd)
            def _(odd=odd):
                for j in range(4):
                    dst = (d2a_ref, d2b_ref)[odd]
                    dst[hidden % 2, lax.rem(j - z + 4, 4)] = dw_scr[1, 192 * j : 192 * j + 192, :]

        @pl.when(step == 3)
        def _():
            out_own[...] = out_scr[:rows, :]
            out_other[...] = out_scr[rows:, :].astype(BF)
            gh_own[...] = gh_scr[:rows, :]
            gh_other[...] = gh_scr[rows:, :].astype(BF)

    def by_z(i, place_ref):
        return (lax.rem(i - place_ref[1] + 4, 4), 0, 0)

    ins = [h2_own, h2_other, cot, cot_in] + list(weights) + [bias]
    full = jax.ShapeDtypeStruct((2, 4, 192, width), BF)
    out_shape = [
        jax.ShapeDtypeStruct((rows, D), F32),
        jax.ShapeDtypeStruct((rows, D), BF),
        jax.ShapeDtypeStruct((rows, D), F32),
        jax.ShapeDtypeStruct((rows, D), BF),
        full,
        full,
        full,
        full,
        jax.ShapeDtypeStruct((4, 1, width), F32),
    ]
    return pl.pallas_call(
        kernel,
        name="feed_forward",
        grid_spec=pltpu.PrefetchScalarGridSpec(
            num_scalar_prefetch=1,
            grid=(4,),
            in_specs=[whole(a.shape) for a in ins],
            out_specs=[whole(o.shape) for o in out_shape[:-1]]
            + [pl.BlockSpec((1, 1, width), by_z)],
            scratch_shapes=[
                pltpu.VMEM((both, D), BF),
                pltpu.VMEM((both, D), BF),
                pltpu.VMEM((D, both), BF),
                pltpu.VMEM((D, both), BF),
                pltpu.VMEM((D, width), BF),
                pltpu.VMEM((D, width), BF),
                pltpu.VMEM((both, width), F32),
                pltpu.VMEM((both, width), F32),
                pltpu.VMEM((both, width), BF),
                pltpu.VMEM((both, width), BF),
                pltpu.VMEM((both, D), F32),
                pltpu.VMEM((both, D), F32),
                pltpu.VMEM((2, D, width), BF),
            ],
        ),
        out_shape=out_shape,
        compiler_params=params("arbitrary"),
        cost_estimate=cost(7.2e9, 1.5e7),
    )(place, *ins)


def residual_backward(place, gh_own, gh_in, residual, cot, cot_in, gain, wout):
    rows, local = residual.shape[0], cot.shape[1]
    groups, hw = wout.shape[0], wout.shape[1]

    def kernel(place_ref, gh_ref, gi_ref, res_ref, ca_ref, cb_ref, gain_ref, w_ref, *outs):
        gres_ref, gproj_ref, vec_ref = outs[:3]
        gm_refs = outs[3:]
        z, c = place_ref[1], place_ref[2]
        gain_row = gain_ref[1:2, :]
        gsum = jnp.zeros((8, D), F32)
        bsum = jnp.zeros((8, D), F32)
        for at, size in cuts(rows, 32):
            part = slice(at, at + size)
            xhat, rstd = normed(res_ref[part, :])
            dy_now = (ca_ref, cb_ref)[at // local][c, at % local : at % local + size, :].astype(F32)
            grad = gh_ref[part, :] + gi_ref[part, :].astype(F32)
            along = grad * xhat
            gsum = gsum + fold8(along, jnp.sum)
            bsum = bsum + fold8(dy_now, jnp.sum)
            u = grad * gain_row
            back = (
                u
                - jnp.mean(u, axis=1, keepdims=True)
                - xhat * jnp.mean(along * gain_row, axis=1, keepdims=True)
            )
            value = dy_now + back * rstd
            gres_ref[part, :] = value
            gproj_ref[part, :] = value.astype(BF)
        vec_ref[0:8, :] = gsum
        vec_ref[8:16, :] = bsum
        for k in range(groups):
            gm_refs[k][...] = dot_t(gproj_ref[...], w_ref[lax.rem(z + k, groups)]).astype(BF)

    ins = [gh_own, gh_in, residual, cot, cot_in, gain, wout]
    out_shape = [
        jax.ShapeDtypeStruct((rows, D), F32),
        jax.ShapeDtypeStruct((rows, D), BF),
        jax.ShapeDtypeStruct((16, D), F32),
    ] + [jax.ShapeDtypeStruct((rows, hw), BF) for _ in range(groups)]
    made = pl.pallas_call(
        kernel,
        name="residual_backward",
        grid_spec=pltpu.PrefetchScalarGridSpec(
            num_scalar_prefetch=1,
            grid=(1,),
            in_specs=[whole(a.shape) for a in ins],
            out_specs=[whole(o.shape) for o in out_shape],
        ),
        out_shape=out_shape,
        compiler_params=params("arbitrary"),
        cost_estimate=cost(1e9, 4e6),
    )(place, *ins)
    return made[0], made[1], made[2], made[3:]


def input_backward(terms, x, gain, gres):
    rows = gres.shape[0]
    count = len(terms)

    def kernel(*refs):
        x_ref, gain_ref, gres_ref, out_ref = refs[count:]
        for at, size in cuts(rows, 32):
            part = slice(at, at + size)
            grad = refs[0][part, :].astype(F32)
            for t in range(1, count):
                grad = grad + refs[t][part, :].astype(F32)
            xhat, rstd = normed(x_ref[part, :].astype(F32))
            u = grad * gain_ref[0:1, :]
            back = (
                u
                - jnp.mean(u, axis=1, keepdims=True)
                - xhat * jnp.mean(u * xhat, axis=1, keepdims=True)
            )
            out_ref[part, :] = (gres_ref[part, :] + back * rstd).astype(BF)

    ins = list(terms) + [x, gain, gres]
    return pl.pallas_call(
        kernel,
        name="input_backward",
        grid=(1,),
        in_specs=[whole(a.shape) for a in ins],
        out_specs=whole((rows, D)),
        out_shape=jax.ShapeDtypeStruct((rows, D), BF),
        compiler_params=params("arbitrary"),
        cost_estimate=cost(1e8, 3e6),
    )(*ins)


def add_low(a, b):
    return (a.astype(F32) + b.astype(F32)).astype(BF)


def pick(v, index):
    return lax.dynamic_index_in_dim(v, index, 0, keepdims=False)


def after(v, *others):
    return lax.optimization_barrier((v, others))[0]


class Links:
    def __init__(self, n_dp, n_seq):
        self.n_dp, self.n_seq, self.nz = n_dp, n_seq, n_seq // 2

    def core(self, v):
        return lax.ppermute(v, "seq", [(s, s ^ 1) for s in range(self.n_seq)])

    def flip(self, v, bit):
        return lax.ppermute(v, "dp", [(i, i ^ bit) for i in range(self.n_dp)])

    def shift(self, v, k):
        n = self.nz
        return lax.ppermute(
            v, "seq", [(s, 2 * ((s // 2 + k) % n) + s % 2) for s in range(self.n_seq)]
        )


def order_matrix(source, valid):
    rows = lax.broadcasted_iota(jnp.int32, (768, 768), 0)
    return jnp.where((rows == source[None, :]) & valid[None, :], 1.0, 0.0).astype(BF)


def per_device(
    n_dp,
    n_seq,
    inputs,
    row_segment,
    row_flag,
    row_block,
    norm1_scale,
    w_qkv,
    w_out,
    norm2_scale,
    w_fc1,
    b_fc1,
    w_fc2,
    b_fc2,
    cotangent,
):
    links = Links(n_dp, n_seq)
    nz = links.nz
    local = inputs.shape[2]
    chunk = 2 * local
    heads = -(-H // nz)
    hw = heads * HD
    lq = -(-hw // 128) * 128
    fast = n_dp == 4 and nz == 4 and H % nz == 0
    d = lax.axis_index("dp")
    s = lax.axis_index("seq")
    z = s // 2
    c = s % 2
    place = jnp.stack([d, z, c]).astype(jnp.int32)
    n_w, b_w = D // n_seq, FF // n_seq
    cols = jnp.arange(768, dtype=jnp.int32)
    side, at = cols // 384, cols % 384
    out_order = order_matrix(
        n_w * (2 * ((z + at // n_w) % nz) + (c ^ side)) + at % n_w, at < 384
    )

    def to_both(w):
        return jnp.where(c == 0, w[0], w[1]), jnp.where(c == 0, w[1], w[0])

    x_loc = inputs[:, 0]
    labels = (row_segment[:, 0], row_flag[:, 0], row_block[:, 0])
    vectors = tuple(v.reshape(1, -1) for v in (norm1_scale, norm2_scale, b_fc2, b_fc1))
    came = links.core(message_rows(place, x_loc, labels, vectors))
    x_ext = own_rows(place, x_loc, labels, vectors, came)
    if nz == 4:
        x_before = links.shift(x_ext, 1)
        x_after = links.shift(x_ext, -1)
        x_low = links.shift(x_before[:144], 1)
        x_high = links.shift(x_after[144:], -1)
        gathered = [[x_ext], [x_after], [x_low, x_high], [x_before]]
    else:
        gathered = [[x_ext]] + [[links.shift(x_ext, -k)] for k in range(1, nz)]
    arrays, plan, extras = [], [], []
    for k, pieces in enumerate(gathered):
        at = 0
        for piece in pieces:
            rows = min(piece.shape[0], chunk - at)
            plan.append((len(arrays), 0, k * chunk + at, rows))
            at += rows
            arrays.append(piece)
        extras.append((len(arrays) - 1, pieces[-1].shape[0] - 16))
    freq = np.tile(
        np.float32(10000.0) ** (np.float32(-2.0) * np.arange(32, dtype=np.float32) / HD), 4
    )
    freq = jnp.asarray(freq.astype(np.float32)[None, :])
    cot = cotangent[:, 0]

    if fast:
        two = w_fc2.astype(BF).T.reshape(96, 2, 384)
        two_keep, two_send = to_both((two[:, 0], two[:, 1]))
        two = jnp.concatenate(to_both((two_keep, links.core(two_send))), axis=0)
        w12 = jnp.stack([w_fc1.astype(BF), two])
        w_before = links.shift(w12, 1)
        w_after = links.shift(w12, -1)
        w1_two = links.shift(w_before[0], 1)
        w2_two = links.shift(w_after[1], -1)
        w1 = jnp.stack([w12[0], w_after[0], w1_two, w_before[0]])
        w2 = jnp.stack([w12[1], w_after[1], w2_two, w_before[1]])

        qkv_order = order_matrix(
            256 * (cols % 384 // 96) + 96 * (c ^ side) + cols % 96, cols % 384 < 288
        )
        wq_parts = after(w_qkv.astype(BF), x_ext)
        parts = []
        for i in range(3):
            parts.append(
                lax.ppermute(
                    wq_parts[:, 96 * i : 96 * i + 96],
                    "seq",
                    [(q, (3 * q + i) % 8) for q in range(8)],
                )
            )
        parts = after(jnp.stack(parts), x_before, x_after)
        wq_own = jnp.concatenate(
            [pick(parts, (2 * t + s) % 3) for t in range(3)] + [w_out.astype(BF)], axis=1
        )
        wq_own = jnp.stack([wq_own, links.flip(wq_own, 1)])
        wq_own = jnp.stack([wq_own, links.flip(wq_own, 2)]).reshape(4, 192, 384)
        wq_own, qkv_order, out_order = lax.optimization_barrier((wq_own, qkv_order, out_order))
        wq = (wq_own, links.core(wq_own))
        wo_own = jnp.concatenate([wq_own[j, :, 288:] for j in range(4)], axis=1)

        arrays, w1, w2, wo_own = lax.optimization_barrier((arrays, w1, w2, wo_own))
        w1_in = links.flip(w1, 2)
        w2_in = links.flip(w2, 1)
        wo_all = [wo_own] + [links.shift(wo_own, -k) for k in range(1, 4)]
        ff_place = place
    else:

        def everywhere(w):
            w = lax.all_gather(w.astype(BF), "seq", axis=1, tiled=True)
            return lax.all_gather(w, "dp", axis=0, tiled=True)

        wq = everywhere(w_qkv).reshape(D, 3, D)
        wq = jnp.pad(wq, ((0, 0), (0, 0), (0, nz * hw - D)))
        wq = lax.dynamic_slice_in_dim(wq, z * hw, hw, 2)
        wq = (jnp.pad(wq, ((0, 0), (0, 0), (0, lq - hw))).reshape(D, 3 * lq),)
        wout = jnp.pad(everywhere(w_out), ((0, nz * hw - D), (0, 0))).reshape(nz, hw, D)
        w1 = lax.dynamic_slice_in_dim(everywhere(w_fc1), c * (FF // 2), FF // 2, 1)
        w1 = w1.reshape(2, 2, 192, 4, 384).transpose(3, 1, 0, 2, 4)
        w2 = lax.dynamic_slice_in_dim(everywhere(w_fc2), c * (FF // 2), FF // 2, 0)
        w2 = w2.reshape(2, 2, 384, 4, 192).transpose(3, 1, 0, 4, 2)
        w1, w2 = w1.transpose(1, 2, 0, 3, 4), w2.transpose(2, 1, 0, 3, 4)
        weights = (w1[0], w1[1], w2[0], w2[1])
        bias_all = lax.all_gather(b_fc1.astype(BF), "seq", axis=0, tiled=True).astype(F32)
        bias = lax.dynamic_slice_in_dim(bias_all, c * (FF // 2), FF // 2, 0).reshape(4, 384)
        bias = jnp.pad(bias, ((0, 4), (0, 0)))
        ff_place = jnp.stack([0 * d, 0 * z, c]).astype(jnp.int32)
    cot_in = links.core(after(cot, arrays))

    far = sorted(range(1, nz), key=lambda k: -min(k, nz - k))
    first = far[: nz // 2]
    rest = far[nz // 2 :] + [0]
    saved, by = attention_first(
        place, arrays, plan, extras, freq, wq, out_order, heads, chunk, first, (n_w, b_w)
    )
    h1, gains = saved[0], saved[9]
    rest_in = tuple(saved[i] for i in (1, 2, 4, 7, 8))
    if fast:
        bias = saved[11]
        w1_in, w2_in, wo_all, _ = lax.optimization_barrier((w1_in, w2_in, wo_all, h1))
        w1a = jnp.stack([w1, w1_in])
        w2a = jnp.stack([w2, w2_in])
        wo_all = jnp.stack(wo_all)
        wo_in = links.core(wo_all)
        w1b = links.flip(w1a, 1)
        w2b = links.flip(w2a, 2)
        weights = (w1a, w1b, w2a, w2b)
        rest_in = after(rest_in, w1a, w2a, wo_all)
    mixed = {k: links.shift(by[k][0], k) for k in first}
    by = {**by, **attention_rest(rest_in, heads, chunk, rest)}
    for k in rest:
        mixed[k] = links.shift(by[k][0], k) if k else by[k][0]
    mixed = [mixed[k] for k in range(nz)]
    h1_t = after(h1, by[0][0]).T
    if fast:
        wout = reorder_out(place, after(wo_all, by[0][0]), wo_in, out_order)
    residual, h2 = output_projection(place, mixed, wout, after(x_ext, h1_t), gains)
    h2_in = links.core(h2)
    (out_own, out_other, gh_own, gh_other, dw1a, dw1b, dw2a, dw2b, db1) = feed_forward(
        ff_place, h2, h2_in, cot, cot_in, weights, bias
    )
    gh_in = links.core(gh_other)
    out_in = links.core(out_other)
    gres, gproj, sums, gmixed = residual_backward(
        place, gh_own, gh_in, residual, cot, cot_in, gains, wout
    )
    if fast:
        dw1_in = links.flip(dw1b, 1)
        dw2_in = links.flip(dw2b, 2)
    pulled = [gmixed[0]] + [links.shift(gmixed[k], k) for k in range(1, nz)]
    pulled = [pulled[(nz - k) % nz] for k in range(nz)]
    part = attention_backward(pulled, by, saved, heads, chunk, [0], None, None)
    if fast:
        part, pulled, gproj = lax.optimization_barrier((part, pulled, gproj))
    out_rows = (residual + out_own + out_in.astype(F32) + gains[2:3]).astype(BF)
    rows_in = links.core(out_rows[local:])
    if fast:
        wo_keep, wo_send = out_weight(place, mixed, gproj, out_order)
        wo_came = links.core(wo_send)
        dw1_in, dw2_in, _ = lax.optimization_barrier((dw1_in, dw2_in, wo_keep))
        dw1_sum = add_low(dw1a[1], dw1_in[1])
        dw2_sum = add_low(dw2a[1], dw2_in[1])
        dwo = [
            add_low(wo_keep[..., 96 * k : 96 * k + 96], wo_came[..., 96 * k : 96 * k + 96])
            for k in range(4)
        ]
        dw1 = dw1a[0].astype(F32) + dw1_in[0].astype(F32)
        dw2 = dw2a[0].astype(F32) + dw2_in[0].astype(F32)
        part, dwo, dw1_sum, dw2_sum, dw1, dw2, _ = lax.optimization_barrier(
            (part, dwo, dw1_sum, dw2_sum, dw1, dw2, out_rows)
        )
        dw1_in = links.flip(dw1_sum, 2)
        dw2_in = links.flip(dw2_sum, 1)
        dwo = [dwo[0]] + [links.shift(dwo[k], k) for k in range(1, 4)]
    made = attention_backward(
        pulled, by, saved, heads, chunk, list(range(1, nz)), part, (sums, out_order)
    )
    if fast:
        made, dwo, dw1_in, dw2_in, rows_in = lax.optimization_barrier(
            (made, dwo, dw1_in, dw2_in, rows_in)
        )
    gqkv, vec_keep, vec_send, gh1 = made[0], made[1], made[2], made[3:]
    if nz == 4:
        low_in = links.shift(gh1[2], 1)
        high_in = links.shift(gh1[4], -1)
        if fast:
            wq_keep, wq_send = qkv_weight(place, h1_t, gqkv, qkv_order)
            low_in, high_in, wq_keep, wq_send = lax.optimization_barrier(
                (low_in, high_in, wq_keep, wq_send)
            )
        up = jnp.concatenate([add_low(gh1[1][:local], low_in), gh1[1][local:]], axis=0)
        down = jnp.concatenate([gh1[3][:local], add_low(gh1[3][local:], high_in)], axis=0)
        terms = [gh1[0], links.shift(up, 1), links.shift(down, -1)]
    else:
        terms = [gh1[0]] + [links.shift(gh1[k], k) for k in range(1, nz)]
    if fast:
        dw1_in, dw2_in, dwo, wq_send = lax.optimization_barrier((dw1_in, dw2_in, dwo, wq_send))
        dw1 = dw1 + dw1_in.astype(F32)
        dw2 = dw2 + dw2_in.astype(F32)
        dw = after(jnp.stack([dw1, dw2], axis=1).astype(BF), up, down)
        dw_came = (
            links.shift(dw[1], 1),
            links.shift(dw[3], -1),
            links.shift(dw[2], 2),
        )
        dwo = sum(t.astype(F32) for t in dwo)
        joint = jnp.concatenate(
            [add_low(wq_keep, links.core(wq_send)), dwo.astype(BF)], axis=2
        )
        joint = joint.reshape(2, 384, 384)
        vec = vec_keep + links.core(vec_send)
        vec = jnp.concatenate([vec[:3], db1[:, 0], jnp.zeros((9, 384), F32)], axis=0)
        came = links.flip(jnp.concatenate([joint[1], vec.astype(BF)], axis=0), 2)
        terms, came = lax.optimization_barrier((terms, came))
    grad_rows = input_backward(terms, x_ext, gains, gres)
    grad_in = links.core(grad_rows[local:])

    def by_micro(own, other):
        return jnp.where(c == 0, jnp.stack([own, other]), jnp.stack([other, own]))[:, None]

    outputs = by_micro(*after((out_rows[:local], rows_in), terms))
    input_grad = by_micro(grad_rows[:local], grad_in)
    if fast:
        joint = add_low(joint[0], came[:384]).reshape(2, 192, 384)
        vec = vec + came[384:].astype(F32)
        came = links.flip(jnp.concatenate([joint[1], vec.astype(BF)], axis=0), 1)
        joint = joint[0].astype(F32) + came[:192].astype(F32)
        vec = vec + came[192:].astype(F32)
        vec = [
            jnp.concatenate(
                [jnp.pad(vec[:3, 96 * k : 96 * k + 96], ((0, 0), (0, 288))), vec[3 + k : 4 + k]],
                axis=0,
            )
            for k in range(4)
        ]
        vec = sum([vec[0]] + [links.shift(vec[k], k) for k in range(1, 4)])
        vecs = (vec[0, :96], vec[1, :96], vec[3], vec[2, :96])
        g_out = joint[:, 288:]
        third = jnp.stack([joint[:, 96 * t : 96 * t + 96] for t in range(3)])
        g_qkv = jnp.concatenate(
            [
                lax.ppermute(
                    pick(third, lax.rem(2 * (i - s + 9), 3)),
                    "seq",
                    [((3 * q + i) % 8, q) for q in range(8)],
                )
                for i in range(3)
            ],
            axis=1,
        )
        dw_came, _ = lax.optimization_barrier((dw_came, (vecs, g_qkv, grad_rows)))
        dw_came = [v.astype(F32) for v in dw_came]
        dw = jnp.stack([dw1[0], dw2[0]]) + dw_came[0] + dw_came[1] + dw_came[2]
        g_fc1 = dw[0]
        keep, send = to_both((dw[1, :96], dw[1, 96:]))
        g_fc2 = jnp.concatenate(to_both((keep, links.core(send))), axis=1).T
    else:

        def owned(w):
            w = lax.psum_scatter(w.astype(BF), "seq", scatter_dimension=1, tiled=True)
            return lax.psum_scatter(w, "dp", scatter_dimension=0, tiled=True).astype(F32)

        dwq = jnp.einsum("rd,rj->dj", h1, gqkv, preferred_element_type=F32)
        spread = jnp.zeros((D, 3, nz * hw), F32)
        spread = lax.dynamic_update_slice_in_dim(
            spread, dwq.reshape(D, 3, lq)[..., :hw], z * hw, 2
        )
        g_qkv = owned(spread[..., :D].reshape(D, 3 * D))
        mixed_all = jnp.concatenate(mixed, axis=1)
        dwo = jnp.einsum("ri,ro->io", mixed_all, gproj, preferred_element_type=F32)
        dwo = dwo.reshape(nz, hw, D)
        dwo = jnp.roll(dwo[::-1], z + 1, axis=0).reshape(nz * hw, D)[:D]
        g_out = owned(dwo)
        half = jnp.stack([dw1a, dw1b]).transpose(1, 0, 3, 2, 4).reshape(D, FF // 2)
        full = lax.dynamic_update_slice_in_dim(
            jnp.zeros((D, FF), BF), half, c * (FF // 2), 1
        )
        g_fc1 = owned(full)
        half = jnp.stack([dw2a, dw2b]).transpose(0, 1, 4, 2, 3).reshape(FF // 2, D)
        full = lax.dynamic_update_slice_in_dim(
            jnp.zeros((FF, D), BF), half, c * (FF // 2), 0
        )
        g_fc2 = owned(full)
        bias_full = lax.dynamic_update_slice_in_dim(
            jnp.zeros((FF,), F32), db1.reshape(-1), c * (FF // 2), 0
        )
        bias_full = lax.psum(
            lax.psum_scatter(bias_full, "seq", scatter_dimension=0, tiled=True), "dp"
        )
        vec = vec_keep + links.core(vec_send)
        vec = vec[:3].reshape(3, nz, n_w)
        vec = sum([vec[:, 0]] + [links.shift(vec[:, k], k) for k in range(1, nz)])
        vec = lax.psum(vec, "dp")
        vecs = (vec[0], vec[1], bias_full, vec[2])

    return (
        outputs,
        input_grad,
        vecs[0],
        g_qkv,
        g_out,
        vecs[1],
        g_fc1,
        vecs[2],
        g_fc2,
        vecs[3],
    )


def solution(mesh):
    rows = P(None, "dp", "seq", None)
    labels = P(None, "dp", "seq")
    matrix = P("dp", "seq")
    vector = P("seq")
    return jax.shard_map(
        functools.partial(per_device, mesh.shape["dp"], mesh.shape["seq"]),
        mesh=mesh,
        in_specs=(
            rows, labels, labels, labels, vector, matrix, matrix, vector, matrix, vector, matrix,
            vector, rows,
        ),
        out_specs=(
            rows, rows, vector, matrix, matrix, vector, matrix, vector, matrix, vector,
        ),
        check_vma=False,
    )
```

```python
import functools

import jax
import jax.numpy as jnp
import numpy as np
from jax import lax
from jax.experimental import pallas as pl
from jax.experimental.pallas import tpu as pltpu
from jax.sharding import PartitionSpec as P

D = 768
H = 12
HD = 64
FF = 3072
BLK = 16
F32 = jnp.float32
BF = jnp.bfloat16
NEG = -1e30
VMEM_LIMIT = 56 * 1024 * 1024


def cost(flops, nbytes, scale=1e-3):
    return pl.CostEstimate(
        flops=int(flops * scale), bytes_accessed=int(nbytes * scale), transcendentals=0
    )


def params(*semantics):
    return pltpu.CompilerParams(
        dimension_semantics=semantics or None, vmem_limit_bytes=VMEM_LIMIT
    )


def dot(a, b):
    return lax.dot_general(a, b, (((1,), (0,)), ((), ())), preferred_element_type=F32)


def dot_t(a, b):
    return lax.dot_general(a, b, (((1,), (1,)), ((), ())), preferred_element_type=F32)


def whole(shape):
    return pl.BlockSpec(shape, lambda *_: (0,) * len(shape))


def cuts(count, step):
    return [(at, min(step, count - at)) for at in range(0, count, step)]


def lane_mask(width, head):
    lanes = lax.broadcasted_iota(jnp.int32, (1, width), 1)
    return jnp.where(lanes // HD == head, 1.0, 0.0).astype(BF)


def per_head(block, heads):
    return jnp.concatenate([block * lane_mask(block.shape[1], h) for h in range(heads)], axis=0)


def swap_halves(v):
    out = []
    for at in range(0, v.shape[1], 128):
        part = v[:, at : at + 128]
        lanes = lax.broadcasted_iota(jnp.int32, part.shape, 1)
        out.append(
            jnp.where(
                lanes % HD < HD // 2,
                pltpu.roll(part, 128 - HD // 2, 1),
                pltpu.roll(part, HD // 2, 1),
            )
        )
    return jnp.concatenate(out, axis=1)


def widen(table, width):
    return jnp.concatenate([table] * (width // 128), axis=1)


def cos_sin(angle):
    turns = jnp.round(angle * np.float32(2.0 / np.pi))
    left = angle - turns * np.float32(1.5703125)
    left = left - turns * np.float32(4.837512969970703125e-4)
    left = left - turns * np.float32(7.54978995489188e-8)
    sq = left * left
    sine = left + left * sq * (
        np.float32(-1.6666654611e-1)
        + sq * (np.float32(8.3321608736e-3) + sq * np.float32(-1.9515295891e-4))
    )
    cosine = (
        1.0
        - 0.5 * sq
        + sq
        * sq
        * (
            np.float32(4.166664568298827e-2)
            + sq * (np.float32(-1.388731625493765e-3) + sq * np.float32(2.443315711809948e-5))
        )
    )
    quarter = jnp.bitwise_and(turns.astype(jnp.int32), 3)
    odd = jnp.bitwise_and(quarter, 1) == 1
    sin_out = jnp.where(odd, cosine, sine)
    cos_out = jnp.where(odd, sine, cosine)
    sin_out = jnp.where(quarter >= 2, -sin_out, sin_out)
    cos_out = jnp.where((quarter == 1) | (quarter == 2), -cos_out, cos_out)
    return cos_out, sin_out


def normed(v):
    centered = v - jnp.mean(v, axis=1, keepdims=True)
    var = jnp.mean(centered * centered, axis=1, keepdims=True)
    rstd = lax.rsqrt(var + 1e-05)
    return centered * rstd, rstd


def fold8(v, op):
    return op(v.reshape(v.shape[0] // 8, 8, v.shape[1]), axis=0)


def pair_mask(kcol_ref, rows, codes):
    key = kcol_ref[rows, 3:4]
    low, high, same = codes
    return ((key >= low) & (key < high)) | (key == same)


def query_codes(qrow_ref, at, count):
    cols = pl.ds(at, count)
    return qrow_ref[0:1, cols], qrow_ref[1:2, cols], qrow_ref[2:3, cols]


SUB = 64


def chosen(step, entries):
    value = jnp.int32(entries[0])
    for i, e in enumerate(entries[1:], 1):
        value = jnp.where(step == i, jnp.int32(e), value)
    return value


def attend(step, entries, q_ref, k_ref, vt_ref, kcol_ref, qrow_ref, s_scr, p_scr, heads, chunk):
    blocks = k_ref.shape[0] // chunk
    lq = k_ref.shape[1]
    at = pl.multiple_of(chosen(step, entries) * chunk, chunk)
    codes = query_codes(qrow_ref, at, chunk)
    query = per_head(q_ref[pl.ds(at, chunk), :], heads)

    def score(block, best):
        base = pl.multiple_of(block * chunk, chunk)
        s_scr[pl.ds(base, chunk), :] = dot_t(k_ref[pl.ds(base, chunk), :], query)
        best = list(best)
        for sub in range(0, chunk, SUB):
            rows = pl.ds(base + sub, SUB)
            mask = pair_mask(kcol_ref, rows, codes)
            for h in range(heads):
                cols = slice(h * chunk, (h + 1) * chunk)
                value = jnp.where(mask, s_scr[rows, cols], NEG)
                s_scr[rows, cols] = value
                best[h] = jnp.maximum(best[h], fold8(value, jnp.max))
        return tuple(best)

    best = lax.fori_loop(
        0, blocks, score, tuple(jnp.full((8, chunk), NEG, F32) for _ in range(heads))
    )
    best = [jnp.max(b, axis=0, keepdims=True) for b in best]

    def soften(block, sums):
        base = pl.multiple_of(block * chunk, chunk)
        sums = list(sums)
        for sub in range(0, chunk, SUB):
            rows = pl.ds(base + sub, SUB)
            for h in range(heads):
                cols = slice(h * chunk, (h + 1) * chunk)
                value = jnp.exp(s_scr[rows, cols] - best[h])
                sums[h] = sums[h] + fold8(value, jnp.sum)
                p_scr[rows, cols] = value.astype(BF)
        return tuple(sums)

    sums = lax.fori_loop(
        0, blocks, soften, tuple(jnp.zeros((8, chunk), F32) for _ in range(heads))
    )
    sums = [jnp.sum(s, axis=0, keepdims=True) for s in sums]
    tops = []
    for h in range(heads):
        made = dot(vt_ref[...], p_scr[:, h * chunk : (h + 1) * chunk])
        tops.append(made[h * HD : (h + 1) * HD, :] * (1.0 / sums[h]))
    if heads * HD < lq:
        tops.append(jnp.zeros((lq - heads * HD, chunk), F32))
    logs = [best[h] + jnp.log(sums[h]) for h in range(heads)]
    logs.append(jnp.zeros((8 - heads, chunk), F32))
    return jnp.concatenate(tops, axis=0), jnp.concatenate(logs, axis=0)


def block_outputs(entries, lq, hw, chunk):
    shapes = []
    for _ in entries:
        shapes += [
            jax.ShapeDtypeStruct((chunk, hw), BF),
            jax.ShapeDtypeStruct((lq, chunk), F32),
            jax.ShapeDtypeStruct((8, chunk), F32),
        ]
    return shapes


def store_block(step, entries, refs, joined, logs, hw):
    attended = joined.T[:, :hw].astype(BF)
    for i in range(len(entries)):

        @pl.when(step == i)
        def _(i=i):
            refs[3 * i][...] = attended
            refs[3 * i + 1][...] = joined
            refs[3 * i + 2][...] = logs


def by_block(entries, made):
    return {e: tuple(made[3 * i : 3 * i + 3]) for i, e in enumerate(entries)}


def fill_rows(scr, row, which, labels, vectors, at):
    local = labels[0].shape[1]
    for i, ref in enumerate(labels):
        value = jnp.where(which == 0, ref[0:1, :], ref[1:2, :]).astype(F32)
        scr[row : row + 1, at + local * i : at + local * (i + 1)] = value
    for i, ref in enumerate(vectors):
        scr[row + 1 : row + 2, 128 * i : 128 * i + ref.shape[1]] = ref[...]


def message_rows(place, x, labels, vectors):
    local = x.shape[1]

    def kernel(place_ref, x_ref, *refs):
        label_refs, vector_refs, out_ref, scr = refs[:3], refs[3:7], refs[7], refs[8]
        other = 1 - place_ref[2]
        out_ref[:local, :] = x_ref[other]
        scr[...] = jnp.zeros_like(scr)
        fill_rows(scr, 0, other, label_refs, vector_refs, 0)
        out_ref[local:, :] = scr[...].astype(BF)

    ins = [x] + list(labels) + list(vectors)
    return pl.pallas_call(
        kernel,
        name="message_rows",
        grid_spec=pltpu.PrefetchScalarGridSpec(
            num_scalar_prefetch=1,
            grid=(1,),
            in_specs=[whole(a.shape) for a in ins],
            out_specs=whole((local + 16, D)),
            scratch_shapes=[pltpu.VMEM((16, D), F32)],
        ),
        out_shape=jax.ShapeDtypeStruct((local + 16, D), BF),
        compiler_params=params("arbitrary"),
        cost_estimate=cost(1e6, 1e6),
    )(place, *ins)


def own_rows(place, x, labels, vectors, came):
    local = x.shape[1]

    def kernel(place_ref, x_ref, *refs):
        label_refs, vector_refs, came_ref, out_ref, scr = refs[:3], refs[3:7], *refs[7:]
        own = place_ref[2]
        out_ref[:local, :] = x_ref[own]
        out_ref[local : 2 * local, :] = came_ref[:local, :]
        scr[...] = jnp.zeros_like(scr)
        fill_rows(scr, 0, own, label_refs, vector_refs, 0)
        extra = came_ref[local:, :].astype(F32)
        scr[0:1, 3 * local : 6 * local] = extra[0:1, : 3 * local]
        scr[2:3, :] = extra[1:2, :]
        out_ref[2 * local :, :] = scr[...].astype(BF)

    ins = [x] + list(labels) + list(vectors) + [came]
    return pl.pallas_call(
        kernel,
        name="own_rows",
        grid_spec=pltpu.PrefetchScalarGridSpec(
            num_scalar_prefetch=1,
            grid=(1,),
            in_specs=[whole(a.shape) for a in ins],
            out_specs=whole((2 * local + 16, D)),
            scratch_shapes=[pltpu.VMEM((16, D), F32)],
        ),
        out_shape=jax.ShapeDtypeStruct((2 * local + 16, D), BF),
        compiler_params=params("arbitrary"),
        cost_estimate=cost(1e6, 1e6),
    )(place, *ins)


def attention_first(place, arrays, plan, extras, freq, wq, order, heads, chunk, entries, widths):
    blocks = len(extras)
    total = blocks * chunk
    local = chunk // 2
    hw = heads * HD
    lq = -(-hw // 128) * 128
    count = len(arrays)
    parts = len(wq)
    n_w, b_w = widths
    fixed = 11

    def kernel(place_ref, *refs):
        x_refs = refs[:count]
        freq_ref, order_ref = refs[count : count + 2]
        wq_refs = refs[count + 2 : count + 2 + parts]
        outs = refs[count + 2 + parts :]
        h1_ref, q_ref, k_ref, v_ref, vt_ref, cs_ref, sn_ref, kcol_ref, qrow_ref, gain_ref, wq_ref = (
            outs[:fixed]
        )
        bias_ref = outs[fixed]
        block_refs = outs[fixed + 1 : fixed + 1 + 3 * len(entries)]
        s_scr, p_scr, g_scr = outs[fixed + 1 + 3 * len(entries) :]
        step = pl.program_id(0)
        d, c = place_ref[0], place_ref[2]

        @pl.when(step == 0)
        def _():
            g_scr[...] = jnp.zeros_like(g_scr)
            bias_ref[...] = jnp.zeros_like(bias_ref)
            turn = lax.broadcasted_iota(jnp.int32, (1, chunk), 1) % BLK
            for k, (which, at) in enumerate(extras):
                rows = x_refs[which][at : at + 16, :].astype(F32)

                def label(i, rows=rows):
                    return jnp.concatenate(
                        [
                            rows[0:1, i * local : (i + 1) * local],
                            rows[0:1, (3 + i) * local : (4 + i) * local],
                        ],
                        axis=1,
                    )

                segment, flag, block = label(0), label(1), label(2)
                start = segment * 4096.0
                clean = flag > 0.5
                key = start + jnp.where(clean, block, block + 2048.0)
                place_now = block * BLK + turn.astype(F32)
                coded = jnp.concatenate(
                    [
                        start,
                        start + block + flag,
                        jnp.where(clean, -1.0, key),
                        key,
                        place_now,
                        jnp.zeros((3, chunk), F32),
                    ],
                    axis=0,
                )
                qrow_ref[:, k * chunk : (k + 1) * chunk] = coded
                kcol_ref[k * chunk : (k + 1) * chunk, :] = coded.T
                for half in range(2):
                    vector = rows[1 + half : 2 + half, :]
                    lane = 384 * half + n_w * k
                    for i in range(3):
                        g_scr[i : i + 1, lane : lane + n_w] = vector[:, 128 * i : 128 * i + n_w]
                if parts == 2:
                    bias_ref[k : k + 1, :b_w] = rows[1:2, 384 : 384 + b_w]
            gain_ref[...] = dot_t(g_scr[...].astype(BF), order_ref[...])
            if parts == 2:
                for half in range(2):

                    @pl.when(c == half)
                    def _(half=half):
                        for j in range(4):
                            rows = slice(192 * j, 192 * j + 192)
                            for t in range(3):
                                for i in range(2):
                                    at = lq * t + 96 * (i ^ half)
                                    wq_ref[rows, at : at + 96] = wq_refs[i][
                                        d ^ j, :, 96 * t : 96 * t + 96
                                    ]

                for t in range(3):
                    if hw < lq:
                        wq_ref[:, lq * t + hw : lq * (t + 1)] = jnp.zeros((D, lq - hw), BF)
            else:
                wq_ref[...] = wq_refs[0][...]
            gain_row = gain_ref[0:1, :]
            for which, src, dst, rows in plan:
                for at, size in cuts(rows, 64):
                    xhat, _ = normed(x_refs[which][src + at : src + at + size, :].astype(F32))
                    h1_ref[dst + at : dst + at + size, :] = (xhat * gain_row).astype(BF)
            lanes = lax.broadcasted_iota(jnp.int32, (1, 128), 1)
            sign = jnp.where(lanes % HD < HD // 2, -1.0, 1.0)

            def project(block, carry):
                rows = pl.ds(pl.multiple_of(block * chunk, chunk), chunk)
                cosine, sine = cos_sin(kcol_ref[rows, 4:5] * freq_ref[...])
                sine = sine * sign
                cs_ref[rows, :] = cosine
                sn_ref[rows, :] = sine
                cosine = widen(cosine, lq)
                sine = widen(sine, lq)
                made = dot(h1_ref[rows, :], wq_ref[...])
                q = made[:, :lq]
                q_ref[rows, :] = ((q * cosine + swap_halves(q) * sine).astype(BF) * 0.125).astype(
                    BF
                )
                k = made[:, lq : 2 * lq]
                k_ref[rows, :] = (k * cosine + swap_halves(k) * sine).astype(BF)
                v = made[:, 2 * lq :]
                v_ref[rows, :] = v.astype(BF)
                vt_ref[:, rows] = v.T.astype(BF)
                return carry

            lax.fori_loop(0, blocks, project, 0)

        joined, logs = attend(
            step, entries, q_ref, k_ref, vt_ref, kcol_ref, qrow_ref, s_scr, p_scr, heads, chunk
        )
        store_block(step, entries, block_refs, joined, logs, hw)

    ins = list(arrays) + [freq, order] + list(wq)
    out_shape = [
        jax.ShapeDtypeStruct((total, D), BF),
        jax.ShapeDtypeStruct((total, lq), BF),
        jax.ShapeDtypeStruct((total, lq), BF),
        jax.ShapeDtypeStruct((total, lq), BF),
        jax.ShapeDtypeStruct((lq, total), BF),
        jax.ShapeDtypeStruct((total, 128), F32),
        jax.ShapeDtypeStruct((total, 128), F32),
        jax.ShapeDtypeStruct((total, 8), F32),
        jax.ShapeDtypeStruct((8, total), F32),
        jax.ShapeDtypeStruct((16, D), F32),
        jax.ShapeDtypeStruct((D, 3 * lq), BF),
        jax.ShapeDtypeStruct((-(-blocks // 8) * 8, 384), F32),
    ] + block_outputs(entries, lq, hw, chunk)
    made = pl.pallas_call(
        kernel,
        name="attention_first",
        grid_spec=pltpu.PrefetchScalarGridSpec(
            num_scalar_prefetch=1,
            grid=(len(entries),),
            in_specs=[whole(v.shape) for v in ins],
            out_specs=[whole(o.shape) for o in out_shape],
            scratch_shapes=[
                pltpu.VMEM((total, heads * chunk), F32),
                pltpu.VMEM((total, heads * chunk), BF),
                pltpu.VMEM((16, D), F32),
            ],
        ),
        out_shape=out_shape,
        compiler_params=params("arbitrary"),
        cost_estimate=cost(8e9, 8e6),
    )(place, *ins)
    return made[:12], by_block(entries, made[12:])


def attention_rest(saved, heads, chunk, entries):
    q, k, vt, kcol, qrow = saved
    total, lq = k.shape
    hw = heads * HD

    def kernel(q_ref, k_ref, vt_ref, kcol_ref, qrow_ref, *refs):
        step = pl.program_id(0)
        s_scr, p_scr = refs[3 * len(entries) :]
        joined, logs = attend(
            step, entries, q_ref, k_ref, vt_ref, kcol_ref, qrow_ref, s_scr, p_scr, heads, chunk
        )
        store_block(step, entries, refs, joined, logs, hw)

    ins = [q, k, vt, kcol, qrow]
    out_shape = block_outputs(entries, lq, hw, chunk)
    made = pl.pallas_call(
        kernel,
        name="attention_rest",
        grid=(len(entries),),
        in_specs=[whole(v.shape) for v in ins],
        out_specs=[whole(o.shape) for o in out_shape],
        out_shape=out_shape,
        scratch_shapes=[
            pltpu.VMEM((total, heads * chunk), F32),
            pltpu.VMEM((total, heads * chunk), BF),
        ],
        compiler_params=params("arbitrary"),
        cost_estimate=cost(5e9, 4e6),
    )(*ins)
    return by_block(entries, made)


def attention_backward(pulls, by, saved, heads, chunk, entries, before, finish):
    h1, q, k, v, _, cs, sn, kcol, qrow, gains, wq = saved[:11]
    last = finish is not None
    total, lq = k.shape
    blocks = total // chunk
    hw = heads * HD
    n = len(entries)
    halves = blocks == 4
    pieces = blocks + 1 if halves else blocks

    def kernel(*refs):
        g_refs, att_refs, lse_refs = refs[:n], refs[n : 2 * n], refs[2 * n : 3 * n]
        q_ref, k_ref, v_ref, cs_ref, sn_ref, kcol_ref, qrow_ref = refs[3 * n : 3 * n + 7]
        refs = refs[3 * n + 7 :]
        if last:
            dq_in, dk_in, dv_in, wq_ref, h1_ref, gains_ref, sums_ref, order_ref = refs[:8]
            gqkv_ref, keep_ref, send_ref = refs[8:11]
            gh_refs = refs[11 : 11 + pieces]
            scr = refs[11 + pieces :]
        else:
            dq_out, dk_out, dv_out = refs[:3]
            scr = refs[3:]
        g_scr, row_scr, kt_scr, dk_scr, dv_scr, s_scr, dp_scr, pb_scr, ds_scr, dst_scr = scr
        step = pl.program_id(0)

        @pl.when(step == 0)
        def _():
            for i in range(n):
                g_scr[i, :, :hw] = g_refs[i][...]
                if hw < lq:
                    g_scr[i, :, hw:] = jnp.zeros((chunk, lq - hw), BF)
                product = g_scr[i].astype(F32).T * att_refs[i][...]
                for h in range(heads):
                    row_scr[i, h : h + 1, :] = jnp.sum(
                        product[h * HD : (h + 1) * HD, :], axis=0, keepdims=True
                    )
                row_scr[i, 8:16, :] = lse_refs[i][...]
            if last:
                dk_scr[...] = dk_in[...]
                dv_scr[...] = dv_in[...]
            else:
                dk_scr[...] = jnp.zeros_like(dk_scr)
                dv_scr[...] = jnp.zeros_like(dv_scr)

            def turn(block, carry):
                rows = pl.ds(pl.multiple_of(block * chunk, chunk), chunk)
                flat = k_ref[rows, :].astype(F32).T
                line = lax.broadcasted_iota(jnp.int32, (lq, 1), 0) // HD
                for h in range(heads):
                    kt_scr[block, :, h * chunk : (h + 1) * chunk] = jnp.where(
                        line == h, flat, 0.0
                    ).astype(BF)
                return carry

            lax.fori_loop(0, blocks, turn, 0)

        at = pl.multiple_of(chosen(step, entries) * chunk, chunk)
        own = pl.ds(at, chunk)
        codes = query_codes(qrow_ref, at, chunk)
        query = per_head(q_ref[own, :], heads)
        pull = per_head(g_scr[step], heads)
        delta = [row_scr[step, h : h + 1, :] for h in range(heads)]
        top = [row_scr[step, 8 + h : 9 + h, :] for h in range(heads)]

        def keys(block, dq_t):
            base = pl.multiple_of(block * chunk, chunk)
            rows = pl.ds(base, chunk)
            s_scr[...] = dot_t(k_ref[rows, :], query)
            dp_scr[...] = dot_t(v_ref[rows, :], pull)
            for sub in range(0, chunk, SUB):
                part = slice(sub, sub + SUB)
                mask = pair_mask(kcol_ref, pl.ds(base + sub, SUB), codes)
                for h in range(heads):
                    cols = slice(h * chunk, (h + 1) * chunk)
                    prob = jnp.exp(jnp.where(mask, s_scr[part, cols] - top[h], NEG))
                    slope = (prob * (dp_scr[part, cols] - delta[h])).astype(BF)
                    pb_scr[part, cols] = prob.astype(BF)
                    ds_scr[part, cols] = slope
                    dst_scr[h * chunk + sub : h * chunk + sub + SUB, :] = slope
            dv_scr[rows, :] += dot(pb_scr[...], pull)
            dk_scr[rows, :] += dot(ds_scr[...], query)
            return dq_t + dot(kt_scr[block], dst_scr[...])

        dq_t = lax.fori_loop(0, blocks, keys, jnp.zeros((lq, chunk), F32))

        def unrotate(value, rows):
            return value * widen(cs_ref[rows, :], lq) - swap_halves(value) * widen(
                sn_ref[rows, :], lq
            )

        dq = unrotate(dq_t.T * 0.125, own).astype(BF)
        if not last:
            dq_out[...] = dq

            @pl.when(step == n - 1)
            def _():
                dk_out[...] = dk_scr[...]
                dv_out[...] = dv_scr[...]

        else:
            gqkv_ref[own, :lq] = dq

            @pl.when(step == n - 1)
            def _():
                gqkv_ref[0:chunk, :lq] = dq_in[...]
                n1 = jnp.zeros((8, D), F32)
                for b in range(blocks):
                    rows = slice(b * chunk, (b + 1) * chunk)
                    gqkv_ref[rows, lq : 2 * lq] = unrotate(dk_scr[rows, :], rows).astype(BF)
                    gqkv_ref[rows, 2 * lq :] = dv_scr[rows, :].astype(BF)
                    gh = dot_t(gqkv_ref[rows, :], wq_ref[...])
                    if halves and b == 2:
                        gh_refs[2][...] = gh[: chunk // 2, :].astype(BF)
                        gh_refs[4][...] = gh[chunk // 2 :, :].astype(BF)
                    else:
                        gh_refs[b][...] = gh.astype(gh_refs[b].dtype)
                    n1 = n1 + fold8(gh * h1_ref[rows, :].astype(F32), jnp.sum)
                lines = [
                    jnp.sum(n1, axis=0, keepdims=True) / gains_ref[0:1, :],
                    jnp.sum(sums_ref[0:8, :], axis=0, keepdims=True),
                    jnp.sum(sums_ref[8:16, :], axis=0, keepdims=True),
                    jnp.zeros((13, D), F32),
                ]
                lines = jnp.concatenate(lines, axis=0)
                high = lines.astype(BF)
                rest = (lines - high.astype(F32)).astype(BF)
                lines = dot(high, order_ref[...]) + dot(rest, order_ref[...])
                keep_ref[...] = lines[:, :384]
                send_ref[...] = lines[:, 384:]

    ins = [pulls[e] for e in entries] + [by[e][1] for e in entries] + [by[e][2] for e in entries]
    ins += [q, k, v, cs, sn, kcol, qrow]
    if last:
        ins += list(before) + [wq, h1, gains] + list(finish)
        out_shape = [
            jax.ShapeDtypeStruct((total, 3 * lq), BF),
            jax.ShapeDtypeStruct((16, 384), F32),
            jax.ShapeDtypeStruct((16, 384), F32),
        ]
        for b in range(pieces):
            rows = chunk // 2 if halves and b in (2, 4) else chunk
            out_shape.append(jax.ShapeDtypeStruct((rows, D), F32 if b == 0 else BF))
    else:
        out_shape = [
            jax.ShapeDtypeStruct((chunk, lq), BF),
            jax.ShapeDtypeStruct((total, lq), F32),
            jax.ShapeDtypeStruct((total, lq), F32),
        ]
    return pl.pallas_call(
        kernel,
        name="attention_backward_last" if last else "attention_backward_own",
        grid=(n,),
        in_specs=[whole(a.shape) for a in ins],
        out_specs=[whole(o.shape) for o in out_shape],
        out_shape=out_shape,
        scratch_shapes=[
            pltpu.VMEM((n, chunk, lq), BF),
            pltpu.VMEM((n, 16, chunk), F32),
            pltpu.VMEM((blocks, lq, heads * chunk), BF),
            pltpu.VMEM((total, lq), F32),
            pltpu.VMEM((total, lq), F32),
            pltpu.VMEM((chunk, heads * chunk), F32),
            pltpu.VMEM((chunk, heads * chunk), F32),
            pltpu.VMEM((chunk, heads * chunk), BF),
            pltpu.VMEM((chunk, heads * chunk), BF),
            pltpu.VMEM((heads * chunk, chunk), BF),
        ],
        compiler_params=params("arbitrary"),
        cost_estimate=cost(3e9 * n, 1e7),
    )(*ins)


def dot_first(a, b):
    return lax.dot_general(a, b, (((0,), (0,)), ((), ())), preferred_element_type=F32)


def reorder_out(place, own, other, order):
    def kernel(place_ref, own_ref, other_ref, order_ref, out_ref, scr):
        d = place_ref[0]
        for j in range(4):
            for k in range(4):
                at = 96 * k
                part = slice(96 * j, 96 * j + 96)
                scr[j, :, at : at + 96] = own_ref[k, :, part]
                scr[j, :, 384 + at : 384 + at + 96] = other_ref[k, :, part]
        for j in range(4):
            out_ref[j] = dot_t(scr[d ^ j], order_ref[...]).astype(BF)

    return pl.pallas_call(
        kernel,
        name="reorder_out",
        grid_spec=pltpu.PrefetchScalarGridSpec(
            num_scalar_prefetch=1,
            grid=(1,),
            in_specs=[whole(own.shape), whole(other.shape), whole(order.shape)],
            out_specs=whole((4, 192, D)),
            scratch_shapes=[pltpu.VMEM((4, 192, 768), BF)],
        ),
        out_shape=jax.ShapeDtypeStruct((4, 192, D), BF),
        compiler_params=params("arbitrary"),
        cost_estimate=cost(1e9, 3e6),
    )(place, own, other, order)


def qkv_weight(place, h1_t, gqkv, order):
    def kernel(place_ref, h_ref, g_ref, order_ref, keep_ref, send_ref):
        d = place_ref[0]
        made = dot(h_ref[...], g_ref[...]).astype(BF)
        made = dot(made, order_ref[...]).astype(BF)
        for j in range(4):
            rows = slice(192 * j, 192 * j + 192)
            keep_ref[d ^ j] = made[rows, :288]
            send_ref[d ^ j] = made[rows, 384:672]

    shape = jax.ShapeDtypeStruct((4, 192, 288), BF)
    return pl.pallas_call(
        kernel,
        name="qkv_weight",
        grid_spec=pltpu.PrefetchScalarGridSpec(
            num_scalar_prefetch=1,
            grid=(1,),
            in_specs=[whole(h1_t.shape), whole(gqkv.shape), whole(order.shape)],
            out_specs=[whole(shape.shape)] * 2,
        ),
        out_shape=[shape, shape],
        compiler_params=params("arbitrary"),
        cost_estimate=cost(2e9, 5e6),
    )(place, h1_t, gqkv, order)


def out_weight(place, mixed, gproj, order):
    groups = len(mixed)

    def kernel(place_ref, *refs):
        m_refs = refs[:groups]
        g_ref, order_ref, keep_ref, send_ref = refs[groups:]
        d, z = place_ref[0], place_ref[1]
        for k in range(groups):
            made = dot_first(m_refs[k][...], g_ref[...]).astype(BF)
            made = dot(made, order_ref[...]).astype(BF)
            row = d ^ lax.rem(z + (groups - k), groups)
            keep_ref[row] = made[:, :384]
            send_ref[row] = made[:, 384:]

    ins = list(mixed) + [gproj, order]
    shape = jax.ShapeDtypeStruct((4, 192, 384), BF)
    return pl.pallas_call(
        kernel,
        name="out_weight",
        grid_spec=pltpu.PrefetchScalarGridSpec(
            num_scalar_prefetch=1,
            grid=(1,),
            in_specs=[whole(a.shape) for a in ins],
            out_specs=[whole(shape.shape)] * 2,
        ),
        out_shape=[shape, shape],
        compiler_params=params("arbitrary"),
        cost_estimate=cost(1e9, 4e6),
    )(place, *ins)


def output_projection(place, mixed, wout, x, gain):
    groups = len(mixed)
    rows = mixed[0].shape[0]

    def kernel(place_ref, *refs):
        m_refs = refs[:groups]
        w_ref, x_ref, gain_ref, res_ref, h2_ref = refs[groups:]
        z = place_ref[1]
        total = x_ref[:rows, :].astype(F32)
        for k in range(groups):
            total = total + dot(m_refs[k][...], w_ref[lax.rem(z + (groups - k), groups)])
        res_ref[...] = total
        for at, size in cuts(rows, 64):
            xhat, _ = normed(res_ref[at : at + size, :])
            h2_ref[at : at + size, :] = (xhat * gain_ref[1:2, :]).astype(BF)

    ins = list(mixed) + [wout, x, gain]
    return pl.pallas_call(
        kernel,
        name="output_projection",
        grid_spec=pltpu.PrefetchScalarGridSpec(
            num_scalar_prefetch=1,
            grid=(1,),
            in_specs=[whole(a.shape) for a in ins],
            out_specs=[whole((rows, D)), whole((rows, D))],
        ),
        out_shape=[jax.ShapeDtypeStruct((rows, D), F32), jax.ShapeDtypeStruct((rows, D), BF)],
        compiler_params=params("arbitrary"),
        cost_estimate=cost(1e9, 3e6),
    )(place, *ins)


def feed_forward(place, h2_own, h2_other, cot, cot_in, weights, bias):
    rows = h2_own.shape[0]
    both = 2 * rows
    width = 384

    def kernel(
        place_ref, ho_ref, hp_ref, go_ref, gp_ref, w1a_ref, w1b_ref, w2a_ref, w2b_ref, b_ref,
        out_own, out_other, gh_own, gh_other, d1a_ref, d1b_ref, d2a_ref, d2b_ref, db_ref,
        h_scr, g_scr, ht_scr, gt_scr, w1_scr, w2_scr, pre_scr, ga_scr, act_scr, slope_scr, out_scr,
        gh_scr, dw_scr,
    ):
        step = pl.program_id(0)
        d = place_ref[0]
        z = place_ref[1]
        c = place_ref[2]

        @pl.when(step == 0)
        def _():
            h_scr[:rows, :] = ho_ref[...]
            h_scr[rows:, :] = hp_ref[...]
            local = rows // 2
            g_scr[:local, :] = go_ref[c]
            g_scr[local:rows, :] = gp_ref[c]
            g_scr[rows : rows + local, :] = gp_ref[1 - c]
            g_scr[rows + local :, :] = go_ref[1 - c]
            for at in range(0, both, 256):
                part = slice(at, at + 256)
                ht_scr[:, part] = h_scr[part, :].astype(F32).T.astype(BF)
                gt_scr[:, part] = g_scr[part, :].astype(F32).T.astype(BF)

        near = lax.rem(step - z + 4, 4)
        hidden = step ^ d
        for odd in range(2):

            @pl.when(d % 2 == odd)
            def _(odd=odd):
                for j in range(4):
                    src = (w1a_ref, w1b_ref)[odd ^ (j % 2)]
                    w1_scr[192 * j : 192 * j + 192, :] = src[(d ^ j) // 2, near]

            @pl.when(hidden // 2 == odd)
            def _(odd=odd):
                for j in range(4):
                    src = (w2a_ref, w2b_ref)[odd]
                    w2_scr[192 * j : 192 * j + 192, :] = src[hidden % 2, lax.rem(j - z + 4, 4)]

        pre_scr[...] = dot(h_scr[...], w1_scr[...])
        ga_scr[...] = dot(g_scr[...], w2_scr[...])
        bias_row = b_ref[pl.ds(near, 1), :]
        total = jnp.zeros((8, width), F32)
        for at in range(0, both, 32):
            part = slice(at, at + 32)
            u = pre_scr[part, :] + bias_row
            usq = u * u
            c = np.float32(np.sqrt(2.0 / np.pi))
            t = jnp.tanh(c * (u + np.float32(0.044715) * (usq * u)))
            half = 0.5 * (1.0 + t)
            act_scr[part, :] = (u * half).astype(BF)
            rise = half + 0.5 * u * (1.0 - t * t) * (c * (1.0 + np.float32(0.134145) * usq))
            slope = (ga_scr[part, :] * rise).astype(BF)
            slope_scr[part, :] = slope
            total = total + fold8(slope.astype(F32), jnp.sum)
        db_ref[0] = jnp.sum(total, axis=0, keepdims=True)

        out_now = dot_t(act_scr[...], w2_scr[...])
        gh_now = dot_t(slope_scr[...], w1_scr[...])

        @pl.when(step == 0)
        def _():
            out_scr[...] = out_now
            gh_scr[...] = gh_now

        @pl.when(step > 0)
        def _():
            out_scr[...] += out_now
            gh_scr[...] += gh_now

        dw_scr[0] = dot(ht_scr[...], slope_scr[...]).astype(BF)
        dw_scr[1] = dot(gt_scr[...], act_scr[...]).astype(BF)
        for odd in range(2):

            @pl.when(d % 2 == odd)
            def _(odd=odd):
                for j in range(4):
                    dst = (d1a_ref, d1b_ref)[odd ^ (j % 2)]
                    dst[(d ^ j) // 2, near] = dw_scr[0, 192 * j : 192 * j + 192, :]

            @pl.when(hidden // 2 == odd)
            def _(odd=odd):
                for j in range(4):
                    dst = (d2a_ref, d2b_ref)[odd]
                    dst[hidden % 2, lax.rem(j - z + 4, 4)] = dw_scr[1, 192 * j : 192 * j + 192, :]

        @pl.when(step == 3)
        def _():
            out_own[...] = out_scr[:rows, :]
            out_other[...] = out_scr[rows:, :].astype(BF)
            gh_own[...] = gh_scr[:rows, :]
            gh_other[...] = gh_scr[rows:, :].astype(BF)

    def by_z(i, place_ref):
        return (lax.rem(i - place_ref[1] + 4, 4), 0, 0)

    ins = [h2_own, h2_other, cot, cot_in] + list(weights) + [bias]
    full = jax.ShapeDtypeStruct((2, 4, 192, width), BF)
    out_shape = [
        jax.ShapeDtypeStruct((rows, D), F32),
        jax.ShapeDtypeStruct((rows, D), BF),
        jax.ShapeDtypeStruct((rows, D), F32),
        jax.ShapeDtypeStruct((rows, D), BF),
        full,
        full,
        full,
        full,
        jax.ShapeDtypeStruct((4, 1, width), F32),
    ]
    return pl.pallas_call(
        kernel,
        name="feed_forward",
        grid_spec=pltpu.PrefetchScalarGridSpec(
            num_scalar_prefetch=1,
            grid=(4,),
            in_specs=[whole(a.shape) for a in ins],
            out_specs=[whole(o.shape) for o in out_shape[:-1]]
            + [pl.BlockSpec((1, 1, width), by_z)],
            scratch_shapes=[
                pltpu.VMEM((both, D), BF),
                pltpu.VMEM((both, D), BF),
                pltpu.VMEM((D, both), BF),
                pltpu.VMEM((D, both), BF),
                pltpu.VMEM((D, width), BF),
                pltpu.VMEM((D, width), BF),
                pltpu.VMEM((both, width), F32),
                pltpu.VMEM((both, width), F32),
                pltpu.VMEM((both, width), BF),
                pltpu.VMEM((both, width), BF),
                pltpu.VMEM((both, D), F32),
                pltpu.VMEM((both, D), F32),
                pltpu.VMEM((2, D, width), BF),
            ],
        ),
        out_shape=out_shape,
        compiler_params=params("arbitrary"),
        cost_estimate=cost(7.2e9, 1.5e7),
    )(place, *ins)


def residual_backward(place, gh_own, gh_in, residual, cot, cot_in, gain, wout):
    rows, local = residual.shape[0], cot.shape[1]
    groups, hw = wout.shape[0], wout.shape[1]

    def kernel(place_ref, gh_ref, gi_ref, res_ref, ca_ref, cb_ref, gain_ref, w_ref, *outs):
        gres_ref, gproj_ref, vec_ref = outs[:3]
        gm_refs = outs[3:]
        z, c = place_ref[1], place_ref[2]
        gain_row = gain_ref[1:2, :]
        gsum = jnp.zeros((8, D), F32)
        bsum = jnp.zeros((8, D), F32)
        for at, size in cuts(rows, 32):
            part = slice(at, at + size)
            xhat, rstd = normed(res_ref[part, :])
            dy_now = (ca_ref, cb_ref)[at // local][c, at % local : at % local + size, :].astype(F32)
            grad = gh_ref[part, :] + gi_ref[part, :].astype(F32)
            along = grad * xhat
            gsum = gsum + fold8(along, jnp.sum)
            bsum = bsum + fold8(dy_now, jnp.sum)
            u = grad * gain_row
            back = (
                u
                - jnp.mean(u, axis=1, keepdims=True)
                - xhat * jnp.mean(along * gain_row, axis=1, keepdims=True)
            )
            value = dy_now + back * rstd
            gres_ref[part, :] = value
            gproj_ref[part, :] = value.astype(BF)
        vec_ref[0:8, :] = gsum
        vec_ref[8:16, :] = bsum
        for k in range(groups):
            gm_refs[k][...] = dot_t(gproj_ref[...], w_ref[lax.rem(z + k, groups)]).astype(BF)

    ins = [gh_own, gh_in, residual, cot, cot_in, gain, wout]
    out_shape = [
        jax.ShapeDtypeStruct((rows, D), F32),
        jax.ShapeDtypeStruct((rows, D), BF),
        jax.ShapeDtypeStruct((16, D), F32),
    ] + [jax.ShapeDtypeStruct((rows, hw), BF) for _ in range(groups)]
    made = pl.pallas_call(
        kernel,
        name="residual_backward",
        grid_spec=pltpu.PrefetchScalarGridSpec(
            num_scalar_prefetch=1,
            grid=(1,),
            in_specs=[whole(a.shape) for a in ins],
            out_specs=[whole(o.shape) for o in out_shape],
        ),
        out_shape=out_shape,
        compiler_params=params("arbitrary"),
        cost_estimate=cost(1e9, 4e6),
    )(place, *ins)
    return made[0], made[1], made[2], made[3:]


def input_backward(terms, x, gain, gres):
    rows = gres.shape[0]
    count = len(terms)

    def kernel(*refs):
        x_ref, gain_ref, gres_ref, out_ref = refs[count:]
        for at, size in cuts(rows, 32):
            part = slice(at, at + size)
            grad = refs[0][part, :].astype(F32)
            for t in range(1, count):
                grad = grad + refs[t][part, :].astype(F32)
            xhat, rstd = normed(x_ref[part, :].astype(F32))
            u = grad * gain_ref[0:1, :]
            back = (
                u
                - jnp.mean(u, axis=1, keepdims=True)
                - xhat * jnp.mean(u * xhat, axis=1, keepdims=True)
            )
            out_ref[part, :] = (gres_ref[part, :] + back * rstd).astype(BF)

    ins = list(terms) + [x, gain, gres]
    return pl.pallas_call(
        kernel,
        name="input_backward",
        grid=(1,),
        in_specs=[whole(a.shape) for a in ins],
        out_specs=whole((rows, D)),
        out_shape=jax.ShapeDtypeStruct((rows, D), BF),
        compiler_params=params("arbitrary"),
        cost_estimate=cost(1e8, 3e6),
    )(*ins)


def add_low(a, b):
    return (a.astype(F32) + b.astype(F32)).astype(BF)


def pick(v, index):
    return lax.dynamic_index_in_dim(v, index, 0, keepdims=False)


def after(v, *others):
    return lax.optimization_barrier((v, others))[0]


class Links:
    def __init__(self, n_dp, n_seq):
        self.n_dp, self.n_seq, self.nz = n_dp, n_seq, n_seq // 2

    def core(self, v):
        return lax.ppermute(v, "seq", [(s, s ^ 1) for s in range(self.n_seq)])

    def flip(self, v, bit):
        return lax.ppermute(v, "dp", [(i, i ^ bit) for i in range(self.n_dp)])

    def shift(self, v, k):
        n = self.nz
        return lax.ppermute(
            v, "seq", [(s, 2 * ((s // 2 + k) % n) + s % 2) for s in range(self.n_seq)]
        )


def order_matrix(source, valid):
    rows = lax.broadcasted_iota(jnp.int32, (768, 768), 0)
    return jnp.where((rows == source[None, :]) & valid[None, :], 1.0, 0.0).astype(BF)


def per_device(
    n_dp,
    n_seq,
    inputs,
    row_segment,
    row_flag,
    row_block,
    norm1_scale,
    w_qkv,
    w_out,
    norm2_scale,
    w_fc1,
    b_fc1,
    w_fc2,
    b_fc2,
    cotangent,
):
    links = Links(n_dp, n_seq)
    nz = links.nz
    local = inputs.shape[2]
    chunk = 2 * local
    heads = -(-H // nz)
    hw = heads * HD
    lq = -(-hw // 128) * 128
    fast = n_dp == 4 and nz == 4 and H % nz == 0
    d = lax.axis_index("dp")
    s = lax.axis_index("seq")
    z = s // 2
    c = s % 2
    place = jnp.stack([d, z, c]).astype(jnp.int32)
    n_w, b_w = D // n_seq, FF // n_seq
    cols = jnp.arange(768, dtype=jnp.int32)
    side, at = cols // 384, cols % 384
    out_order = order_matrix(
        n_w * (2 * ((z + at // n_w) % nz) + (c ^ side)) + at % n_w, at < 384
    )

    def to_both(w):
        return jnp.where(c == 0, w[0], w[1]), jnp.where(c == 0, w[1], w[0])

    x_loc = inputs[:, 0]
    labels = (row_segment[:, 0], row_flag[:, 0], row_block[:, 0])
    vectors = tuple(v.reshape(1, -1) for v in (norm1_scale, norm2_scale, b_fc2, b_fc1))
    came = links.core(message_rows(place, x_loc, labels, vectors))
    x_ext = own_rows(place, x_loc, labels, vectors, came)
    if nz == 4:
        x_before = links.shift(x_ext, 1)
        x_after = links.shift(x_ext, -1)
        x_low = links.shift(x_before[:144], 1)
        x_high = links.shift(x_after[144:], -1)
        gathered = [[x_ext], [x_after], [x_low, x_high], [x_before]]
    else:
        gathered = [[x_ext]] + [[links.shift(x_ext, -k)] for k in range(1, nz)]
    arrays, plan, extras = [], [], []
    for k, pieces in enumerate(gathered):
        at = 0
        for piece in pieces:
            rows = min(piece.shape[0], chunk - at)
            plan.append((len(arrays), 0, k * chunk + at, rows))
            at += rows
            arrays.append(piece)
        extras.append((len(arrays) - 1, pieces[-1].shape[0] - 16))
    freq = np.tile(
        np.float32(10000.0) ** (np.float32(-2.0) * np.arange(32, dtype=np.float32) / HD), 4
    )
    freq = jnp.asarray(freq.astype(np.float32)[None, :])
    cot = cotangent[:, 0]

    if fast:
        two = w_fc2.astype(BF).T.reshape(96, 2, 384)
        two_keep, two_send = to_both((two[:, 0], two[:, 1]))
        two = jnp.concatenate(to_both((two_keep, links.core(two_send))), axis=0)
        w12 = jnp.stack([w_fc1.astype(BF), two])
        w_before = links.shift(w12, 1)
        w_after = links.shift(w12, -1)
        w1_two = links.shift(w_before[0], 1)
        w2_two = links.shift(w_after[1], -1)
        w1 = jnp.stack([w12[0], w_after[0], w1_two, w_before[0]])
        w2 = jnp.stack([w12[1], w_after[1], w2_two, w_before[1]])

        qkv_order = order_matrix(
            256 * (cols % 384 // 96) + 96 * (c ^ side) + cols % 96, cols % 384 < 288
        )
        wq_parts = after(w_qkv.astype(BF), x_ext)
        parts = []
        for i in range(3):
            parts.append(
                lax.ppermute(
                    wq_parts[:, 96 * i : 96 * i + 96],
                    "seq",
                    [(q, (3 * q + i) % 8) for q in range(8)],
                )
            )
        parts = after(jnp.stack(parts), x_before, x_after)
        wq_own = jnp.concatenate(
            [pick(parts, (2 * t + s) % 3) for t in range(3)] + [w_out.astype(BF)], axis=1
        )
        wq_own = jnp.stack([wq_own, links.flip(wq_own, 1)])
        wq_own = jnp.stack([wq_own, links.flip(wq_own, 2)]).reshape(4, 192, 384)
        wq_own, qkv_order, out_order = lax.optimization_barrier((wq_own, qkv_order, out_order))
        wq = (wq_own, links.core(wq_own))
        wo_own = jnp.concatenate([wq_own[j, :, 288:] for j in range(4)], axis=1)

        arrays, w1, w2, wo_own = lax.optimization_barrier((arrays, w1, w2, wo_own))
        w1_in = links.flip(w1, 2)
        w2_in = links.flip(w2, 1)
        wo_all = [wo_own] + [links.shift(wo_own, -k) for k in range(1, 4)]
        ff_place = place
    else:

        def everywhere(w):
            w = lax.all_gather(w.astype(BF), "seq", axis=1, tiled=True)
            return lax.all_gather(w, "dp", axis=0, tiled=True)

        wq = everywhere(w_qkv).reshape(D, 3, D)
        wq = jnp.pad(wq, ((0, 0), (0, 0), (0, nz * hw - D)))
        wq = lax.dynamic_slice_in_dim(wq, z * hw, hw, 2)
        wq = (jnp.pad(wq, ((0, 0), (0, 0), (0, lq - hw))).reshape(D, 3 * lq),)
        wout = jnp.pad(everywhere(w_out), ((0, nz * hw - D), (0, 0))).reshape(nz, hw, D)
        w1 = lax.dynamic_slice_in_dim(everywhere(w_fc1), c * (FF // 2), FF // 2, 1)
        w1 = w1.reshape(2, 2, 192, 4, 384).transpose(3, 1, 0, 2, 4)
        w2 = lax.dynamic_slice_in_dim(everywhere(w_fc2), c * (FF // 2), FF // 2, 0)
        w2 = w2.reshape(2, 2, 384, 4, 192).transpose(3, 1, 0, 4, 2)
        w1, w2 = w1.transpose(1, 2, 0, 3, 4), w2.transpose(2, 1, 0, 3, 4)
        weights = (w1[0], w1[1], w2[0], w2[1])
        bias_all = lax.all_gather(b_fc1.astype(BF), "seq", axis=0, tiled=True).astype(F32)
        bias = lax.dynamic_slice_in_dim(bias_all, c * (FF // 2), FF // 2, 0).reshape(4, 384)
        bias = jnp.pad(bias, ((0, 4), (0, 0)))
        ff_place = jnp.stack([0 * d, 0 * z, c]).astype(jnp.int32)
    cot_in = links.core(after(cot, arrays))

    far = sorted(range(1, nz), key=lambda k: -min(k, nz - k))
    first = far[: nz // 2]
    rest = far[nz // 2 :] + [0]
    saved, by = attention_first(
        place, arrays, plan, extras, freq, wq, out_order, heads, chunk, first, (n_w, b_w)
    )
    h1, gains = saved[0], saved[9]
    rest_in = tuple(saved[i] for i in (1, 2, 4, 7, 8))
    if fast:
        bias = saved[11]
        w1_in, w2_in, wo_all, _ = lax.optimization_barrier((w1_in, w2_in, wo_all, h1))
        w1a = jnp.stack([w1, w1_in])
        w2a = jnp.stack([w2, w2_in])
        wo_all = jnp.stack(wo_all)
        wo_in = links.core(wo_all)
        w1b = links.flip(w1a, 1)
        w2b = links.flip(w2a, 2)
        weights = (w1a, w1b, w2a, w2b)
        rest_in = after(rest_in, w1a, w2a, wo_all)
    mixed = {k: links.shift(by[k][0], k) for k in first}
    by = {**by, **attention_rest(rest_in, heads, chunk, rest)}
    for k in rest:
        mixed[k] = links.shift(by[k][0], k) if k else by[k][0]
    mixed = [mixed[k] for k in range(nz)]
    h1_t = after(h1, by[0][0]).T
    if fast:
        wout = reorder_out(place, after(wo_all, by[0][0]), wo_in, out_order)
    residual, h2 = output_projection(place, mixed, wout, after(x_ext, h1_t), gains)
    h2_in = links.core(h2)
    (out_own, out_other, gh_own, gh_other, dw1a, dw1b, dw2a, dw2b, db1) = feed_forward(
        ff_place, h2, h2_in, cot, cot_in, weights, bias
    )
    gh_in = links.core(gh_other)
    out_in = links.core(out_other)
    gres, gproj, sums, gmixed = residual_backward(
        place, gh_own, gh_in, residual, cot, cot_in, gains, wout
    )
    if fast:
        dw1_in = links.flip(dw1b, 1)
        dw2_in = links.flip(dw2b, 2)
    pulled = [gmixed[0]] + [links.shift(gmixed[k], k) for k in range(1, nz)]
    pulled = [pulled[(nz - k) % nz] for k in range(nz)]
    part = attention_backward(pulled, by, saved, heads, chunk, [0], None, None)
    if fast:
        part, pulled, gproj = lax.optimization_barrier((part, pulled, gproj))
    out_rows = (residual + out_own + out_in.astype(F32) + gains[2:3]).astype(BF)
    rows_in = links.core(out_rows[local:])
    if fast:
        wo_keep, wo_send = out_weight(place, mixed, gproj, out_order)
        wo_came = links.core(wo_send)
        dw1_in, dw2_in, _ = lax.optimization_barrier((dw1_in, dw2_in, wo_keep))
        dw1_sum = add_low(dw1a[1], dw1_in[1])
        dw2_sum = add_low(dw2a[1], dw2_in[1])
        dwo = [
            add_low(wo_keep[..., 96 * k : 96 * k + 96], wo_came[..., 96 * k : 96 * k + 96])
            for k in range(4)
        ]
        dw1 = dw1a[0].astype(F32) + dw1_in[0].astype(F32)
        dw2 = dw2a[0].astype(F32) + dw2_in[0].astype(F32)
        part, dwo, dw1_sum, dw2_sum, dw1, dw2, _ = lax.optimization_barrier(
            (part, dwo, dw1_sum, dw2_sum, dw1, dw2, out_rows)
        )
        dw1_in = links.flip(dw1_sum, 2)
        dw2_in = links.flip(dw2_sum, 1)
        dwo = [dwo[0]] + [links.shift(dwo[k], k) for k in range(1, 4)]
    made = attention_backward(
        pulled, by, saved, heads, chunk, list(range(1, nz)), part, (sums, out_order)
    )
    if fast:
        made, dwo, dw1_in, dw2_in, rows_in = lax.optimization_barrier(
            (made, dwo, dw1_in, dw2_in, rows_in)
        )
    gqkv, vec_keep, vec_send, gh1 = made[0], made[1], made[2], made[3:]
    if nz == 4:
        low_in = links.shift(gh1[2], 1)
        high_in = links.shift(gh1[4], -1)
        if fast:
            wq_keep, wq_send = qkv_weight(place, h1_t, gqkv, qkv_order)
            low_in, high_in, wq_keep, wq_send = lax.optimization_barrier(
                (low_in, high_in, wq_keep, wq_send)
            )
        up = jnp.concatenate([add_low(gh1[1][:local], low_in), gh1[1][local:]], axis=0)
        down = jnp.concatenate([gh1[3][:local], add_low(gh1[3][local:], high_in)], axis=0)
        terms = [gh1[0], links.shift(up, 1), links.shift(down, -1)]
    else:
        terms = [gh1[0]] + [links.shift(gh1[k], k) for k in range(1, nz)]
    if fast:
        dw1_in, dw2_in, dwo, wq_send = lax.optimization_barrier((dw1_in, dw2_in, dwo, wq_send))
        dw1 = dw1 + dw1_in.astype(F32)
        dw2 = dw2 + dw2_in.astype(F32)
        dw = after(jnp.stack([dw1, dw2], axis=1).astype(BF), up, down)
        dw_came = (
            links.shift(dw[1], 1),
            links.shift(dw[3], -1),
            links.shift(dw[2], 2),
        )
        dwo = sum(t.astype(F32) for t in dwo)
        joint = jnp.concatenate(
            [add_low(wq_keep, links.core(wq_send)), dwo.astype(BF)], axis=2
        )
        joint = joint.reshape(2, 384, 384)
        vec = vec_keep + links.core(vec_send)
        vec = jnp.concatenate([vec[:3], db1[:, 0], jnp.zeros((9, 384), F32)], axis=0)
        came = links.flip(jnp.concatenate([joint[1], vec.astype(BF)], axis=0), 2)
        terms, came = lax.optimization_barrier((terms, came))
    grad_rows = input_backward(terms, x_ext, gains, gres)
    grad_in = links.core(grad_rows[local:])

    def by_micro(own, other):
        return jnp.where(c == 0, jnp.stack([own, other]), jnp.stack([other, own]))[:, None]

    outputs = by_micro(*after((out_rows[:local], rows_in), terms))
    input_grad = by_micro(grad_rows[:local], grad_in)
    if fast:
        joint = add_low(joint[0], came[:384]).reshape(2, 192, 384)
        vec = vec + came[384:].astype(F32)
        came = links.flip(jnp.concatenate([joint[1], vec.astype(BF)], axis=0), 1)
        joint = joint[0].astype(F32) + came[:192].astype(F32)
        vec = vec + came[192:].astype(F32)
        vec = [
            jnp.concatenate(
                [jnp.pad(vec[:3, 96 * k : 96 * k + 96], ((0, 0), (0, 288))), vec[3 + k : 4 + k]],
                axis=0,
            )
            for k in range(4)
        ]
        vec = sum([vec[0]] + [links.shift(vec[k], k) for k in range(1, 4)])
        vecs = (vec[0, :96], vec[1, :96], vec[3], vec[2, :96])
        g_out = joint[:, 288:]
        third = jnp.stack([joint[:, 96 * t : 96 * t + 96] for t in range(3)]).astype(BF)
        g_qkv = jnp.concatenate(
            [
                lax.ppermute(
                    pick(third, lax.rem(2 * (i - s + 9), 3)),
                    "seq",
                    [((3 * q + i) % 8, q) for q in range(8)],
                )
                for i in range(3)
            ],
            axis=1,
        ).astype(F32)
        dw_came, _ = lax.optimization_barrier((dw_came, (vecs, g_qkv, grad_rows)))
        dw_came = [v.astype(F32) for v in dw_came]
        dw = jnp.stack([dw1[0], dw2[0]]) + dw_came[0] + dw_came[1] + dw_came[2]
        g_fc1 = dw[0]
        keep, send = to_both((dw[1, :96], dw[1, 96:]))
        g_fc2 = jnp.concatenate(to_both((keep, links.core(send))), axis=1).T
    else:

        def owned(w):
            w = lax.psum_scatter(w.astype(BF), "seq", scatter_dimension=1, tiled=True)
            return lax.psum_scatter(w, "dp", scatter_dimension=0, tiled=True).astype(F32)

        dwq = jnp.einsum("rd,rj->dj", h1, gqkv, preferred_element_type=F32)
        spread = jnp.zeros((D, 3, nz * hw), F32)
        spread = lax.dynamic_update_slice_in_dim(
            spread, dwq.reshape(D, 3, lq)[..., :hw], z * hw, 2
        )
        g_qkv = owned(spread[..., :D].reshape(D, 3 * D))
        mixed_all = jnp.concatenate(mixed, axis=1)
        dwo = jnp.einsum("ri,ro->io", mixed_all, gproj, preferred_element_type=F32)
        dwo = dwo.reshape(nz, hw, D)
        dwo = jnp.roll(dwo[::-1], z + 1, axis=0).reshape(nz * hw, D)[:D]
        g_out = owned(dwo)
        half = jnp.stack([dw1a, dw1b]).transpose(1, 0, 3, 2, 4).reshape(D, FF // 2)
        full = lax.dynamic_update_slice_in_dim(
            jnp.zeros((D, FF), BF), half, c * (FF // 2), 1
        )
        g_fc1 = owned(full)
        half = jnp.stack([dw2a, dw2b]).transpose(0, 1, 4, 2, 3).reshape(FF // 2, D)
        full = lax.dynamic_update_slice_in_dim(
            jnp.zeros((FF, D), BF), half, c * (FF // 2), 0
        )
        g_fc2 = owned(full)
        bias_full = lax.dynamic_update_slice_in_dim(
            jnp.zeros((FF,), F32), db1.reshape(-1), c * (FF // 2), 0
        )
        bias_full = lax.psum(
            lax.psum_scatter(bias_full, "seq", scatter_dimension=0, tiled=True), "dp"
        )
        vec = vec_keep + links.core(vec_send)
        vec = vec[:3].reshape(3, nz, n_w)
        vec = sum([vec[:, 0]] + [links.shift(vec[:, k], k) for k in range(1, nz)])
        vec = lax.psum(vec, "dp")
        vecs = (vec[0], vec[1], bias_full, vec[2])

    return (
        outputs,
        input_grad,
        vecs[0],
        g_qkv,
        g_out,
        vecs[1],
        g_fc1,
        vecs[2],
        g_fc2,
        vecs[3],
    )


def solution(mesh):
    rows = P(None, "dp", "seq", None)
    labels = P(None, "dp", "seq")
    matrix = P("dp", "seq")
    vector = P("seq")
    return jax.shard_map(
        functools.partial(per_device, mesh.shape["dp"], mesh.shape["seq"]),
        mesh=mesh,
        in_specs=(
            rows, labels, labels, labels, vector, matrix, matrix, vector, matrix, vector, matrix,
            vector, rows,
        ),
        out_specs=(
            rows, rows, vector, matrix, matrix, vector, matrix, vector, matrix, vector,
        ),
        check_vma=False,
    )
```
